32 devices in a mesh: grp: 2 (over x), gx: 8 (over z, y), gy: 2 (over core).
Axes of the slice: x: 2, y: 2, z: 4, core: 2. Of those that a mesh axis runs over, the one named last changes fastest.
Arguments:
- warmth_anomaly: float32 [64, 128, 256], P('grp', 'gx', 'gy'), may hold values from -6 to 6
- humidity_anomaly: float32 [64, 128, 256], P('grp', 'gx', 'gy'), may hold values from -6 to 6
- horizontal_line_advective_ratio: float32 [64], replicated, may hold values from -0.5 to 0.5
- vertical_line_advective_ratio: float32 [64], replicated, may hold values from -0.5 to 0.5
- molecular_extinction_coefficient: float32 [112], replicated, may hold values from 0.002 to 0.05
- droplet_extinction_thickness: float32 [112], replicated, may hold values from 0.005 to 0.1
- shortwave_quadrature_share: float32 [112], replicated, may hold values from 0.5 to 5
- longwave_quadrature_share: float32 [112], replicated, may hold values from 0.5 to 5
- overcast_layer_flags: int32 [8192, 64], P(('grp', 'gx', 'gy')), may hold values 0 or 1
- profile_position_within_tile: int32 [64, 128], P('gx', 'gy'), may hold values from 0 to 511, as said below
Outputs:
- temperature_out: float32 [64, 128, 256], P('grp', 'gx', 'gy')
- moisture_out: float32 [64, 128, 256], P('grp', 'gx', 'gy')
- warming_rates: float32 [8192, 64], P(('grp', 'gx', 'gy'))
The draws below stay inside these ranges and needn't reach their ends.
Inputs may be any that keep to these rules, and one draw needn't show every extreme that they name: `profile_position_within_tile`: each tile's block of 8 x 64 entries holds every number from 0 to 511 exactly once.
All inputs are finite; a program needn't handle non-finite values. No bound on the sum of `overcast_layer_flags` on one device may be relied on, other than what follows from the above.
Results may differ from the reference program's by a relative error of at most 0.000092.
Values sent between devices are 32-bit elements; how exact they have to be, the bound alone decides.
A program may use at most 64 MiB of HBM per device.

```python
import math
import jax
import jax.numpy as jnp
from jax import lax

VERTICAL_LAYERS = 64
G = 112
SWEEPS = 8
MESH_HEIGHT = 128
MESH_WIDTH = 256
CXC = 8
CYC = 64
NXC = 64
NYC = 128
SLOTS = 512
BATCH_PROFILES = 256
NB = 8192
N_GRP = 2
N_GX = 8
N_GY = 2


def draw_profile_position_within_tile(key, part):
    tiles_x = NXC // CXC
    tiles_y = NYC // CYC
    keys = jax.random.split(key, tiles_x * tiles_y)
    perms = jax.vmap(lambda subkey: jax.random.permutation(subkey, CXC * CYC))(keys)
    perms = perms.reshape(tiles_x, tiles_y, CXC, CYC).transpose(0, 2, 1, 3)
    return perms.reshape(NXC, NYC).astype(jnp.int32)


def set_ends(values, stream_key, least, high):
    longest = values.shape.index(max(values.shape))
    spots = []
    for shift in (0, 1):
        where = [jax.random.randint(jax.random.fold_in(stream_key, axis), (), 0, length) for axis, length in enumerate(values.shape)]
        where[longest] = (where[longest] + shift) % values.shape[longest]
        spots.append(tuple(where))
    return values.at[spots[0]].set(least).at[spots[1]].set(high)


def levels(stream_key, shape, shards, least, high):
    def one(dim, shards_of):
        heights = jax.random.uniform(jax.random.fold_in(jax.random.fold_in(stream_key, 6), dim), (shards_of,), jnp.float32, least / len(shards), high / len(shards))
        return jnp.repeat(jnp.exp(heights), shape[dim] // shards_of).reshape((-1,) + (1,) * (len(shape) - dim - 1))

    gain = one(*shards[0])
    for cut in shards[1:]:
        gain = gain * one(*cut)
    return gain


def gaussian(stream_key, extent, spread, reach, cuts=(), kind=jnp.bfloat16):
    array = spread * jax.random.normal(stream_key, extent, jnp.float32)
    if cuts:
        array = array * levels(stream_key, extent, cuts, -0.22, 0.18)
    return jnp.clip(array, -reach, reach).astype(kind)


def setup_inputs(seed: int = 0) -> dict:
    splits = jax.random.split(jax.random.key(seed), 11)
    warmth_anomaly = gaussian(splits[0], (VERTICAL_LAYERS, MESH_HEIGHT, MESH_WIDTH), 1.0, 6.0, ((0, 2), (1, 8), (2, 2)), jnp.float32)
    humidity_anomaly = gaussian(splits[1], (VERTICAL_LAYERS, MESH_HEIGHT, MESH_WIDTH), 1.0, 6.0, ((0, 2), (1, 8), (2, 2)), jnp.float32)
    horizontal_line_advective_ratio = jnp.clip(jax.random.uniform(splits[2], (VERTICAL_LAYERS,), jnp.float32, -0.5, 0.5), -0.5, 0.5)
    vertical_line_advective_ratio = jnp.clip(jax.random.uniform(splits[3], (VERTICAL_LAYERS,), jnp.float32, -0.5, 0.5), -0.5, 0.5)
    molecular_extinction_coefficient = jnp.clip(jnp.exp(jax.random.uniform(splits[4], (G,), jnp.float32, math.log(0.002), math.log(0.05))), 0.002, 0.05)
    droplet_extinction_thickness = jnp.clip(jnp.exp(jax.random.uniform(splits[5], (G,), jnp.float32, math.log(0.005), math.log(0.1))), 0.005, 0.1)
    shortwave_quadrature_share = jnp.clip(jnp.exp(jax.random.uniform(splits[6], (G,), jnp.float32, math.log(0.5), math.log(5.0))), 0.5, 5.0)
    longwave_quadrature_share = jnp.clip(jnp.exp(jax.random.uniform(splits[7], (G,), jnp.float32, math.log(0.5), math.log(5.0))), 0.5, 5.0)
    overcast_layer_flags = set_ends((jax.random.randint(splits[8], (NB, VERTICAL_LAYERS), 0, 2) < 1).astype(jnp.int32), jax.random.fold_in(splits[8], 1), 0, 1)
    profile_position_within_tile = draw_profile_position_within_tile(jax.random.fold_in(splits[10], 71), 0)
    return dict(warmth_anomaly=warmth_anomaly, humidity_anomaly=humidity_anomaly, horizontal_line_advective_ratio=horizontal_line_advective_ratio, vertical_line_advective_ratio=vertical_line_advective_ratio, molecular_extinction_coefficient=molecular_extinction_coefficient, droplet_extinction_thickness=droplet_extinction_thickness, shortwave_quadrature_share=shortwave_quadrature_share, longwave_quadrature_share=longwave_quadrature_share, overcast_layer_flags=overcast_layer_flags, profile_position_within_tile=profile_position_within_tile)


NU_H = 0.15
NU_V = 0.15
HEATING_INTERVAL = 0.5


def advance_variable(grid_field, horizontal_line_advective_ratio, vertical_line_advective_ratio):
    row_next = jnp.roll(grid_field, -1, 1)
    row_prev = jnp.roll(grid_field, 1, 1)
    col_next = jnp.roll(grid_field, -1, 2)
    col_prev = jnp.roll(grid_field, 1, 2)
    padded = jnp.pad(grid_field, ((1, 1), (0, 0), (0, 0)))
    lev_next = padded[2:]
    lev_prev = padded[:-2]
    speed_x = horizontal_line_advective_ratio[:, None, None]
    speed_y = vertical_line_advective_ratio[:, None, None]
    return (grid_field - 0.5 * speed_x * (row_next - row_prev) - 0.5 * speed_y * (col_next - col_prev)
            + NU_H * (row_next + row_prev + col_next + col_prev - 4.0 * grid_field)
            + NU_V * (lev_next + lev_prev - 2.0 * grid_field))


def reduce_mesh_resolution(grid_field):
    return grid_field.reshape(VERTICAL_LAYERS, NXC, 2, NYC, 2).mean(axis=(2, 4))


def tile_slots(profile_position_within_tile):
    return profile_position_within_tile.reshape(N_GX, CXC, N_GY, CYC).transpose(0, 2, 1, 3).reshape(N_GX, N_GY, SLOTS)


def collect_profiles(coarse, profile_position_within_tile):
    tiles = coarse.reshape(VERTICAL_LAYERS, N_GX, CXC, N_GY, CYC).transpose(1, 3, 2, 4, 0).reshape(N_GX, N_GY, SLOTS, VERTICAL_LAYERS)
    inverse = jnp.argsort(tile_slots(profile_position_within_tile), axis=2).astype(jnp.int32)
    packed = jnp.take_along_axis(tiles, inverse[:, :, :, None], axis=2)
    return packed.reshape(N_GX, N_GY, N_GRP, BATCH_PROFILES, VERTICAL_LAYERS).transpose(2, 0, 1, 3, 4).reshape(NB, VERTICAL_LAYERS)


def unpack_columns(warming_rates, profile_position_within_tile):
    tiles = warming_rates.reshape(N_GRP, N_GX, N_GY, BATCH_PROFILES, VERTICAL_LAYERS).transpose(1, 2, 0, 3, 4).reshape(N_GX, N_GY, SLOTS, VERTICAL_LAYERS)
    placed = jnp.take_along_axis(tiles, tile_slots(profile_position_within_tile)[:, :, :, None], axis=2)
    return placed.reshape(N_GX, N_GY, CXC, CYC, VERTICAL_LAYERS).transpose(4, 0, 2, 1, 3).reshape(VERTICAL_LAYERS, NXC, NYC)


def refine_heat(coarse):
    even_rows = 0.75 * coarse + 0.25 * jnp.roll(coarse, 1, 1)
    odd_rows = 0.75 * coarse + 0.25 * jnp.roll(coarse, -1, 1)
    rows_done = jnp.stack([even_rows, odd_rows], axis=2).reshape(VERTICAL_LAYERS, MESH_HEIGHT, NYC)
    even_cols = 0.75 * rows_done + 0.25 * jnp.roll(rows_done, 1, 2)
    odd_cols = 0.75 * rows_done + 0.25 * jnp.roll(rows_done, -1, 2)
    return jnp.stack([even_cols, odd_cols], axis=3).reshape(VERTICAL_LAYERS, MESH_HEIGHT, MESH_WIDTH)


def radiate(theta_rows, moist_rows, mask_rows, molecular_extinction_coefficient, droplet_extinction_thickness, shortwave_quadrature_share, longwave_quadrature_share):
    absorber = jax.nn.softplus(moist_rows)
    cloudy = mask_rows.astype(jnp.float32)
    optical_depth = absorber[:, :, None] * molecular_extinction_coefficient + cloudy[:, :, None] * droplet_extinction_thickness
    optical_path_above = jnp.cumsum(optical_depth, axis=1) - optical_depth
    absorbed = 1.0 - jnp.exp(-optical_depth)
    shortwave_total = jnp.sum(shortwave_quadrature_share * jnp.exp(-optical_path_above) * absorbed, axis=2)
    longwave_total = jnp.sum(longwave_quadrature_share * absorbed, axis=2)
    return (shortwave_total - longwave_total * (1.0 + 0.1 * theta_rows)) * (4.0 / G)


def reference(warmth_anomaly, humidity_anomaly, horizontal_line_advective_ratio, vertical_line_advective_ratio, molecular_extinction_coefficient, droplet_extinction_thickness, shortwave_quadrature_share, longwave_quadrature_share, overcast_layer_flags, profile_position_within_tile):
    theta_vertical_profile = collect_profiles(reduce_mesh_resolution(warmth_anomaly), profile_position_within_tile)
    humidity_profile = collect_profiles(reduce_mesh_resolution(humidity_anomaly), profile_position_within_tile)
    partitions = NB // BATCH_PROFILES

    def within_partition(items):
        return radiate(items[0], items[1], items[2], molecular_extinction_coefficient, droplet_extinction_thickness, shortwave_quadrature_share, longwave_quadrature_share)

    warming_rates = lax.map(within_partition, (theta_vertical_profile.reshape(partitions, BATCH_PROFILES, VERTICAL_LAYERS), humidity_profile.reshape(partitions, BATCH_PROFILES, VERTICAL_LAYERS),
                                  overcast_layer_flags.reshape(partitions, BATCH_PROFILES, VERTICAL_LAYERS))).reshape(NB, VERTICAL_LAYERS)
    warming_refined = refine_heat(unpack_columns(warming_rates, profile_position_within_tile))
    present_heat_anomaly = warmth_anomaly
    humidity_present = humidity_anomaly
    for sweep_index in range(SWEEPS):
        present_heat_anomaly = advance_variable(present_heat_anomaly, horizontal_line_advective_ratio, vertical_line_advective_ratio)
        humidity_present = advance_variable(humidity_present, horizontal_line_advective_ratio, vertical_line_advective_ratio)
    return present_heat_anomaly + HEATING_INTERVAL * warming_refined, humidity_present, warming_rates
```

```python
import functools
import math

import jax
import jax.numpy as jnp
from jax import lax
from jax.experimental import pallas as pl
from jax.experimental.pallas import tpu as pltpu
from jax.sharding import PartitionSpec as P

SWEEPS = 8
NU_H = 0.15
NU_V = 0.15
HEATING_INTERVAL = 0.5
UNROLL = 8
M = 8
MESH = pl.DeviceIdType.MESH
BF = jnp.bfloat16
F32 = jnp.float32


def split_bf16(x):
    hi = x.astype(BF)
    lo = (x - hi.astype(F32)).astype(BF)
    return hi, lo


def kernel(
    n_gx, n_gy, L, R, C, S, B, G,
    warm_in, humid_in, cx_ref, cy_ref, gas_ref, drop_ref, sw_ref, lw_ref, flags_ref, slot_ref,
    t_out, m_out, rates_out,
    ext0, ext1, edge_send, edge_recv, qt, packed, rad, coef, cloudy, absorber, theta, rates, heat, ucols,
    hedge_send, hedge_recv, rows_send, rows_recv,
    halo_send_sem, halo_recv_sem, edge_send_sem, edge_recv_sem, misc_send_sem, misc_recv_sem,
):
    g = lax.axis_index("grp")
    x = lax.axis_index("gx")
    y = lax.axis_index("gy")
    og = 1 - g
    xn, xp = lax.rem(x + 1, n_gx), lax.rem(x + n_gx - 1, n_gx)
    yn, yp = lax.rem(y + 1, n_gy), lax.rem(y + n_gy - 1, n_gy)
    fields = (warm_in, humid_in)
    ext = (ext0, ext1)
    outs = (t_out, m_out)
    LE = L + M
    T = (R + 2 * M) // 8
    per = C // T
    NP = -(-LE // per)
    RI = R // 2
    RLO = 8
    ROWN = RLO + M
    RE = R + 2 * M

    barrier = pltpu.get_barrier_semaphore()
    for dev in ((g, xn, y), (g, xp, y), (og, x, y), (og, xn, y), (og, xp, y), (g, x, yn), (g, x, yp)):
        pl.semaphore_signal(barrier, inc=1, device_id=dev, device_id_type=MESH)
    pl.semaphore_wait(barrier, 7)

    def remote(src, dst, ss, rs, dev):
        c = pltpu.make_async_remote_copy(
            src_ref=src, dst_ref=dst, send_sem=ss, recv_sem=rs, device_id=dev, device_id_type=MESH
        )
        c.start()
        return c

    half = slot_ref.shape[1]
    slots = slot_ref[...]
    rep = (
        lax.broadcasted_iota(jnp.int32, (half, C), 1) // 2
        == lax.broadcasted_iota(jnp.int32, (half, C), 0)
    ).astype(F32).astype(BF)
    s_hi = (slots // 16).astype(F32).astype(BF)
    s_lo = (slots % 16).astype(F32).astype(BF)
    slot_rep = (
        16.0 * jnp.dot(s_hi, rep, preferred_element_type=F32)
        + jnp.dot(s_lo, rep, preferred_element_type=F32)
    ).astype(jnp.int32)
    s_iota = lax.broadcasted_iota(jnp.int32, (S, C), 0)
    for i in range(RI):
        qt[:, i * C : (i + 1) * C] = jnp.where(s_iota == slot_rep[i : i + 1, :], 1.0, 0.0).astype(BF)
    parts = []
    for i in range(RI):
        col = []
        for f in range(2):
            flat = fields[f].reshape(L * R, C)
            col.append(
                flat[pl.ds(2 * i, L, stride=R), :] + flat[pl.ds(2 * i + 1, L, stride=R), :]
            )
        hi, lo = split_bf16(0.25 * jnp.concatenate(col, axis=0))
        parts.append(jnp.concatenate([hi, lo], axis=0))
    lhs = jnp.concatenate(parts, axis=1)
    both = lax.dot_general(
        lhs, qt[...], (((1,), (1,)), ((), ())), preferred_element_type=F32
    )
    both = both[: 2 * L] + both[2 * L :]
    for h in range(2):
        packed[h] = both[:, h * B : (h + 1) * B]
    c_packed = remote(packed.at[og], rad.at[g], misc_send_sem.at[0], misc_recv_sem.at[0], (og, x, y))

    lev_src = (L - M) * og
    lev_dst = 1 + L * g
    own_dst = 1 + M * g
    halos = []
    n = 0
    for f in range(2):
        for levs, dlevs, count, gg in ((0, own_dst, L, g), (lev_src, lev_dst, M, og)):
            for r0, d0, xx in ((R - M, RLO, xn), (0, ROWN + R, xp)):
                halos.append(remote(
                    fields[f].at[pl.ds(levs, count), r0 : r0 + M, :],
                    ext0.at[f, pl.ds(dlevs, count), d0 : d0 + M, :],
                    halo_send_sem.at[n], halo_recv_sem.at[n], (gg, xx, y),
                ))
                n += 1
        halos.append(remote(
            fields[f].at[pl.ds(lev_src, M)],
            ext0.at[f, pl.ds(lev_dst, M), ROWN : ROWN + R, :],
            halo_send_sem.at[n], halo_recv_sem.at[n], (og, x, y),
        ))
        n += 1
    rad[g] = packed[g]
    for f in range(2):
        ext0[f, pl.ds(own_dst, L), ROWN : ROWN + R, :] = fields[f][...]
        for b in range(2):
            for p in (0, LE + 1):
                ext[b][f, p] = jnp.zeros((RE + 16, C), F32)

    log2e = 1.0 / math.log(2.0)
    for q, (ref, scale) in enumerate(((gas_ref, -log2e), (drop_ref, -log2e), (sw_ref, 1.0), (lw_ref, 1.0))):
        coef[q] = jnp.broadcast_to(ref[...] * scale, (128, G)).T
    for hb in range(B // 128):
        cloudy[hb] = flags_ref[:, hb * 128 : (hb + 1) * 128].astype(F32)

    c_packed.wait()
    for o in range(2):
        mo = rad[o, L : 2 * L, :]
        soft = jnp.maximum(mo, 0.0) + jnp.log1p(jnp.exp(-jnp.abs(mo)))
        for hb in range(B // 128):
            absorber[hb, o * L : (o + 1) * L, :] = soft[:, hb * 128 : (hb + 1) * 128]
            theta[hb, o * L : (o + 1) * L, :] = rad[o, 0:L, hb * 128 : (hb + 1) * 128]

    GB = G // 8
    norm = 4.0 / G
    for hb in range(B // 128):
        for o in range(2):
            def level(l, flux, o=o, hb=hb):
                lg = l + o * L
                a = jnp.broadcast_to(absorber[hb, pl.ds(lg, 1), :], (8, 128))
                c = jnp.broadcast_to(cloudy[hb, pl.ds(lg, 1), :], (8, 128))
                th = 1.0 + 0.1 * theta[hb, pl.ds(lg, 1), :]
                sw = lw = None
                new = []
                for q in range(GB):
                    rows = slice(8 * q, 8 * q + 8)
                    d = 1.0 - jnp.exp2(a * coef[0, rows, :] + c * coef[1, rows, :])
                    s = flux[q] * d
                    w = coef[3, rows, :] * d
                    sw = s if sw is None else sw + s
                    lw = w if lw is None else lw + w
                    new.append(flux[q] - s)
                total = jnp.sum(sw - lw * th, axis=0, keepdims=True) * norm
                rates[o, hb, pl.ds(l, 1), :] = total
                return tuple(new)

            if o == 0:
                flux = tuple(coef[2, 8 * q : 8 * q + 8, :] for q in range(GB))
            flux = lax.fori_loop(0, L, level, flux, unroll=2)
    c_heat = remote(rates.at[og], heat.at[g], misc_send_sem.at[1], misc_recv_sem.at[1], (og, x, y))
    heat[g] = rates[g]
    for o in range(2):
        for hb in range(B // 128):
            rates_out[o * L : (o + 1) * L, hb * 128 : (hb + 1) * 128] = rates[o, hb]

    lane = lax.broadcasted_iota(jnp.int32, (8, C), 1)

    def pack(vals, j, accs):
        right, left = accs
        for t in range(T):
            k = j * T + t
            turned = pltpu.roll(vals[8 * t : 8 * t + 8, :], lax.rem(k + 1, C), 1)
            right = jnp.where(lane == k, turned, right)
            left = jnp.where(lane == lax.rem(k + 1, C), turned, left)
        return right, left

    def send_edges(k, f):
        return (
            remote(edge_send.at[k, f, 0], edge_recv.at[k, f, 0],
                   edge_send_sem.at[k, f, 0], edge_recv_sem.at[k, f, 0], (g, x, yn)),
            remote(edge_send.at[k, f, 1], edge_recv.at[k, f, 1],
                   edge_send_sem.at[k, f, 1], edge_recv_sem.at[k, f, 1], (g, x, yp)),
        )

    zero = jnp.zeros((8, C), F32)

    def run_levels(k, f, count, values):
        for p in range(NP):
            lo, hi = p * per, min(count, (p + 1) * per)
            if lo >= hi:
                edge_send[k, f, 0, p] = zero
                edge_send[k, f, 1, p] = zero
                continue
            right, left = lax.fori_loop(
                lo, hi, lambda j, accs, lo=lo: pack(values(j), j - lo, accs), (zero, zero),
                unroll=min(UNROLL, hi - lo),
            )
            edge_send[k, f, 0, p] = right
            edge_send[k, f, 1, p] = left

    def first(f):
        run_levels(0, f, LE, lambda j: ext0[f, j + 1, RLO : RLO + RE, :])
        return send_edges(0, f)

    def sweep(k, f):
        src, dst = (k - 1) % 2, k % 2
        start = g * k
        last = k == SWEEPS
        t0, t1 = (M // 8, M // 8 + R // 8) if last else (0, T)
        r0, r1 = RLO + 8 * t0, RLO + 8 * t1

        def values(j):
            lev = start + j
            p = lev + 1
            jj = j + g
            which = jj // per
            kk = (jj - which * per) * T
            from_left = edge_recv[k - 1, f, 0, which]
            from_right = edge_recv[k - 1, f, 1, which]
            lg = lev + (L - M) * g
            sx = 0.5 * cx_ref[lg]
            sy = 0.5 * cy_ref[lg]
            cen = ext[src][f, p, r0:r1, :]
            base = (
                (1.0 - 4.0 * NU_H - 2.0 * NU_V) * cen
                + NU_V * (ext[src][f, p + 1, r0:r1, :] + ext[src][f, p - 1, r0:r1, :])
                + (NU_H - sx) * ext[src][f, p, r0 + 1 : r1 + 1, :]
                + (NU_H + sx) * ext[src][f, p, r0 - 1 : r1 - 1, :]
            )
            res = []
            for t in range(t0, t1):
                q = 8 * (t - t0)
                v = cen[q : q + 8, :]
                kt = kk + t
                prev = jnp.where(lane == 0, pltpu.roll(from_left, lax.rem(C - kt, C), 1), pltpu.roll(v, 1, 1))
                nxt = jnp.where(
                    lane == C - 1, pltpu.roll(from_right, lax.rem(2 * C - 2 - kt, C), 1), pltpu.roll(v, C - 1, 1)
                )
                res.append(base[q : q + 8, :] + (NU_H - sy) * nxt + (NU_H + sy) * prev)
            new = jnp.concatenate(res, axis=0)
            if last:
                outs[f][j] = new
            else:
                ext[dst][f, p, RLO : RLO + RE, :] = new
            return new

        count = LE - k
        if last:
            @pl.loop(0, count, unroll=UNROLL)
            def _(j):
                values(j)
            return None
        run_levels(k, f, count, values)
        return send_edges(k, f)

    for c in halos:
        c.wait()
    flight = [first(0), first(1)]
    sent = []

    def advance(ks):
        for k in ks:
            for f in range(2):
                for c in flight[f]:
                    c.wait()
                flight[f] = sweep(k, f)

    advance((1, 2))

    c_heat.wait()
    hi, lo = split_bf16(jnp.concatenate([heat[h, hb] for h in range(2) for hb in range(B // 128)], axis=1))
    spread = jnp.dot(jnp.concatenate([hi, lo], axis=0), qt[...], preferred_element_type=F32)
    spread = spread[:L] + spread[L:]
    LT = L // 8
    ehi = zero
    elo = zero
    for i in range(RI):
        ui = spread[:, i * C : (i + 1) * C]
        ucols[i] = ui
        for t in range(LT):
            k = i * LT + t
            turned = pltpu.roll(ui[8 * t : 8 * t + 8, :], (k + 1) % C, 1)
            ehi = jnp.where(lane == k, turned, ehi)
            elo = jnp.where(lane == (k + 1) % C, turned, elo)
    hedge_send[0] = ehi
    hedge_send[1] = elo
    c_he = [
        remote(hedge_send.at[0], hedge_recv.at[0], misc_send_sem.at[2], misc_recv_sem.at[2], (g, x, yn)),
        remote(hedge_send.at[1], hedge_recv.at[1], misc_send_sem.at[3], misc_recv_sem.at[3], (g, x, yp)),
    ]
    advance((3,))
    for c in c_he:
        c.wait()
    from_left = hedge_recv[0]
    from_right = hedge_recv[1]
    even = lane % 2 == 0
    for i in range(RI):
        for t in range(LT):
            k = i * LT + t
            v = ucols[i, 8 * t : 8 * t + 8, :]
            prev = jnp.where(lane == 0, pltpu.roll(from_left, (C - k) % C, 1), pltpu.roll(v, 1, 1))
            nxt = jnp.where(lane == C - 1, pltpu.roll(from_right, (2 * C - 2 - k) % C, 1), pltpu.roll(v, C - 1, 1))
            w = 0.75 * v + 0.25 * jnp.where(even, prev, nxt)
            ucols[i, 8 * t : 8 * t + 8, :] = w
            if i == 0:
                rows_send[0, 8 * t : 8 * t + 8, :] = w
            if i == RI - 1:
                rows_send[1, 8 * t : 8 * t + 8, :] = w
    c_rows = [
        remote(rows_send.at[0], rows_recv.at[0], misc_send_sem.at[4], misc_recv_sem.at[4], (g, xp, y)),
        remote(rows_send.at[1], rows_recv.at[1], misc_send_sem.at[5], misc_recv_sem.at[5], (g, xn, y)),
    ]
    advance(range(4, SWEEPS + 1))
    for c in c_rows:
        c.wait()
    flat = t_out.reshape(L * R, C)
    for i in range(RI):
        v = ucols[i]
        above = rows_recv[1] if i == 0 else ucols[i - 1]
        below = rows_recv[0] if i == RI - 1 else ucols[i + 1]
        flat[pl.ds(2 * i, L, stride=R), :] = flat[pl.ds(2 * i, L, stride=R), :] + HEATING_INTERVAL * (0.75 * v + 0.25 * above)
        flat[pl.ds(2 * i + 1, L, stride=R), :] = flat[pl.ds(2 * i + 1, L, stride=R), :] + HEATING_INTERVAL * (0.75 * v + 0.25 * below)


def hand_on(t_in, m_in, r_in, t_out, m_out, r_out):
    t_out[...] = t_in[...]
    m_out[...] = m_in[...]
    r_out[...] = r_in[...]


def body(n_gx, n_gy, warm, humid, cx, cy, gas, drop, sw, lw, flags, slots):
    L, R, C = warm.shape
    S = slots.shape[0] * slots.shape[1]
    B = flags.shape[0]
    flags = flags.T
    G = gas.shape[0]
    LE = L + M
    T = (R + 2 * M) // 8
    NP = -(-LE // (C // T))
    vmem = pl.BlockSpec(memory_space=pltpu.VMEM)
    smem = pl.BlockSpec(memory_space=pltpu.SMEM)
    t, m, rates = pl.pallas_call(
        functools.partial(kernel, n_gx, n_gy, L, R, C, S, B, G),
        out_shape=(
            jax.ShapeDtypeStruct((L, R, C), F32),
            jax.ShapeDtypeStruct((L, R, C), F32),
            jax.ShapeDtypeStruct((2 * L, B), F32),
        ),
        in_specs=[vmem, vmem, smem, smem] + [vmem] * 6,
        out_specs=(vmem, vmem, vmem),
        scratch_shapes=[
            pltpu.VMEM((2, LE + 2, R + 2 * M + 16, C), F32),
            pltpu.VMEM((2, LE + 2, R + 2 * M + 16, C), F32),
            pltpu.VMEM((SWEEPS, 2, 2, NP, 8, C), F32),
            pltpu.VMEM((SWEEPS, 2, 2, NP, 8, C), F32),
            pltpu.VMEM((S, (R // 2) * C), BF),
            pltpu.VMEM((2, 2 * L, B), F32),
            pltpu.VMEM((2, 2 * L, B), F32),
            pltpu.VMEM((4, G, 128), F32),
            pltpu.VMEM((B // 128, 2 * L, 128), F32),
            pltpu.VMEM((B // 128, 2 * L, 128), F32),
            pltpu.VMEM((B // 128, 2 * L, 128), F32),
            pltpu.VMEM((2, B // 128, L, 128), F32),
            pltpu.VMEM((2, B // 128, L, 128), F32),
            pltpu.VMEM((R // 2, L, C), F32),
            pltpu.VMEM((2, 8, C), F32),
            pltpu.VMEM((2, 8, C), F32),
            pltpu.VMEM((2, L, C), F32),
            pltpu.VMEM((2, L, C), F32),
            pltpu.SemaphoreType.DMA((10,)),
            pltpu.SemaphoreType.DMA((10,)),
            pltpu.SemaphoreType.DMA((SWEEPS, 2, 2)),
            pltpu.SemaphoreType.DMA((SWEEPS, 2, 2)),
            pltpu.SemaphoreType.DMA((6,)),
            pltpu.SemaphoreType.DMA((6,)),
        ],
        compiler_params=pltpu.CompilerParams(collective_id=0, has_side_effects=True, vmem_limit_bytes=32*1024*1024),
    )(
        warm, humid, cx, cy, gas[None], drop[None], sw[None], lw[None], flags, slots,
    )
    t, m, rates = pl.pallas_call(
        hand_on,
        out_shape=tuple(jax.ShapeDtypeStruct(a.shape, F32) for a in (t, m, rates)),
        in_specs=[vmem] * 3,
        out_specs=(vmem,) * 3, compiler_params=pltpu.CompilerParams(vmem_limit_bytes=8*1024*1024),
    )(t, m, rates)
    return t, m, rates.T


def solution(mesh):
    assert mesh.shape["grp"] == 2
    in_specs = (
        P("grp", "gx", "gy"), P("grp", "gx", "gy"), P(), P(), P(), P(), P(), P(),
        P(("grp", "gx", "gy"), None), P("gx", "gy"),
    )
    out_specs = (P("grp", "gx", "gy"), P("grp", "gx", "gy"), P(("grp", "gx", "gy"), None))
    return jax.shard_map(
        functools.partial(body, mesh.shape["gx"], mesh.shape["gy"]),
        mesh=mesh, in_specs=in_specs, out_specs=out_specs, check_vma=False,
    )
```

```python
import functools
import math

import jax
import jax.numpy as jnp
from jax import lax
from jax.experimental import pallas as pl
from jax.experimental.pallas import tpu as pltpu
from jax.sharding import PartitionSpec as P

SWEEPS = 8
NU_H = 0.15
NU_V = 0.15
HEATING_INTERVAL = 0.5
UNROLL = 8
M = 8
MESH = pl.DeviceIdType.MESH
BF = jnp.bfloat16
F32 = jnp.float32


def split_bf16(x):
    hi = x.astype(BF)
    lo = (x - hi.astype(F32)).astype(BF)
    return hi, lo


def wide_kernel(
    n_gx, n_gy, L, R, C, S, B, G,
    warm_in, humid_in, cx_ref, cy_ref, gas_ref, drop_ref, sw_ref, lw_ref, flags_ref, slot_ref,
    t_out, m_out, rates_out,
    ext0, ext1, edge_send, edge_recv, qt, packed, rad, coef, cloudy, absorber, theta, rates, heat, ucols,
    hedge_send, hedge_recv, rows_send, rows_recv,
    halo_send_sem, halo_recv_sem, edge_send_sem, edge_recv_sem, misc_send_sem, misc_recv_sem,
):
    g = lax.axis_index("grp")
    x = lax.axis_index("gx")
    y = lax.axis_index("gy")
    og = 1 - g
    xn, xp = lax.rem(x + 1, n_gx), lax.rem(x + n_gx - 1, n_gx)
    yn, yp = lax.rem(y + 1, n_gy), lax.rem(y + n_gy - 1, n_gy)
    fields = (warm_in, humid_in)
    ext = (ext0, ext1)
    outs = (t_out, m_out)
    LE = L + M
    T = (R + 2 * M) // 8
    per = C // T
    NP = -(-LE // per)
    RI = R // 2
    RLO = 8
    ROWN = RLO + M
    RE = R + 2 * M

    barrier = pltpu.get_barrier_semaphore()
    for dev in ((g, xn, y), (g, xp, y), (og, x, y), (og, xn, y), (og, xp, y), (g, x, yn), (g, x, yp)):
        pl.semaphore_signal(barrier, inc=1, device_id=dev, device_id_type=MESH)
    pl.semaphore_wait(barrier, 7)

    def remote(src, dst, ss, rs, dev):
        c = pltpu.make_async_remote_copy(
            src_ref=src, dst_ref=dst, send_sem=ss, recv_sem=rs, device_id=dev, device_id_type=MESH
        )
        c.start()
        return c

    half = slot_ref.shape[1]
    slots = slot_ref[...]
    rep = (
        lax.broadcasted_iota(jnp.int32, (half, C), 1) // 2
        == lax.broadcasted_iota(jnp.int32, (half, C), 0)
    ).astype(F32).astype(BF)
    s_hi = (slots // 16).astype(F32).astype(BF)
    s_lo = (slots % 16).astype(F32).astype(BF)
    slot_rep = (
        16.0 * jnp.dot(s_hi, rep, preferred_element_type=F32)
        + jnp.dot(s_lo, rep, preferred_element_type=F32)
    ).astype(jnp.int32)
    s_iota = lax.broadcasted_iota(jnp.int32, (S, C), 0)
    for i in range(RI):
        qt[:, i * C : (i + 1) * C] = jnp.where(s_iota == slot_rep[i : i + 1, :], 1.0, 0.0).astype(BF)
    parts = []
    for i in range(RI):
        col = []
        for f in range(2):
            flat = fields[f].reshape(L * R, C)
            col.append(
                flat[pl.ds(2 * i, L, stride=R), :] + flat[pl.ds(2 * i + 1, L, stride=R), :]
            )
        hi, lo = split_bf16(0.25 * jnp.concatenate(col, axis=0))
        parts.append(jnp.concatenate([hi, lo], axis=0))
    lhs = jnp.concatenate(parts, axis=1)
    both = lax.dot_general(
        lhs, qt[...], (((1,), (1,)), ((), ())), preferred_element_type=F32
    )
    both = both[: 2 * L] + both[2 * L :]
    for h in range(2):
        packed[h] = both[:, h * B : (h + 1) * B]
    c_packed = remote(packed.at[og], rad.at[g], misc_send_sem.at[0], misc_recv_sem.at[0], (og, x, y))

    lev_src = (L - M) * og
    lev_dst = 1 + L * g
    own_dst = 1 + M * g
    halos = []
    n = 0
    for f in range(2):
        for levs, dlevs, count, gg in ((0, own_dst, L, g), (lev_src, lev_dst, M, og)):
            for r0, d0, xx in ((R - M, RLO, xn), (0, ROWN + R, xp)):
                halos.append(remote(
                    fields[f].at[pl.ds(levs, count), r0 : r0 + M, :],
                    ext0.at[f, pl.ds(dlevs, count), d0 : d0 + M, :],
                    halo_send_sem.at[n], halo_recv_sem.at[n], (gg, xx, y),
                ))
                n += 1
        halos.append(remote(
            fields[f].at[pl.ds(lev_src, M)],
            ext0.at[f, pl.ds(lev_dst, M), ROWN : ROWN + R, :],
            halo_send_sem.at[n], halo_recv_sem.at[n], (og, x, y),
        ))
        n += 1
    rad[g] = packed[g]
    for f in range(2):
        ext0[f, pl.ds(own_dst, L), ROWN : ROWN + R, :] = fields[f][...]
        for b in range(2):
            for p in (0, LE + 1):
                ext[b][f, p] = jnp.zeros((RE + 16, C), F32)

    log2e = 1.0 / math.log(2.0)
    for q, (ref, scale) in enumerate(((gas_ref, -log2e), (drop_ref, -log2e), (sw_ref, 1.0), (lw_ref, 1.0))):
        coef[q] = jnp.broadcast_to(ref[...] * scale, (128, G)).T
    for hb in range(B // 128):
        cloudy[hb] = flags_ref[:, hb * 128 : (hb + 1) * 128].astype(F32)

    c_packed.wait()
    for o in range(2):
        mo = rad[o, L : 2 * L, :]
        soft = jnp.maximum(mo, 0.0) + jnp.log1p(jnp.exp(-jnp.abs(mo)))
        for hb in range(B // 128):
            absorber[hb, o * L : (o + 1) * L, :] = soft[:, hb * 128 : (hb + 1) * 128]
            theta[hb, o * L : (o + 1) * L, :] = rad[o, 0:L, hb * 128 : (hb + 1) * 128]

    GB = G // 8
    norm = 4.0 / G
    for hb in range(B // 128):
        for o in range(2):
            def level(l, flux, o=o, hb=hb):
                lg = l + o * L
                a = jnp.broadcast_to(absorber[hb, pl.ds(lg, 1), :], (8, 128))
                c = jnp.broadcast_to(cloudy[hb, pl.ds(lg, 1), :], (8, 128))
                th = 1.0 + 0.1 * theta[hb, pl.ds(lg, 1), :]
                sw = lw = None
                new = []
                for q in range(GB):
                    rows = slice(8 * q, 8 * q + 8)
                    d = 1.0 - jnp.exp2(a * coef[0, rows, :] + c * coef[1, rows, :])
                    s = flux[q] * d
                    w = coef[3, rows, :] * d
                    sw = s if sw is None else sw + s
                    lw = w if lw is None else lw + w
                    new.append(flux[q] - s)
                total = jnp.sum(sw - lw * th, axis=0, keepdims=True) * norm
                rates[o, hb, pl.ds(l, 1), :] = total
                return tuple(new)

            if o == 0:
                flux = tuple(coef[2, 8 * q : 8 * q + 8, :] for q in range(GB))
            flux = lax.fori_loop(0, L, level, flux, unroll=2)
    c_heat = remote(rates.at[og], heat.at[g], misc_send_sem.at[1], misc_recv_sem.at[1], (og, x, y))
    heat[g] = rates[g]
    for o in range(2):
        for hb in range(B // 128):
            rates_out[o * L : (o + 1) * L, hb * 128 : (hb + 1) * 128] = rates[o, hb]

    lane = lax.broadcasted_iota(jnp.int32, (8, C), 1)

    def pack(vals, j, accs):
        right, left = accs
        for t in range(T):
            k = j * T + t
            turned = pltpu.roll(vals[8 * t : 8 * t + 8, :], lax.rem(k + 1, C), 1)
            right = jnp.where(lane == k, turned, right)
            left = jnp.where(lane == lax.rem(k + 1, C), turned, left)
        return right, left

    def send_edges(k, f):
        return (
            remote(edge_send.at[k, f, 0], edge_recv.at[k, f, 0],
                   edge_send_sem.at[k, f, 0], edge_recv_sem.at[k, f, 0], (g, x, yn)),
            remote(edge_send.at[k, f, 1], edge_recv.at[k, f, 1],
                   edge_send_sem.at[k, f, 1], edge_recv_sem.at[k, f, 1], (g, x, yp)),
        )

    zero = jnp.zeros((8, C), F32)

    def run_levels(k, f, count, values):
        for p in range(NP):
            lo, hi = p * per, min(count, (p + 1) * per)
            if lo >= hi:
                edge_send[k, f, 0, p] = zero
                edge_send[k, f, 1, p] = zero
                continue
            right, left = lax.fori_loop(
                lo, hi, lambda j, accs, lo=lo: pack(values(j), j - lo, accs), (zero, zero),
                unroll=min(UNROLL, hi - lo),
            )
            edge_send[k, f, 0, p] = right
            edge_send[k, f, 1, p] = left

    def first(f):
        run_levels(0, f, LE, lambda j: ext0[f, j + 1, RLO : RLO + RE, :])
        return send_edges(0, f)

    def sweep(k, f):
        src, dst = (k - 1) % 2, k % 2
        start = g * k
        last = k == SWEEPS
        t0, t1 = (M // 8, M // 8 + R // 8) if last else (0, T)
        r0, r1 = RLO + 8 * t0, RLO + 8 * t1

        def values(j):
            lev = start + j
            p = lev + 1
            jj = j + g
            which = jj // per
            kk = (jj - which * per) * T
            from_left = edge_recv[k - 1, f, 0, which]
            from_right = edge_recv[k - 1, f, 1, which]
            lg = lev + (L - M) * g
            sx = 0.5 * cx_ref[lg]
            sy = 0.5 * cy_ref[lg]
            cen = ext[src][f, p, r0:r1, :]
            base = (
                (1.0 - 4.0 * NU_H - 2.0 * NU_V) * cen
                + NU_V * (ext[src][f, p + 1, r0:r1, :] + ext[src][f, p - 1, r0:r1, :])
                + (NU_H - sx) * ext[src][f, p, r0 + 1 : r1 + 1, :]
                + (NU_H + sx) * ext[src][f, p, r0 - 1 : r1 - 1, :]
            )
            res = []
            for t in range(t0, t1):
                q = 8 * (t - t0)
                v = cen[q : q + 8, :]
                kt = kk + t
                prev = jnp.where(lane == 0, pltpu.roll(from_left, lax.rem(C - kt, C), 1), pltpu.roll(v, 1, 1))
                nxt = jnp.where(
                    lane == C - 1, pltpu.roll(from_right, lax.rem(2 * C - 2 - kt, C), 1), pltpu.roll(v, C - 1, 1)
                )
                res.append(base[q : q + 8, :] + (NU_H - sy) * nxt + (NU_H + sy) * prev)
            new = jnp.concatenate(res, axis=0)
            if last:
                outs[f][j] = new
            else:
                ext[dst][f, p, RLO : RLO + RE, :] = new
            return new

        count = LE - k
        if last:
            @pl.loop(0, count, unroll=UNROLL)
            def _(j):
                values(j)
            return None
        run_levels(k, f, count, values)
        return send_edges(k, f)

    for c in halos:
        c.wait()
    flight = [first(0), first(1)]
    sent = []

    def advance(ks):
        for k in ks:
            for f in range(2):
                for c in flight[f]:
                    c.wait()
                flight[f] = sweep(k, f)

    advance((1, 2))

    c_heat.wait()
    hi, lo = split_bf16(jnp.concatenate([heat[h, hb] for h in range(2) for hb in range(B // 128)], axis=1))
    spread = jnp.dot(jnp.concatenate([hi, lo], axis=0), qt[...], preferred_element_type=F32)
    spread = spread[:L] + spread[L:]
    LT = L // 8
    ehi = zero
    elo = zero
    for i in range(RI):
        ui = spread[:, i * C : (i + 1) * C]
        ucols[i] = ui
        for t in range(LT):
            k = i * LT + t
            turned = pltpu.roll(ui[8 * t : 8 * t + 8, :], (k + 1) % C, 1)
            ehi = jnp.where(lane == k, turned, ehi)
            elo = jnp.where(lane == (k + 1) % C, turned, elo)
    hedge_send[0] = ehi
    hedge_send[1] = elo
    c_he = [
        remote(hedge_send.at[0], hedge_recv.at[0], misc_send_sem.at[2], misc_recv_sem.at[2], (g, x, yn)),
        remote(hedge_send.at[1], hedge_recv.at[1], misc_send_sem.at[3], misc_recv_sem.at[3], (g, x, yp)),
    ]
    advance((3,))
    for c in c_he:
        c.wait()
    from_left = hedge_recv[0]
    from_right = hedge_recv[1]
    even = lane % 2 == 0
    for i in range(RI):
        for t in range(LT):
            k = i * LT + t
            v = ucols[i, 8 * t : 8 * t + 8, :]
            prev = jnp.where(lane == 0, pltpu.roll(from_left, (C - k) % C, 1), pltpu.roll(v, 1, 1))
            nxt = jnp.where(lane == C - 1, pltpu.roll(from_right, (2 * C - 2 - k) % C, 1), pltpu.roll(v, C - 1, 1))
            w = 0.75 * v + 0.25 * jnp.where(even, prev, nxt)
            ucols[i, 8 * t : 8 * t + 8, :] = w
            if i == 0:
                rows_send[0, 8 * t : 8 * t + 8, :] = w
            if i == RI - 1:
                rows_send[1, 8 * t : 8 * t + 8, :] = w
    c_rows = [
        remote(rows_send.at[0], rows_recv.at[0], misc_send_sem.at[4], misc_recv_sem.at[4], (g, xp, y)),
        remote(rows_send.at[1], rows_recv.at[1], misc_send_sem.at[5], misc_recv_sem.at[5], (g, xn, y)),
    ]
    advance(range(4, SWEEPS + 1))
    for c in c_rows:
        c.wait()
    flat = t_out.reshape(L * R, C)
    for i in range(RI):
        v = ucols[i]
        above = rows_recv[1] if i == 0 else ucols[i - 1]
        below = rows_recv[0] if i == RI - 1 else ucols[i + 1]
        flat[pl.ds(2 * i, L, stride=R), :] = flat[pl.ds(2 * i, L, stride=R), :] + HEATING_INTERVAL * (0.75 * v + 0.25 * above)
        flat[pl.ds(2 * i + 1, L, stride=R), :] = flat[pl.ds(2 * i + 1, L, stride=R), :] + HEATING_INTERVAL * (0.75 * v + 0.25 * below)


def hand_on(t_in, m_in, r_in, t_out, m_out, r_out):
    t_out[...] = t_in[...]
    m_out[...] = m_in[...]
    r_out[...] = r_in[...]


def wide_body(n_gx, n_gy, warm, humid, cx, cy, gas, drop, sw, lw, flags, slots):
    L, R, C = warm.shape
    S = slots.shape[0] * slots.shape[1]
    B = flags.shape[0]
    flags = flags.T
    G = gas.shape[0]
    LE = L + M
    T = (R + 2 * M) // 8
    NP = -(-LE // (C // T))
    vmem = pl.BlockSpec(memory_space=pltpu.VMEM)
    smem = pl.BlockSpec(memory_space=pltpu.SMEM)
    t, m, rates = pl.pallas_call(
        functools.partial(wide_kernel, n_gx, n_gy, L, R, C, S, B, G),
        out_shape=(
            jax.ShapeDtypeStruct((L, R, C), F32),
            jax.ShapeDtypeStruct((L, R, C), F32),
            jax.ShapeDtypeStruct((2 * L, B), F32),
        ),
        in_specs=[vmem, vmem, smem, smem] + [vmem] * 6,
        out_specs=(vmem, vmem, vmem),
        scratch_shapes=[
            pltpu.VMEM((2, LE + 2, R + 2 * M + 16, C), F32),
            pltpu.VMEM((2, LE + 2, R + 2 * M + 16, C), F32),
            pltpu.VMEM((SWEEPS, 2, 2, NP, 8, C), F32),
            pltpu.VMEM((SWEEPS, 2, 2, NP, 8, C), F32),
            pltpu.VMEM((S, (R // 2) * C), BF),
            pltpu.VMEM((2, 2 * L, B), F32),
            pltpu.VMEM((2, 2 * L, B), F32),
            pltpu.VMEM((4, G, 128), F32),
            pltpu.VMEM((B // 128, 2 * L, 128), F32),
            pltpu.VMEM((B // 128, 2 * L, 128), F32),
            pltpu.VMEM((B // 128, 2 * L, 128), F32),
            pltpu.VMEM((2, B // 128, L, 128), F32),
            pltpu.VMEM((2, B // 128, L, 128), F32),
            pltpu.VMEM((R // 2, L, C), F32),
            pltpu.VMEM((2, 8, C), F32),
            pltpu.VMEM((2, 8, C), F32),
            pltpu.VMEM((2, L, C), F32),
            pltpu.VMEM((2, L, C), F32),
            pltpu.SemaphoreType.DMA((10,)),
            pltpu.SemaphoreType.DMA((10,)),
            pltpu.SemaphoreType.DMA((SWEEPS, 2, 2)),
            pltpu.SemaphoreType.DMA((SWEEPS, 2, 2)),
            pltpu.SemaphoreType.DMA((6,)),
            pltpu.SemaphoreType.DMA((6,)),
        ],
        compiler_params=pltpu.CompilerParams(collective_id=0, has_side_effects=True),
    )(
        warm, humid, cx, cy, gas[None], drop[None], sw[None], lw[None], flags, slots,
    )
    t, m, rates = pl.pallas_call(
        hand_on,
        out_shape=tuple(jax.ShapeDtypeStruct(a.shape, F32) for a in (t, m, rates)),
        in_specs=[vmem] * 3,
        out_specs=(vmem,) * 3,
    )(t, m, rates)
    return t, m, rates.T


CHUNK = 2
PAD = 8


def pair_kernel(
    n_gx, L, R, C, S, B, G,
    warm_hbm, humid_hbm, cx_hbm, cy_hbm, gas_hbm, drop_hbm, sw_hbm, lw_hbm, flags_hbm, slot_hbm,
    res, heat_out, rates_out,
    fields, small, gpoint, flags_ref, slot_ref,
    loc, buf0, buf1, fin, adv, lines, qt, packed, rad, coef, cloudy, absorber, theta, rates, heat, ucols,
    hedge_send, hedge_recv, rows_send, rows_recv,
    in_sem, pair_sem, lev_send_sem, lev_recv_sem, row_send_sem, row_recv_sem,
    corner_send_sem, corner_recv_sem, misc_send_sem, misc_recv_sem,
):
    g = lax.axis_index("grp")
    x = lax.axis_index("gx")
    y = lax.axis_index("gy")
    og = 1 - g
    oy = 1 - y
    xn, xp = lax.rem(x + 1, n_gx), lax.rem(x + n_gx - 1, n_gx)
    LE = L + M
    RE = R + 2 * M
    RI = R // 2
    NC = M // CHUNK
    bufs = (buf0, buf1)

    barrier = pltpu.get_barrier_semaphore()
    partners = [(g, x, oy), (og, x, 0), (og, x, 1)]
    for gg in (g, og):
        for xx in (xn, xp):
            for yy in range(2):
                partners.append((gg, xx, yy))
    for dev in partners:
        pl.semaphore_signal(barrier, inc=1, device_id=dev, device_id_type=MESH)

    loads = []
    pairs = [(warm_hbm, fields.at[0]), (humid_hbm, fields.at[1]), (slot_hbm, slot_ref)]
    pairs += [(cx_hbm, small.at[0]), (cy_hbm, small.at[1])]
    pairs += [(r, gpoint.at[q]) for q, r in enumerate((gas_hbm, drop_hbm, sw_hbm, lw_hbm))]
    pairs += [(flags_hbm, flags_ref)]
    for n, (src, dst) in enumerate(pairs):
        c = pltpu.make_async_copy(src, dst, in_sem.at[n])
        c.start()
        loads.append(c)

    def remote(src, dst, ss, rs, dev):
        c = pltpu.make_async_remote_copy(
            src_ref=src, dst_ref=dst, send_sem=ss, recv_sem=rs, device_id=dev, device_id_type=MESH
        )
        c.start()
        return c

    def arrived(dst, rs):
        pltpu.make_async_remote_copy(
            src_ref=dst, dst_ref=dst, send_sem=rs, recv_sem=rs, device_id=(g, x, oy), device_id_type=MESH
        ).wait_recv()

    zero = jnp.zeros((8, C), F32)
    edge = jnp.zeros((RE, 8, C), F32)
    for b in bufs:
        for h in range(2):
            b[h, :, 0:PAD, :] = edge
            b[h, :, PAD + LE : PAD + LE + 8, :] = edge

    for n in range(2):
        loads[n].wait()
    for f in range(2):
        flat = fields.at[f].reshape(L * R, C)
        for r in range(R):
            loc[f, r] = flat[pl.ds(r, L, stride=R), :]

    pl.semaphore_wait(barrier, 11)

    own_dst = pl.multiple_of(PAD + M * g, 8)
    lev_src = pl.multiple_of((L - M) * og, 8)
    lev_dst = pl.multiple_of(PAD + L * g, 8)
    pending = []
    pending.append(remote(
        loc.at[oy], buf0.at[y, M : M + R, pl.ds(own_dst, L), :],
        pair_sem.at[0], pair_sem.at[1], (g, x, oy),
    ))

    def row_copies(c):
        out = []
        d1, d0 = CHUNK * c, CHUNK * (c + 1)
        near = 1 if d0 == M else 0
        for f in range(2):
            for side, xx in ((0, xn), (1, xp)):
                s0 = R - d0 if side == 0 else d1
                t0 = M - d0 if side == 0 else M + R + d1
                out.append(remote(
                    loc.at[f, s0 : s0 + CHUNK], buf0.at[y, t0 : t0 + CHUNK, pl.ds(own_dst, L), :],
                    row_send_sem.at[c, side, f], row_recv_sem.at[c, side, y], (g, xx, f),
                ))
                n = CHUNK - near
                s1 = s0 + near if side == 0 else s0
                t1 = t0 + near if side == 0 else t0
                out.append(remote(
                    loc.at[f, s1 : s1 + n, pl.ds(lev_src, M), :],
                    buf0.at[y, t1 : t1 + n, pl.ds(lev_dst, M), :],
                    corner_send_sem.at[c, side, f], corner_recv_sem.at[c, side, y], (og, xx, f),
                ))
        return out

    def rows_arrived(c):
        d1, d0 = CHUNK * c, CHUNK * (c + 1)
        near = 1 if d0 == M else 0
        n = CHUNK - near
        for h in range(2):
            for side in range(2):
                t0 = M - d0 if side == 0 else M + R + d1
                t1 = t0 + near if side == 0 else t0
                arrived(buf0.at[h, t0 : t0 + CHUNK, pl.ds(own_dst, L), :], row_recv_sem.at[c, side, h])
                arrived(buf0.at[h, t1 : t1 + n, pl.ds(lev_dst_in, M), :], corner_recv_sem.at[c, side, h])

    lev_dst_in = pl.multiple_of(PAD + L * og, 8)
    for c in range(NC):
        pending += row_copies(c)

    loads[2].wait()
    half = slot_ref.shape[1]
    slots = slot_ref[...]
    rep = (
        lax.broadcasted_iota(jnp.int32, (half, C), 1) // 2
        == lax.broadcasted_iota(jnp.int32, (half, C), 0)
    ).astype(F32).astype(BF)
    s_hi = (slots // 16).astype(F32).astype(BF)
    s_lo = (slots % 16).astype(F32).astype(BF)
    slot_rep = (
        16.0 * jnp.dot(s_hi, rep, preferred_element_type=F32)
        + jnp.dot(s_lo, rep, preferred_element_type=F32)
    ).astype(jnp.int32)
    s_iota = lax.broadcasted_iota(jnp.int32, (S, C), 0)
    for i in range(RI):
        qt[:, i * C : (i + 1) * C] = jnp.where(s_iota == slot_rep[i : i + 1, :], 1.0, 0.0).astype(BF)
    parts = []
    for i in range(RI):
        col = [loc[f, 2 * i] + loc[f, 2 * i + 1] for f in range(2)]
        hi, lo = split_bf16(0.25 * jnp.concatenate(col, axis=0))
        parts.append(jnp.concatenate([hi, lo], axis=0))
    lhs = jnp.concatenate(parts, axis=1)
    both = lax.dot_general(
        lhs, qt[...], (((1,), (1,)), ((), ())), preferred_element_type=F32
    )
    both = both[: 2 * L] + both[2 * L :]
    for h in range(2):
        packed[h] = both[:, h * B : (h + 1) * B]
    c_packed = remote(packed.at[og], rad.at[g], misc_send_sem.at[0], misc_recv_sem.at[0], (og, x, y))
    for f in range(2):
        pending.append(remote(
            loc.at[f, :, pl.ds(lev_src, M), :], buf0.at[y, M : M + R, pl.ds(lev_dst, M), :],
            lev_send_sem.at[f], lev_recv_sem.at[y], (og, x, f),
        ))
    rad[g] = packed[g]
    buf0[y, M : M + R, pl.ds(own_dst, L), :] = loc[y]

    for n in range(3, len(loads)):
        loads[n].wait()
    for q in range(2):
        lines[q] = jnp.broadcast_to(small[q], (C, 2 * L)).T
    for q in range(2):
        part = 0.5 * lines[q, pl.ds(pl.multiple_of((L - M) * g, 8), LE), :]
        adv[2 * q] = NU_H - part
        adv[2 * q + 1] = NU_H + part
    log2e = 1.0 / math.log(2.0)
    for q, scale in enumerate((-log2e, -log2e, 1.0, 1.0)):
        coef[q] = jnp.broadcast_to(gpoint[q] * scale, (128, G)).T
    for hb in range(B // 128):
        cloudy[hb] = flags_ref[:, hb * 128 : (hb + 1) * 128].astype(F32)

    c_packed.wait()
    for o in range(2):
        mo = rad[o, L : 2 * L, :]
        soft = jnp.maximum(mo, 0.0) + jnp.log1p(jnp.exp(-jnp.abs(mo)))
        for hb in range(B // 128):
            absorber[hb, o * L : (o + 1) * L, :] = soft[:, hb * 128 : (hb + 1) * 128]
            theta[hb, o * L : (o + 1) * L, :] = rad[o, 0:L, hb * 128 : (hb + 1) * 128]

    GB = G // 8
    norm = 4.0 / G
    for hb in range(B // 128):
        for o in range(2):
            def level(l, flux, o=o, hb=hb):
                lg = l + o * L
                a = jnp.broadcast_to(absorber[hb, pl.ds(lg, 1), :], (8, 128))
                c = jnp.broadcast_to(cloudy[hb, pl.ds(lg, 1), :], (8, 128))
                th = 1.0 + 0.1 * theta[hb, pl.ds(lg, 1), :]
                sw = lw = None
                new = []
                for q in range(GB):
                    rows = slice(8 * q, 8 * q + 8)
                    d = 1.0 - jnp.exp2(a * coef[0, rows, :] + c * coef[1, rows, :])
                    s = flux[q] * d
                    w = coef[3, rows, :] * d
                    sw = s if sw is None else sw + s
                    lw = w if lw is None else lw + w
                    new.append(flux[q] - s)
                total = jnp.sum(sw - lw * th, axis=0, keepdims=True) * norm
                rates[o, hb, pl.ds(l, 1), :] = total
                return tuple(new)

            if o == 0:
                flux = tuple(coef[2, 8 * q : 8 * q + 8, :] for q in range(GB))
            flux = lax.fori_loop(0, L, level, flux, unroll=2)
    c_heat = remote(rates.at[og], heat.at[g], misc_send_sem.at[1], misc_recv_sem.at[1], (og, x, y))
    heat[g] = rates[g]
    for o in range(2):
        for hb in range(B // 128):
            rates_out[o * L : (o + 1) * L, hb * 128 : (hb + 1) * 128] = rates[o, hb]

    def stencil(k, i0, n):
        src, dst = bufs[(k - 1) % 2], bufs[k % 2]
        lane = lax.broadcasted_iota(jnp.int32, (n * LE, C), 1)
        span = [src[h, i0 - 1 : i0 + n + 1, PAD : PAD + LE, :] for h in range(2)]
        mid = [v[1 : n + 1].reshape(n * LE, C) for v in span]
        right = [pltpu.roll(v, 1, 1) for v in mid]
        left = [pltpu.roll(v, C - 1, 1) for v in mid]
        for h in range(2):
            prev = jnp.where(lane == 0, right[1 - h], right[h]).reshape(n, LE, C)
            nxt = jnp.where(lane == C - 1, left[1 - h], left[h]).reshape(n, LE, C)
            up = src[h, i0 : i0 + n, PAD - 1 : PAD + LE - 1, :]
            down = src[h, i0 : i0 + n, PAD + 1 : PAD + LE + 1, :]
            new = (
                (1.0 - 4.0 * NU_H - 2.0 * NU_V) * span[h][1 : n + 1]
                + NU_V * (up + down)
                + adv[0][None] * span[h][2 : n + 2]
                + adv[1][None] * span[h][0:n]
                + adv[2][None] * nxt
                + adv[3][None] * prev
            )
            if k == SWEEPS:
                fin[h, i0 - M : i0 - M + n] = new
            else:
                dst[h, i0 : i0 + n, PAD : PAD + LE, :] = new

    def strip(c):
        h = CHUNK * (c + 1)
        for k in range(1, SWEEPS + 1):
            stencil(k, M + k - h, CHUNK)
            stencil(k, M + R - (k - h) - CHUNK, CHUNK)

    arrived(buf0.at[oy, M : M + R, pl.ds(own_dst, L), :], pair_sem.at[1])
    for h in range(2):
        arrived(buf0.at[h, M : M + R, pl.ds(lev_dst_in, M), :], lev_recv_sem.at[h])
    for k in range(1, SWEEPS):
        i0, i1 = M + k, M + R - k
        while i0 < i1:
            n = min(2, i1 - i0)
            stencil(k, i0, n)
            i0 += n

    c_heat.wait()
    hi, lo = split_bf16(jnp.concatenate([heat[h, hb] for h in range(2) for hb in range(B // 128)], axis=1))
    spread = jnp.dot(jnp.concatenate([hi, lo], axis=0), qt[...], preferred_element_type=F32)
    spread = spread[:L] + spread[L:]
    lane = lax.broadcasted_iota(jnp.int32, (8, C), 1)
    LT = L // 8
    ehi = zero
    elo = zero
    for i in range(RI):
        ui = spread[:, i * C : (i + 1) * C]
        ucols[i] = ui
        for t in range(LT):
            k = i * LT + t
            turned = pltpu.roll(ui[8 * t : 8 * t + 8, :], (k + 1) % C, 1)
            ehi = jnp.where(lane == k, turned, ehi)
            elo = jnp.where(lane == (k + 1) % C, turned, elo)
    hedge_send[0] = ehi
    hedge_send[1] = elo
    c_he = [
        remote(hedge_send.at[n], hedge_recv.at[n], misc_send_sem.at[2 + n], misc_recv_sem.at[2 + n], (g, x, oy))
        for n in range(2)
    ]

    rows_arrived(0)
    strip(0)

    for c in c_he:
        c.wait()
    from_left = hedge_recv[0]
    from_right = hedge_recv[1]
    even = lane % 2 == 0
    for i in range(RI):
        for t in range(LT):
            k = i * LT + t
            v = ucols[i, 8 * t : 8 * t + 8, :]
            prev = jnp.where(lane == 0, pltpu.roll(from_left, (C - k) % C, 1), pltpu.roll(v, 1, 1))
            nxt = jnp.where(lane == C - 1, pltpu.roll(from_right, (2 * C - 2 - k) % C, 1), pltpu.roll(v, C - 1, 1))
            w = 0.75 * v + 0.25 * jnp.where(even, prev, nxt)
            ucols[i, 8 * t : 8 * t + 8, :] = w
            if i == 0:
                rows_send[0, 8 * t : 8 * t + 8, :] = w
            if i == RI - 1:
                rows_send[1, 8 * t : 8 * t + 8, :] = w
    c_rows = [
        remote(rows_send.at[0], rows_recv.at[0], misc_send_sem.at[4], misc_recv_sem.at[4], (g, xp, y)),
        remote(rows_send.at[1], rows_recv.at[1], misc_send_sem.at[5], misc_recv_sem.at[5], (g, xn, y)),
    ]

    for c in range(1, NC):
        rows_arrived(c)
        strip(c)

    mine = pl.multiple_of(M * g, 8)
    c_fin = remote(
        fin.at[oy, :, pl.ds(mine, L), :], res.at[y], pair_sem.at[2], pair_sem.at[3], (g, x, oy)
    )
    res[y] = fin[y, :, pl.ds(mine, L), :]
    for c in c_rows:
        c.wait()
    for i in range(RI):
        v = ucols[i]
        above = rows_recv[1] if i == 0 else ucols[i - 1]
        below = rows_recv[0] if i == RI - 1 else ucols[i + 1]
        heat_out[2 * i] = HEATING_INTERVAL * (0.75 * v + 0.25 * above)
        heat_out[2 * i + 1] = HEATING_INTERVAL * (0.75 * v + 0.25 * below)
    for c in pending:
        c.wait_send()
    c_fin.wait_send()
    arrived(res.at[oy], pair_sem.at[3])


def settle(res, heat, r_in, t_out, m_out, r_out):
    L, R, C = t_out.shape
    t_flat = t_out.reshape(L * R, C)
    m_flat = m_out.reshape(L * R, C)
    for r in range(R):
        t_flat[pl.ds(r, L, stride=R), :] = res[0, r] + heat[r]
        m_flat[pl.ds(r, L, stride=R), :] = res[1, r]
    r_out[...] = r_in[...]


def pair_body(n_gx, n_gy, warm, humid, cx, cy, gas, drop, sw, lw, flags, slots):
    L, R, C = warm.shape
    S = slots.shape[0] * slots.shape[1]
    B = flags.shape[0]
    flags = flags.T
    G = gas.shape[0]
    LE = L + M
    LP = PAD + LE + 8
    RE = R + 2 * M
    NC = M // CHUNK
    vmem = pl.BlockSpec(memory_space=pltpu.VMEM)
    hbm = pl.BlockSpec(memory_space=pltpu.HBM)
    res, heat, rates = pl.pallas_call(
        functools.partial(pair_kernel, n_gx, L, R, C, S, B, G),
        out_shape=(
            jax.ShapeDtypeStruct((2, R, L, C), F32),
            jax.ShapeDtypeStruct((R, L, C), F32),
            jax.ShapeDtypeStruct((2 * L, B), F32),
        ),
        in_specs=[hbm] * 10,
        out_specs=(vmem, vmem, vmem),
        scratch_shapes=[
            pltpu.VMEM((2, L, R, C), F32),
            pltpu.VMEM((2, 1, 2 * L), F32),
            pltpu.VMEM((4, 1, G), F32),
            pltpu.VMEM((2 * L, B), jnp.int32),
            pltpu.VMEM(slots.shape, jnp.int32),
            pltpu.VMEM((2, R, L, C), F32),
            pltpu.VMEM((2, RE, LP, C), F32),
            pltpu.VMEM((2, RE, LP, C), F32),
            pltpu.VMEM((2, R, LE, C), F32),
            pltpu.VMEM((4, LE, C), F32),
            pltpu.VMEM((2, 2 * L, C), F32),
            pltpu.VMEM((S, (R // 2) * C), BF),
            pltpu.VMEM((2, 2 * L, B), F32),
            pltpu.VMEM((2, 2 * L, B), F32),
            pltpu.VMEM((4, G, 128), F32),
            pltpu.VMEM((B // 128, 2 * L, 128), F32),
            pltpu.VMEM((B // 128, 2 * L, 128), F32),
            pltpu.VMEM((B // 128, 2 * L, 128), F32),
            pltpu.VMEM((2, B // 128, L, 128), F32),
            pltpu.VMEM((2, B // 128, L, 128), F32),
            pltpu.VMEM((R // 2, L, C), F32),
            pltpu.VMEM((2, 8, C), F32),
            pltpu.VMEM((2, 8, C), F32),
            pltpu.VMEM((2, L, C), F32),
            pltpu.VMEM((2, L, C), F32),
            pltpu.SemaphoreType.DMA((10,)),
            pltpu.SemaphoreType.DMA((4,)),
            pltpu.SemaphoreType.DMA((2,)),
            pltpu.SemaphoreType.DMA((2,)),
            pltpu.SemaphoreType.DMA((NC, 2, 2)),
            pltpu.SemaphoreType.DMA((NC, 2, 2)),
            pltpu.SemaphoreType.DMA((NC, 2, 2)),
            pltpu.SemaphoreType.DMA((NC, 2, 2)),
            pltpu.SemaphoreType.DMA((6,)),
            pltpu.SemaphoreType.DMA((6,)),
        ],
        compiler_params=pltpu.CompilerParams(
            collective_id=0, has_side_effects=True, vmem_limit_bytes=32 * 1024 * 1024
        ),
    )(*(
        pltpu.with_memory_space_constraint(a, pltpu.HBM)
        for a in (warm, humid, cx[None], cy[None], gas[None], drop[None], sw[None], lw[None], flags, slots)
    ))
    t, m, rates = pl.pallas_call(
        settle,
        out_shape=(
            jax.ShapeDtypeStruct((L, R, C), F32),
            jax.ShapeDtypeStruct((L, R, C), F32),
            jax.ShapeDtypeStruct((2 * L, B), F32),
        ),
        in_specs=[vmem] * 3,
        out_specs=(vmem,) * 3,
        compiler_params=pltpu.CompilerParams(vmem_limit_bytes=8 * 1024 * 1024),
    )(res, heat, rates)
    return t, m, rates.T


def solution(mesh):
    assert mesh.shape["grp"] == 2
    in_specs = (
        P("grp", "gx", "gy"), P("grp", "gx", "gy"), P(), P(), P(), P(), P(), P(),
        P(("grp", "gx", "gy"), None), P("gx", "gy"),
    )
    out_specs = (P("grp", "gx", "gy"), P("grp", "gx", "gy"), P(("grp", "gx", "gy"), None))
    paired = mesh.shape["gy"] == 2 and mesh.shape["gx"] > 2
    return jax.shard_map(
        functools.partial(pair_body if paired else wide_body, mesh.shape["gx"], mesh.shape["gy"]),
        mesh=mesh, in_specs=in_specs, out_specs=out_specs, check_vma=False,
    )
```

```python
import functools
import math

import jax
import jax.numpy as jnp
from jax import lax
from jax.experimental import pallas as pl
from jax.experimental.pallas import tpu as pltpu
from jax.sharding import PartitionSpec as P

SWEEPS = 8
NU_H = 0.15
NU_V = 0.15
HEATING_INTERVAL = 0.5
UNROLL = 8
M = 8
MESH = pl.DeviceIdType.MESH
BF = jnp.bfloat16
F32 = jnp.float32


def split_bf16(x):
    hi = x.astype(BF)
    lo = (x - hi.astype(F32)).astype(BF)
    return hi, lo


def wide_kernel(
    n_gx, n_gy, L, R, C, S, B, G,
    warm_in, humid_in, cx_ref, cy_ref, gas_ref, drop_ref, sw_ref, lw_ref, flags_ref, slot_ref,
    t_out, m_out, rates_out,
    ext0, ext1, edge_send, edge_recv, qt, packed, rad, coef, cloudy, absorber, theta, rates, heat, ucols,
    hedge_send, hedge_recv, rows_send, rows_recv,
    halo_send_sem, halo_recv_sem, edge_send_sem, edge_recv_sem, misc_send_sem, misc_recv_sem,
):
    g = lax.axis_index("grp")
    x = lax.axis_index("gx")
    y = lax.axis_index("gy")
    og = 1 - g
    xn, xp = lax.rem(x + 1, n_gx), lax.rem(x + n_gx - 1, n_gx)
    yn, yp = lax.rem(y + 1, n_gy), lax.rem(y + n_gy - 1, n_gy)
    fields = (warm_in, humid_in)
    ext = (ext0, ext1)
    outs = (t_out, m_out)
    LE = L + M
    T = (R + 2 * M) // 8
    per = C // T
    NP = -(-LE // per)
    RI = R // 2
    RLO = 8
    ROWN = RLO + M
    RE = R + 2 * M

    barrier = pltpu.get_barrier_semaphore()
    for dev in ((g, xn, y), (g, xp, y), (og, x, y), (og, xn, y), (og, xp, y), (g, x, yn), (g, x, yp)):
        pl.semaphore_signal(barrier, inc=1, device_id=dev, device_id_type=MESH)
    pl.semaphore_wait(barrier, 7)

    def remote(src, dst, ss, rs, dev):
        c = pltpu.make_async_remote_copy(
            src_ref=src, dst_ref=dst, send_sem=ss, recv_sem=rs, device_id=dev, device_id_type=MESH
        )
        c.start()
        return c

    half = slot_ref.shape[1]
    slots = slot_ref[...]
    rep = (
        lax.broadcasted_iota(jnp.int32, (half, C), 1) // 2
        == lax.broadcasted_iota(jnp.int32, (half, C), 0)
    ).astype(F32).astype(BF)
    s_hi = (slots // 16).astype(F32).astype(BF)
    s_lo = (slots % 16).astype(F32).astype(BF)
    slot_rep = (
        16.0 * jnp.dot(s_hi, rep, preferred_element_type=F32)
        + jnp.dot(s_lo, rep, preferred_element_type=F32)
    ).astype(jnp.int32)
    s_iota = lax.broadcasted_iota(jnp.int32, (S, C), 0)
    for i in range(RI):
        qt[:, i * C : (i + 1) * C] = jnp.where(s_iota == slot_rep[i : i + 1, :], 1.0, 0.0).astype(BF)
    parts = []
    for i in range(RI):
        col = []
        for f in range(2):
            flat = fields[f].reshape(L * R, C)
            col.append(
                flat[pl.ds(2 * i, L, stride=R), :] + flat[pl.ds(2 * i + 1, L, stride=R), :]
            )
        hi, lo = split_bf16(0.25 * jnp.concatenate(col, axis=0))
        parts.append(jnp.concatenate([hi, lo], axis=0))
    lhs = jnp.concatenate(parts, axis=1)
    both = lax.dot_general(
        lhs, qt[...], (((1,), (1,)), ((), ())), preferred_element_type=F32
    )
    both = both[: 2 * L] + both[2 * L :]
    for h in range(2):
        packed[h] = both[:, h * B : (h + 1) * B]
    c_packed = remote(packed.at[og], rad.at[g], misc_send_sem.at[0], misc_recv_sem.at[0], (og, x, y))

    lev_src = (L - M) * og
    lev_dst = 1 + L * g
    own_dst = 1 + M * g
    halos = []
    n = 0
    for f in range(2):
        for levs, dlevs, count, gg in ((0, own_dst, L, g), (lev_src, lev_dst, M, og)):
            for r0, d0, xx in ((R - M, RLO, xn), (0, ROWN + R, xp)):
                halos.append(remote(
                    fields[f].at[pl.ds(levs, count), r0 : r0 + M, :],
                    ext0.at[f, pl.ds(dlevs, count), d0 : d0 + M, :],
                    halo_send_sem.at[n], halo_recv_sem.at[n], (gg, xx, y),
                ))
                n += 1
        halos.append(remote(
            fields[f].at[pl.ds(lev_src, M)],
            ext0.at[f, pl.ds(lev_dst, M), ROWN : ROWN + R, :],
            halo_send_sem.at[n], halo_recv_sem.at[n], (og, x, y),
        ))
        n += 1
    rad[g] = packed[g]
    for f in range(2):
        ext0[f, pl.ds(own_dst, L), ROWN : ROWN + R, :] = fields[f][...]
        for b in range(2):
            for p in (0, LE + 1):
                ext[b][f, p] = jnp.zeros((RE + 16, C), F32)

    log2e = 1.0 / math.log(2.0)
    for q, (ref, scale) in enumerate(((gas_ref, -log2e), (drop_ref, -log2e), (sw_ref, 1.0), (lw_ref, 1.0))):
        coef[q] = jnp.broadcast_to(ref[...] * scale, (128, G)).T
    for hb in range(B // 128):
        cloudy[hb] = flags_ref[:, hb * 128 : (hb + 1) * 128].astype(F32)

    c_packed.wait()
    for o in range(2):
        mo = rad[o, L : 2 * L, :]
        soft = jnp.maximum(mo, 0.0) + jnp.log1p(jnp.exp(-jnp.abs(mo)))
        for hb in range(B // 128):
            absorber[hb, o * L : (o + 1) * L, :] = soft[:, hb * 128 : (hb + 1) * 128]
            theta[hb, o * L : (o + 1) * L, :] = rad[o, 0:L, hb * 128 : (hb + 1) * 128]

    GB = G // 8
    norm = 4.0 / G
    for hb in range(B // 128):
        for o in range(2):
            def level(l, flux, o=o, hb=hb):
                lg = l + o * L
                a = jnp.broadcast_to(absorber[hb, pl.ds(lg, 1), :], (8, 128))
                c = jnp.broadcast_to(cloudy[hb, pl.ds(lg, 1), :], (8, 128))
                th = 1.0 + 0.1 * theta[hb, pl.ds(lg, 1), :]
                sw = lw = None
                new = []
                for q in range(GB):
                    rows = slice(8 * q, 8 * q + 8)
                    d = 1.0 - jnp.exp2(a * coef[0, rows, :] + c * coef[1, rows, :])
                    s = flux[q] * d
                    w = coef[3, rows, :] * d
                    sw = s if sw is None else sw + s
                    lw = w if lw is None else lw + w
                    new.append(flux[q] - s)
                total = jnp.sum(sw - lw * th, axis=0, keepdims=True) * norm
                rates[o, hb, pl.ds(l, 1), :] = total
                return tuple(new)

            if o == 0:
                flux = tuple(coef[2, 8 * q : 8 * q + 8, :] for q in range(GB))
            flux = lax.fori_loop(0, L, level, flux, unroll=2)
    c_heat = remote(rates.at[og], heat.at[g], misc_send_sem.at[1], misc_recv_sem.at[1], (og, x, y))
    heat[g] = rates[g]
    for o in range(2):
        for hb in range(B // 128):
            rates_out[o * L : (o + 1) * L, hb * 128 : (hb + 1) * 128] = rates[o, hb]

    lane = lax.broadcasted_iota(jnp.int32, (8, C), 1)

    def pack(vals, j, accs):
        right, left = accs
        for t in range(T):
            k = j * T + t
            turned = pltpu.roll(vals[8 * t : 8 * t + 8, :], lax.rem(k + 1, C), 1)
            right = jnp.where(lane == k, turned, right)
            left = jnp.where(lane == lax.rem(k + 1, C), turned, left)
        return right, left

    def send_edges(k, f):
        return (
            remote(edge_send.at[k, f, 0], edge_recv.at[k, f, 0],
                   edge_send_sem.at[k, f, 0], edge_recv_sem.at[k, f, 0], (g, x, yn)),
            remote(edge_send.at[k, f, 1], edge_recv.at[k, f, 1],
                   edge_send_sem.at[k, f, 1], edge_recv_sem.at[k, f, 1], (g, x, yp)),
        )

    zero = jnp.zeros((8, C), F32)

    def run_levels(k, f, count, values):
        for p in range(NP):
            lo, hi = p * per, min(count, (p + 1) * per)
            if lo >= hi:
                edge_send[k, f, 0, p] = zero
                edge_send[k, f, 1, p] = zero
                continue
            right, left = lax.fori_loop(
                lo, hi, lambda j, accs, lo=lo: pack(values(j), j - lo, accs), (zero, zero),
                unroll=min(UNROLL, hi - lo),
            )
            edge_send[k, f, 0, p] = right
            edge_send[k, f, 1, p] = left

    def first(f):
        run_levels(0, f, LE, lambda j: ext0[f, j + 1, RLO : RLO + RE, :])
        return send_edges(0, f)

    def sweep(k, f):
        src, dst = (k - 1) % 2, k % 2
        start = g * k
        last = k == SWEEPS
        t0, t1 = (M // 8, M // 8 + R // 8) if last else (0, T)
        r0, r1 = RLO + 8 * t0, RLO + 8 * t1

        def values(j):
            lev = start + j
            p = lev + 1
            jj = j + g
            which = jj // per
            kk = (jj - which * per) * T
            from_left = edge_recv[k - 1, f, 0, which]
            from_right = edge_recv[k - 1, f, 1, which]
            lg = lev + (L - M) * g
            sx = 0.5 * cx_ref[lg]
            sy = 0.5 * cy_ref[lg]
            cen = ext[src][f, p, r0:r1, :]
            base = (
                (1.0 - 4.0 * NU_H - 2.0 * NU_V) * cen
                + NU_V * (ext[src][f, p + 1, r0:r1, :] + ext[src][f, p - 1, r0:r1, :])
                + (NU_H - sx) * ext[src][f, p, r0 + 1 : r1 + 1, :]
                + (NU_H + sx) * ext[src][f, p, r0 - 1 : r1 - 1, :]
            )
            res = []
            for t in range(t0, t1):
                q = 8 * (t - t0)
                v = cen[q : q + 8, :]
                kt = kk + t
                prev = jnp.where(lane == 0, pltpu.roll(from_left, lax.rem(C - kt, C), 1), pltpu.roll(v, 1, 1))
                nxt = jnp.where(
                    lane == C - 1, pltpu.roll(from_right, lax.rem(2 * C - 2 - kt, C), 1), pltpu.roll(v, C - 1, 1)
                )
                res.append(base[q : q + 8, :] + (NU_H - sy) * nxt + (NU_H + sy) * prev)
            new = jnp.concatenate(res, axis=0)
            if last:
                outs[f][j] = new
            else:
                ext[dst][f, p, RLO : RLO + RE, :] = new
            return new

        count = LE - k
        if last:
            @pl.loop(0, count, unroll=UNROLL)
            def _(j):
                values(j)
            return None
        run_levels(k, f, count, values)
        return send_edges(k, f)

    for c in halos:
        c.wait()
    flight = [first(0), first(1)]
    sent = []

    def advance(ks):
        for k in ks:
            for f in range(2):
                for c in flight[f]:
                    c.wait()
                flight[f] = sweep(k, f)

    advance((1, 2))

    c_heat.wait()
    hi, lo = split_bf16(jnp.concatenate([heat[h, hb] for h in range(2) for hb in range(B // 128)], axis=1))
    spread = jnp.dot(jnp.concatenate([hi, lo], axis=0), qt[...], preferred_element_type=F32)
    spread = spread[:L] + spread[L:]
    LT = L // 8
    ehi = zero
    elo = zero
    for i in range(RI):
        ui = spread[:, i * C : (i + 1) * C]
        ucols[i] = ui
        for t in range(LT):
            k = i * LT + t
            turned = pltpu.roll(ui[8 * t : 8 * t + 8, :], (k + 1) % C, 1)
            ehi = jnp.where(lane == k, turned, ehi)
            elo = jnp.where(lane == (k + 1) % C, turned, elo)
    hedge_send[0] = ehi
    hedge_send[1] = elo
    c_he = [
        remote(hedge_send.at[0], hedge_recv.at[0], misc_send_sem.at[2], misc_recv_sem.at[2], (g, x, yn)),
        remote(hedge_send.at[1], hedge_recv.at[1], misc_send_sem.at[3], misc_recv_sem.at[3], (g, x, yp)),
    ]
    advance((3,))
    for c in c_he:
        c.wait()
    from_left = hedge_recv[0]
    from_right = hedge_recv[1]
    even = lane % 2 == 0
    for i in range(RI):
        for t in range(LT):
            k = i * LT + t
            v = ucols[i, 8 * t : 8 * t + 8, :]
            prev = jnp.where(lane == 0, pltpu.roll(from_left, (C - k) % C, 1), pltpu.roll(v, 1, 1))
            nxt = jnp.where(lane == C - 1, pltpu.roll(from_right, (2 * C - 2 - k) % C, 1), pltpu.roll(v, C - 1, 1))
            w = 0.75 * v + 0.25 * jnp.where(even, prev, nxt)
            ucols[i, 8 * t : 8 * t + 8, :] = w
            if i == 0:
                rows_send[0, 8 * t : 8 * t + 8, :] = w
            if i == RI - 1:
                rows_send[1, 8 * t : 8 * t + 8, :] = w
    c_rows = [
        remote(rows_send.at[0], rows_recv.at[0], misc_send_sem.at[4], misc_recv_sem.at[4], (g, xp, y)),
        remote(rows_send.at[1], rows_recv.at[1], misc_send_sem.at[5], misc_recv_sem.at[5], (g, xn, y)),
    ]
    advance(range(4, SWEEPS + 1))
    for c in c_rows:
        c.wait()
    flat = t_out.reshape(L * R, C)
    for i in range(RI):
        v = ucols[i]
        above = rows_recv[1] if i == 0 else ucols[i - 1]
        below = rows_recv[0] if i == RI - 1 else ucols[i + 1]
        flat[pl.ds(2 * i, L, stride=R), :] = flat[pl.ds(2 * i, L, stride=R), :] + HEATING_INTERVAL * (0.75 * v + 0.25 * above)
        flat[pl.ds(2 * i + 1, L, stride=R), :] = flat[pl.ds(2 * i + 1, L, stride=R), :] + HEATING_INTERVAL * (0.75 * v + 0.25 * below)


def hand_on(t_in, m_in, r_in, t_out, m_out, r_out):
    t_out[...] = t_in[...]
    m_out[...] = m_in[...]
    r_out[...] = r_in[...]


def wide_body(n_gx, n_gy, warm, humid, cx, cy, gas, drop, sw, lw, flags, slots):
    L, R, C = warm.shape
    S = slots.shape[0] * slots.shape[1]
    B = flags.shape[0]
    flags = flags.T
    G = gas.shape[0]
    LE = L + M
    T = (R + 2 * M) // 8
    NP = -(-LE // (C // T))
    vmem = pl.BlockSpec(memory_space=pltpu.VMEM)
    smem = pl.BlockSpec(memory_space=pltpu.SMEM)
    t, m, rates = pl.pallas_call(
        functools.partial(wide_kernel, n_gx, n_gy, L, R, C, S, B, G),
        out_shape=(
            jax.ShapeDtypeStruct((L, R, C), F32),
            jax.ShapeDtypeStruct((L, R, C), F32),
            jax.ShapeDtypeStruct((2 * L, B), F32),
        ),
        in_specs=[vmem, vmem, smem, smem] + [vmem] * 6,
        out_specs=(vmem, vmem, vmem),
        scratch_shapes=[
            pltpu.VMEM((2, LE + 2, R + 2 * M + 16, C), F32),
            pltpu.VMEM((2, LE + 2, R + 2 * M + 16, C), F32),
            pltpu.VMEM((SWEEPS, 2, 2, NP, 8, C), F32),
            pltpu.VMEM((SWEEPS, 2, 2, NP, 8, C), F32),
            pltpu.VMEM((S, (R // 2) * C), BF),
            pltpu.VMEM((2, 2 * L, B), F32),
            pltpu.VMEM((2, 2 * L, B), F32),
            pltpu.VMEM((4, G, 128), F32),
            pltpu.VMEM((B // 128, 2 * L, 128), F32),
            pltpu.VMEM((B // 128, 2 * L, 128), F32),
            pltpu.VMEM((B // 128, 2 * L, 128), F32),
            pltpu.VMEM((2, B // 128, L, 128), F32),
            pltpu.VMEM((2, B // 128, L, 128), F32),
            pltpu.VMEM((R // 2, L, C), F32),
            pltpu.VMEM((2, 8, C), F32),
            pltpu.VMEM((2, 8, C), F32),
            pltpu.VMEM((2, L, C), F32),
            pltpu.VMEM((2, L, C), F32),
            pltpu.SemaphoreType.DMA((10,)),
            pltpu.SemaphoreType.DMA((10,)),
            pltpu.SemaphoreType.DMA((SWEEPS, 2, 2)),
            pltpu.SemaphoreType.DMA((SWEEPS, 2, 2)),
            pltpu.SemaphoreType.DMA((6,)),
            pltpu.SemaphoreType.DMA((6,)),
        ],
        compiler_params=pltpu.CompilerParams(collective_id=0, has_side_effects=True),
    )(
        warm, humid, cx, cy, gas[None], drop[None], sw[None], lw[None], flags, slots,
    )
    t, m, rates = pl.pallas_call(
        hand_on,
        out_shape=tuple(jax.ShapeDtypeStruct(a.shape, F32) for a in (t, m, rates)),
        in_specs=[vmem] * 3,
        out_specs=(vmem,) * 3,
    )(t, m, rates)
    return t, m, rates.T


CHUNK = 4
PAD = 8


def pair_kernel(
    n_gx, L, R, C, S, B, G,
    warm_hbm, humid_hbm, cx_hbm, cy_hbm, gas_hbm, drop_hbm, sw_hbm, lw_hbm, flags_hbm, slot_hbm,
    res, heat_out, rates_out,
    fields, small, gpoint, flags_ref, slot_ref,
    loc, buf0, buf1, fin, adv, lines, qt, packed, rad, coef, cloudy, absorber, theta, passed, rates, heat, ucols, corner_send, corner_recv,
    in_sem, pair_sem, lev_sem, row_send_sem, row_recv_sem, corner_sem, misc_sem,
):
    g = lax.axis_index("grp")
    x = lax.axis_index("gx")
    y = lax.axis_index("gy")
    og = 1 - g
    oy = 1 - y
    xn, xp = lax.rem(x + 1, n_gx), lax.rem(x + n_gx - 1, n_gx)
    LE = L + M
    RE = R + 2 * M
    RI = R // 2
    NC = M // CHUNK
    bufs = (buf0, buf1)

    sub = lax.broadcasted_iota(jnp.int32, (M, C), 0)
    barrier = pltpu.get_barrier_semaphore()
    partners = [(g, x, oy), (og, x, 0), (og, x, 1)]
    for gg in (g, og):
        for xx in (xn, xp):
            for yy in range(2):
                partners.append((gg, xx, yy))
    for dev in partners:
        pl.semaphore_signal(barrier, inc=1, device_id=dev, device_id_type=MESH)

    loads = []
    pairs = [(slot_hbm, slot_ref), (warm_hbm, fields.at[0]), (humid_hbm, fields.at[1])]
    pairs += [(cx_hbm, small.at[0]), (cy_hbm, small.at[1])]
    pairs += [(r, gpoint.at[q]) for q, r in enumerate((gas_hbm, drop_hbm, sw_hbm, lw_hbm))]
    pairs += [(flags_hbm, flags_ref)]
    for n, (src, dst) in enumerate(pairs):
        c = pltpu.make_async_copy(src, dst, in_sem.at[n])
        c.start()
        loads.append(c)

    def remote(src, dst, ss, rs, dev):
        c = pltpu.make_async_remote_copy(
            src_ref=src, dst_ref=dst, send_sem=ss, recv_sem=rs, device_id=dev, device_id_type=MESH
        )
        c.start()
        return c

    def matching(ref, sem):
        return pltpu.make_async_remote_copy(
            src_ref=ref, dst_ref=ref, send_sem=sem, recv_sem=sem, device_id=(g, x, oy), device_id_type=MESH
        )

    def arrived(ref, sem):
        matching(ref, sem).wait_recv()

    def left(ref, sem):
        matching(ref, sem).wait_send()

    edge = jnp.zeros((RE, 8, C), F32)
    for b in bufs:
        for h in range(2):
            b[h, :, 0:PAD, :] = edge
            b[h, :, PAD + LE : PAD + LE + 8, :] = edge

    loads[0].wait()
    half = slot_ref.shape[1]
    slots = slot_ref[...]
    rep = (
        lax.broadcasted_iota(jnp.int32, (half, C), 1) // 2
        == lax.broadcasted_iota(jnp.int32, (half, C), 0)
    ).astype(F32).astype(BF)
    s_hi = (slots // 16).astype(F32).astype(BF)
    s_lo = (slots % 16).astype(F32).astype(BF)
    slot_rep = (
        16.0 * jnp.dot(s_hi, rep, preferred_element_type=F32)
        + jnp.dot(s_lo, rep, preferred_element_type=F32)
    ).astype(jnp.int32)
    s_iota = lax.broadcasted_iota(jnp.int32, (S, C), 0)
    for i in range(RI):
        qt[:, i * C : (i + 1) * C] = jnp.where(s_iota == slot_rep[i : i + 1, :], 1.0, 0.0).astype(BF)
    for n in range(1, 3):
        loads[n].wait()
    for f in range(2):
        flat = fields.at[f].reshape(L * R, C)
        for r in range(R):
            loc[f, r] = flat[pl.ds(r, L, stride=R), :]

    pl.semaphore_wait(barrier, 11)

    own_dst = pl.multiple_of(PAD + M * g, 8)
    lev_src = pl.multiple_of((L - M) * og, 8)
    lev_own = pl.multiple_of(PAD + M * g + (L - M) * og, 8)
    lev_dst = pl.multiple_of(PAD + L * g, 8)
    lev_in = pl.multiple_of(PAD + L * og, 8)

    lead = jnp.where(x == n_gx - 1, 0, 1)
    for turn in range(2):
        side = lead if turn == 0 else 1 - lead
        up = side == 0
        xx = jnp.where(up, xn, xp)
        for c in range(NC):
            d1, d0 = CHUNK * c, CHUNK * (c + 1)
            s0 = jnp.where(up, R - d0, d1)
            t0 = jnp.where(up, M - d0, M + R + d1)
            for f in range(2):
                remote(
                    loc.at[f, pl.ds(s0, CHUNK)], buf0.at[y, pl.ds(t0, CHUNK), pl.ds(own_dst, L), :],
                    row_send_sem.at[0], row_recv_sem.at[c], (g, xx, f),
                )

    remote(
        loc.at[oy], buf0.at[y, M : M + R, pl.ds(own_dst, L), :], pair_sem.at[0], pair_sem.at[1], (g, x, oy)
    )
    parts = []
    for i in range(RI):
        col = [loc[f, 2 * i] + loc[f, 2 * i + 1] for f in range(2)]
        hi, lo = split_bf16(0.25 * jnp.concatenate(col, axis=0))
        parts.append(jnp.concatenate([hi, lo], axis=0))
    lhs = jnp.concatenate(parts, axis=1)
    both = lax.dot_general(
        lhs, qt[...], (((1,), (1,)), ((), ())), preferred_element_type=F32
    )
    both = both[: 2 * L] + both[2 * L :]
    for h in range(2):
        packed[h] = both[:, h * B : (h + 1) * B]
    c_packed = remote(packed.at[og], rad.at[g], misc_sem.at[0], misc_sem.at[1], (og, x, y))
    for f in range(2):
        for side in range(2):
            for j in range(M // 2):
                d = j + 1
                near, far = (R - d, R - M + d) if side == 0 else (d - 1, M - d - 1)
                a = loc[f, near, pl.ds(lev_src, M), :]
                b = loc[f, far, pl.ds(lev_src, M), :]
                above = jnp.where(sub >= d, a, pltpu.roll(b, d, 0))
                below = jnp.where(sub < M - d, a, pltpu.roll(b, M - d, 0))
                corner_send[f, side, j] = jnp.where(g == 0, above, below)
    for f in range(2):
        for side, xx in ((0, xn), (1, xp)):
            remote(
                corner_send.at[f, side], corner_recv.at[y, side],
                corner_sem.at[0], corner_sem.at[1], (og, xx, f),
            )
    for f in range(2):
        remote(
            loc.at[f, :, pl.ds(lev_src, M), :], buf0.at[y, M : M + R, pl.ds(lev_dst, M), :],
            lev_sem.at[0], lev_sem.at[1], (og, x, f),
        )

    def rows_arrived(c):
        arrived(buf0.at[:, 0 : 2 * CHUNK, pl.ds(own_dst, L), :], row_recv_sem.at[c])

    def corners_arrived():
        arrived(corner_recv, corner_sem.at[1])
        for h in range(2):
            for side in range(2):
                for j in range(M // 2):
                    d = j + 1
                    near, far = (M - d, d) if side == 0 else (M + R + d - 1, R + 2 * M - d - 1)
                    v = corner_recv[h, side, j]
                    buf0[h, near, pl.ds(lev_in, M), :] = v
                    if near != far:
                        back = jnp.where(g == 1, pltpu.roll(v, M - d, 0), pltpu.roll(v, d, 0))
                        buf0[h, far, pl.ds(lev_in, M), :] = back

    rad[g] = packed[g]
    buf0[y, M : M + R, pl.ds(own_dst, L), :] = loc[y]

    for n in range(3, len(loads)):
        loads[n].wait()
    for q in range(2):
        lines[q] = jnp.broadcast_to(small[q], (C, 2 * L)).T
    for q in range(2):
        part = 0.5 * lines[q, pl.ds(pl.multiple_of((L - M) * g, 8), LE), :]
        adv[2 * q] = NU_H - part
        adv[2 * q + 1] = NU_H + part
    log2e = 1.0 / math.log(2.0)
    for q, scale in enumerate((-log2e, -log2e, 1.0, 1.0)):
        coef[q] = jnp.broadcast_to(gpoint[q] * scale, (128, G)).T
    for hb in range(B // 128):
        cloudy[hb] = flags_ref[:, hb * 128 : (hb + 1) * 128].astype(F32)

    GB = G // 8
    HB = B // 128
    norm = 4.0 / G
    c_heat = pltpu.make_async_remote_copy(
        src_ref=rates.at[og], dst_ref=heat.at[g], send_sem=misc_sem.at[2], recv_sem=misc_sem.at[3],
        device_id=(og, x, y), device_id_type=MESH,
    )
    for o in range(2):
        @pl.when(og == o)
        def _():
            c_packed.wait()

        mo = rad[o, L : 2 * L, :]
        soft = jnp.maximum(mo, 0.0) + jnp.log1p(jnp.exp(-jnp.abs(mo)))
        for hb in range(HB):
            absorber[hb, o * L : (o + 1) * L, :] = soft[:, hb * 128 : (hb + 1) * 128]
            theta[hb, o * L : (o + 1) * L, :] = rad[o, 0:L, hb * 128 : (hb + 1) * 128]
        for hb in range(HB):
            def level(l, flux, o=o, hb=hb):
                lg = l + o * L
                a = jnp.broadcast_to(absorber[hb, pl.ds(lg, 1), :], (8, 128))
                c = jnp.broadcast_to(cloudy[hb, pl.ds(lg, 1), :], (8, 128))
                th = 1.0 + 0.1 * theta[hb, pl.ds(lg, 1), :]
                sw = lw = None
                new = []
                for q in range(GB):
                    rows = slice(8 * q, 8 * q + 8)
                    d = 1.0 - jnp.exp2(a * coef[0, rows, :] + c * coef[1, rows, :])
                    s = flux[q] * d
                    w = coef[3, rows, :] * d
                    sw = s if sw is None else sw + s
                    lw = w if lw is None else lw + w
                    new.append(flux[q] - s)
                total = jnp.sum(sw - lw * th, axis=0, keepdims=True) * norm
                rates[o, hb, pl.ds(l, 1), :] = total
                return tuple(new)

            start = coef.at[2] if o == 0 else passed.at[hb]
            flux = tuple(start[8 * q : 8 * q + 8, :] for q in range(GB))
            flux = lax.fori_loop(0, L, level, flux, unroll=2)
            if o == 0:
                for q in range(GB):
                    passed[hb, 8 * q : 8 * q + 8, :] = flux[q]
            rates_out[o * L : (o + 1) * L, hb * 128 : (hb + 1) * 128] = rates[o, hb]

        @pl.when(og == o)
        def _():
            c_heat.start()
    heat[g] = rates[g]

    def stencil(k, i0, n):
        src, dst = bufs[(k - 1) % 2], bufs[k % 2]
        lane = lax.broadcasted_iota(jnp.int32, (n * LE, C), 1)
        span = [src[h, i0 - 1 : i0 + n + 1, PAD : PAD + LE, :] for h in range(2)]
        mid = [v[1 : n + 1].reshape(n * LE, C) for v in span]
        right = [pltpu.roll(v, 1, 1) for v in mid]
        left = [pltpu.roll(v, C - 1, 1) for v in mid]
        for h in range(2):
            prev = jnp.where(lane == 0, right[1 - h], right[h]).reshape(n, LE, C)
            nxt = jnp.where(lane == C - 1, left[1 - h], left[h]).reshape(n, LE, C)
            up = src[h, i0 : i0 + n, PAD - 1 : PAD + LE - 1, :]
            down = src[h, i0 : i0 + n, PAD + 1 : PAD + LE + 1, :]
            new = (
                (1.0 - 4.0 * NU_H - 2.0 * NU_V) * span[h][1 : n + 1]
                + NU_V * (up + down)
                + adv[0][None] * span[h][2 : n + 2]
                + adv[1][None] * span[h][0:n]
                + adv[2][None] * nxt
                + adv[3][None] * prev
            )
            if k == SWEEPS:
                fin[h, i0 - M : i0 - M + n] = new
            else:
                dst[h, i0 : i0 + n, PAD : PAD + LE, :] = new

    def strip(c):
        h = CHUNK * (c + 1)
        for k in range(1, SWEEPS + 1):
            stencil(k, M + k - h, CHUNK)
            stencil(k, M + R - (k - h) - CHUNK, CHUNK)

    arrived(buf0.at[oy, M : M + R, pl.ds(own_dst, L), :], pair_sem.at[1])
    arrived(buf0.at[:, M : M + R, pl.ds(lev_in, M), :], lev_sem.at[1])
    for k in range(1, SWEEPS):
        i0, i1 = M + k, M + R - k
        while i0 < i1:
            n = min(2, i1 - i0)
            stencil(k, i0, n)
            i0 += n

    c_heat.wait()
    hi, lo = split_bf16(jnp.concatenate([heat[h, hb] for h in range(2) for hb in range(B // 128)], axis=1))
    spread = jnp.dot(jnp.concatenate([hi, lo], axis=0), qt[...], preferred_element_type=F32)
    spread = spread[:L] + spread[L:]
    for i in range(RI):
        ucols[y, 1 + i] = spread[:, i * C : (i + 1) * C]
    for i, t, xx in ((1, RI + 1, xp), (RI, 0, xn)):
        for yy in range(2):
            remote(ucols.at[y, i], ucols.at[y, t], misc_sem.at[4], misc_sem.at[5], (g, xx, yy))
    c_cols = remote(
        ucols.at[y, 1 : RI + 1], ucols.at[y, 1 : RI + 1], misc_sem.at[6], misc_sem.at[7], (g, x, oy)
    )

    mine = pl.multiple_of(M * g, 8)
    corners_arrived()
    for c in range(NC):
        rows_arrived(c)
        strip(c)
        h = CHUNK * (c + 1)
        for r in (M - h, R - M + h - CHUNK):
            remote(
                fin.at[oy, r : r + CHUNK, pl.ds(mine, L), :], res.at[y, r : r + CHUNK],
                pair_sem.at[2], pair_sem.at[3], (g, x, oy),
            )
    res[y] = fin[y, :, pl.ds(mine, L), :]

    c_cols.wait()
    arrived(ucols.at[:, 0:2], misc_sem.at[5])
    lane = lax.broadcasted_iota(jnp.int32, (L, C), 1)
    even = lane % 2 == 0
    cols = []
    for i in range(RI + 2):
        v, o = ucols[y, i], ucols[oy, i]
        prev = jnp.where(lane == 0, pltpu.roll(o, 1, 1), pltpu.roll(v, 1, 1))
        nxt = jnp.where(lane == C - 1, pltpu.roll(o, C - 1, 1), pltpu.roll(v, C - 1, 1))
        cols.append(HEATING_INTERVAL * (0.75 * v + 0.25 * jnp.where(even, prev, nxt)))
    for i in range(RI):
        heat_out[2 * i] = 0.75 * cols[i + 1] + 0.25 * cols[i]
        heat_out[2 * i + 1] = 0.75 * cols[i + 1] + 0.25 * cols[i + 2]
    left(buf0.at[:, 0 : 2 * M, 0:L, :], row_send_sem.at[0])
    left(corner_send, corner_sem.at[0])
    left(buf0.at[:, 0:R, 0:M, :], lev_sem.at[0])
    left(loc.at[oy], pair_sem.at[0])
    left(ucols.at[:, 0:2], misc_sem.at[4])
    left(res.at[oy], pair_sem.at[2])
    arrived(res.at[oy], pair_sem.at[3])


def settle(res, heat, r_in, t_out, m_out, r_out):
    L, R, C = t_out.shape
    t_flat = t_out.reshape(L * R, C)
    m_flat = m_out.reshape(L * R, C)
    for r in range(R):
        t_flat[pl.ds(r, L, stride=R), :] = res[0, r] + heat[r]
        m_flat[pl.ds(r, L, stride=R), :] = res[1, r]
    r_out[...] = r_in[...]


def pair_body(n_gx, n_gy, warm, humid, cx, cy, gas, drop, sw, lw, flags, slots):
    L, R, C = warm.shape
    S = slots.shape[0] * slots.shape[1]
    B = flags.shape[0]
    flags = flags.T
    G = gas.shape[0]
    LE = L + M
    LP = PAD + LE + 8
    RE = R + 2 * M
    NC = M // CHUNK
    vmem = pl.BlockSpec(memory_space=pltpu.VMEM)
    hbm = pl.BlockSpec(memory_space=pltpu.HBM)
    res, heat, rates = pl.pallas_call(
        functools.partial(pair_kernel, n_gx, L, R, C, S, B, G),
        out_shape=(
            jax.ShapeDtypeStruct((2, R, L, C), F32),
            jax.ShapeDtypeStruct((R, L, C), F32),
            jax.ShapeDtypeStruct((2 * L, B), F32),
        ),
        in_specs=[hbm] * 10,
        out_specs=(vmem, vmem, vmem),
        scratch_shapes=[
            pltpu.VMEM((2, L, R, C), F32),
            pltpu.VMEM((2, 1, 2 * L), F32),
            pltpu.VMEM((4, 1, G), F32),
            pltpu.VMEM((2 * L, B), jnp.int32),
            pltpu.VMEM(slots.shape, jnp.int32),
            pltpu.VMEM((2, R, L, C), F32),
            pltpu.VMEM((2, RE, LP, C), F32),
            pltpu.VMEM((2, RE, LP, C), F32),
            pltpu.VMEM((2, R, LE, C), F32),
            pltpu.VMEM((4, LE, C), F32),
            pltpu.VMEM((2, 2 * L, C), F32),
            pltpu.VMEM((S, (R // 2) * C), BF),
            pltpu.VMEM((2, 2 * L, B), F32),
            pltpu.VMEM((2, 2 * L, B), F32),
            pltpu.VMEM((4, G, 128), F32),
            pltpu.VMEM((B // 128, 2 * L, 128), F32),
            pltpu.VMEM((B // 128, 2 * L, 128), F32),
            pltpu.VMEM((B // 128, 2 * L, 128), F32),
            pltpu.VMEM((B // 128, G, 128), F32),
            pltpu.VMEM((2, B // 128, L, 128), F32),
            pltpu.VMEM((2, B // 128, L, 128), F32),
            pltpu.VMEM((2, R // 2 + 2, L, C), F32),
            pltpu.VMEM((2, 2, M // 2, M, C), F32),
            pltpu.VMEM((2, 2, M // 2, M, C), F32),
            pltpu.SemaphoreType.DMA((10,)),
            pltpu.SemaphoreType.DMA((4,)),
            pltpu.SemaphoreType.DMA((2,)),
            pltpu.SemaphoreType.DMA((1,)),
            pltpu.SemaphoreType.DMA((NC,)),
            pltpu.SemaphoreType.DMA((2,)),
            pltpu.SemaphoreType.DMA((8,)),
        ],
        compiler_params=pltpu.CompilerParams(
            collective_id=0, has_side_effects=True, vmem_limit_bytes=32 * 1024 * 1024
        ),
    )(*(
        pltpu.with_memory_space_constraint(a, pltpu.HBM)
        for a in (warm, humid, cx[None], cy[None], gas[None], drop[None], sw[None], lw[None], flags, slots)
    ))
    t, m, rates = pl.pallas_call(
        settle,
        out_shape=(
            jax.ShapeDtypeStruct((L, R, C), F32),
            jax.ShapeDtypeStruct((L, R, C), F32),
            jax.ShapeDtypeStruct((2 * L, B), F32),
        ),
        in_specs=[vmem] * 3,
        out_specs=(vmem,) * 3,
        compiler_params=pltpu.CompilerParams(vmem_limit_bytes=8 * 1024 * 1024),
    )(res, heat, rates)
    return t, m, rates.T


def solution(mesh):
    assert mesh.shape["grp"] == 2
    in_specs = (
        P("grp", "gx", "gy"), P("grp", "gx", "gy"), P(), P(), P(), P(), P(), P(),
        P(("grp", "gx", "gy"), None), P("gx", "gy"),
    )
    out_specs = (P("grp", "gx", "gy"), P("grp", "gx", "gy"), P(("grp", "gx", "gy"), None))
    paired = mesh.shape["gy"] == 2 and mesh.shape["gx"] > 2
    return jax.shard_map(
        functools.partial(pair_body if paired else wide_body, mesh.shape["gx"], mesh.shape["gy"]),
        mesh=mesh, in_specs=in_specs, out_specs=out_specs, check_vma=False,
    )
```

```python
import functools
import math

import jax
import jax.numpy as jnp
from jax import lax
from jax.experimental import pallas as pl
from jax.experimental.pallas import tpu as pltpu
from jax.sharding import PartitionSpec as P

SWEEPS = 8
NU_H = 0.15
NU_V = 0.15
HEATING_INTERVAL = 0.5
UNROLL = 8
M = 8
MESH = pl.DeviceIdType.MESH
BF = jnp.bfloat16
F32 = jnp.float32


def split_bf16(x):
    hi = x.astype(BF)
    lo = (x - hi.astype(F32)).astype(BF)
    return hi, lo


def wide_kernel(
    n_gx, n_gy, L, R, C, S, B, G,
    warm_in, humid_in, cx_ref, cy_ref, gas_ref, drop_ref, sw_ref, lw_ref, flags_ref, slot_ref,
    t_out, m_out, rates_out,
    ext0, ext1, edge_send, edge_recv, qt, packed, rad, coef, cloudy, absorber, theta, rates, heat, ucols,
    hedge_send, hedge_recv, rows_send, rows_recv,
    halo_send_sem, halo_recv_sem, edge_send_sem, edge_recv_sem, misc_send_sem, misc_recv_sem,
):
    g = lax.axis_index("grp")
    x = lax.axis_index("gx")
    y = lax.axis_index("gy")
    og = 1 - g
    xn, xp = lax.rem(x + 1, n_gx), lax.rem(x + n_gx - 1, n_gx)
    yn, yp = lax.rem(y + 1, n_gy), lax.rem(y + n_gy - 1, n_gy)
    fields = (warm_in, humid_in)
    ext = (ext0, ext1)
    outs = (t_out, m_out)
    LE = L + M
    T = (R + 2 * M) // 8
    per = C // T
    NP = -(-LE // per)
    RI = R // 2
    RLO = 8
    ROWN = RLO + M
    RE = R + 2 * M

    barrier = pltpu.get_barrier_semaphore()
    for dev in ((g, xn, y), (g, xp, y), (og, x, y), (og, xn, y), (og, xp, y), (g, x, yn), (g, x, yp)):
        pl.semaphore_signal(barrier, inc=1, device_id=dev, device_id_type=MESH)
    pl.semaphore_wait(barrier, 7)

    def remote(src, dst, ss, rs, dev):
        c = pltpu.make_async_remote_copy(
            src_ref=src, dst_ref=dst, send_sem=ss, recv_sem=rs, device_id=dev, device_id_type=MESH
        )
        c.start()
        return c

    half = slot_ref.shape[1]
    slots = slot_ref[...]
    rep = (
        lax.broadcasted_iota(jnp.int32, (half, C), 1) // 2
        == lax.broadcasted_iota(jnp.int32, (half, C), 0)
    ).astype(F32).astype(BF)
    s_hi = (slots // 16).astype(F32).astype(BF)
    s_lo = (slots % 16).astype(F32).astype(BF)
    slot_rep = (
        16.0 * jnp.dot(s_hi, rep, preferred_element_type=F32)
        + jnp.dot(s_lo, rep, preferred_element_type=F32)
    ).astype(jnp.int32)
    s_iota = lax.broadcasted_iota(jnp.int32, (S, C), 0)
    for i in range(RI):
        qt[:, i * C : (i + 1) * C] = jnp.where(s_iota == slot_rep[i : i + 1, :], 1.0, 0.0).astype(BF)
    parts = []
    for i in range(RI):
        col = []
        for f in range(2):
            flat = fields[f].reshape(L * R, C)
            col.append(
                flat[pl.ds(2 * i, L, stride=R), :] + flat[pl.ds(2 * i + 1, L, stride=R), :]
            )
        hi, lo = split_bf16(0.25 * jnp.concatenate(col, axis=0))
        parts.append(jnp.concatenate([hi, lo], axis=0))
    lhs = jnp.concatenate(parts, axis=1)
    both = lax.dot_general(
        lhs, qt[...], (((1,), (1,)), ((), ())), preferred_element_type=F32
    )
    both = both[: 2 * L] + both[2 * L :]
    for h in range(2):
        packed[h] = both[:, h * B : (h + 1) * B]
    c_packed = remote(packed.at[og], rad.at[g], misc_send_sem.at[0], misc_recv_sem.at[0], (og, x, y))

    lev_src = (L - M) * og
    lev_dst = 1 + L * g
    own_dst = 1 + M * g
    halos = []
    n = 0
    for f in range(2):
        for levs, dlevs, count, gg in ((0, own_dst, L, g), (lev_src, lev_dst, M, og)):
            for r0, d0, xx in ((R - M, RLO, xn), (0, ROWN + R, xp)):
                halos.append(remote(
                    fields[f].at[pl.ds(levs, count), r0 : r0 + M, :],
                    ext0.at[f, pl.ds(dlevs, count), d0 : d0 + M, :],
                    halo_send_sem.at[n], halo_recv_sem.at[n], (gg, xx, y),
                ))
                n += 1
        halos.append(remote(
            fields[f].at[pl.ds(lev_src, M)],
            ext0.at[f, pl.ds(lev_dst, M), ROWN : ROWN + R, :],
            halo_send_sem.at[n], halo_recv_sem.at[n], (og, x, y),
        ))
        n += 1
    rad[g] = packed[g]
    for f in range(2):
        ext0[f, pl.ds(own_dst, L), ROWN : ROWN + R, :] = fields[f][...]
        for b in range(2):
            for p in (0, LE + 1):
                ext[b][f, p] = jnp.zeros((RE + 16, C), F32)

    log2e = 1.0 / math.log(2.0)
    for q, (ref, scale) in enumerate(((gas_ref, -log2e), (drop_ref, -log2e), (sw_ref, 1.0), (lw_ref, 1.0))):
        coef[q] = jnp.broadcast_to(ref[...] * scale, (128, G)).T
    for hb in range(B // 128):
        cloudy[hb] = flags_ref[:, hb * 128 : (hb + 1) * 128].astype(F32)

    c_packed.wait()
    for o in range(2):
        mo = rad[o, L : 2 * L, :]
        soft = jnp.maximum(mo, 0.0) + jnp.log1p(jnp.exp(-jnp.abs(mo)))
        for hb in range(B // 128):
            absorber[hb, o * L : (o + 1) * L, :] = soft[:, hb * 128 : (hb + 1) * 128]
            theta[hb, o * L : (o + 1) * L, :] = rad[o, 0:L, hb * 128 : (hb + 1) * 128]

    GB = G // 8
    norm = 4.0 / G
    for hb in range(B // 128):
        for o in range(2):
            def level(l, flux, o=o, hb=hb):
                lg = l + o * L
                a = jnp.broadcast_to(absorber[hb, pl.ds(lg, 1), :], (8, 128))
                c = jnp.broadcast_to(cloudy[hb, pl.ds(lg, 1), :], (8, 128))
                th = 1.0 + 0.1 * theta[hb, pl.ds(lg, 1), :]
                sw = lw = None
                new = []
                for q in range(GB):
                    rows = slice(8 * q, 8 * q + 8)
                    d = 1.0 - jnp.exp2(a * coef[0, rows, :] + c * coef[1, rows, :])
                    s = flux[q] * d
                    w = coef[3, rows, :] * d
                    sw = s if sw is None else sw + s
                    lw = w if lw is None else lw + w
                    new.append(flux[q] - s)
                total = jnp.sum(sw - lw * th, axis=0, keepdims=True) * norm
                rates[o, hb, pl.ds(l, 1), :] = total
                return tuple(new)

            if o == 0:
                flux = tuple(coef[2, 8 * q : 8 * q + 8, :] for q in range(GB))
            flux = lax.fori_loop(0, L, level, flux, unroll=2)
    c_heat = remote(rates.at[og], heat.at[g], misc_send_sem.at[1], misc_recv_sem.at[1], (og, x, y))
    heat[g] = rates[g]
    for o in range(2):
        for hb in range(B // 128):
            rates_out[o * L : (o + 1) * L, hb * 128 : (hb + 1) * 128] = rates[o, hb]

    lane = lax.broadcasted_iota(jnp.int32, (8, C), 1)

    def pack(vals, j, accs):
        right, left = accs
        for t in range(T):
            k = j * T + t
            turned = pltpu.roll(vals[8 * t : 8 * t + 8, :], lax.rem(k + 1, C), 1)
            right = jnp.where(lane == k, turned, right)
            left = jnp.where(lane == lax.rem(k + 1, C), turned, left)
        return right, left

    def send_edges(k, f):
        return (
            remote(edge_send.at[k, f, 0], edge_recv.at[k, f, 0],
                   edge_send_sem.at[k, f, 0], edge_recv_sem.at[k, f, 0], (g, x, yn)),
            remote(edge_send.at[k, f, 1], edge_recv.at[k, f, 1],
                   edge_send_sem.at[k, f, 1], edge_recv_sem.at[k, f, 1], (g, x, yp)),
        )

    zero = jnp.zeros((8, C), F32)

    def run_levels(k, f, count, values):
        for p in range(NP):
            lo, hi = p * per, min(count, (p + 1) * per)
            if lo >= hi:
                edge_send[k, f, 0, p] = zero
                edge_send[k, f, 1, p] = zero
                continue
            right, left = lax.fori_loop(
                lo, hi, lambda j, accs, lo=lo: pack(values(j), j - lo, accs), (zero, zero),
                unroll=min(UNROLL, hi - lo),
            )
            edge_send[k, f, 0, p] = right
            edge_send[k, f, 1, p] = left

    def first(f):
        run_levels(0, f, LE, lambda j: ext0[f, j + 1, RLO : RLO + RE, :])
        return send_edges(0, f)

    def sweep(k, f):
        src, dst = (k - 1) % 2, k % 2
        start = g * k
        last = k == SWEEPS
        t0, t1 = (M // 8, M // 8 + R // 8) if last else (0, T)
        r0, r1 = RLO + 8 * t0, RLO + 8 * t1

        def values(j):
            lev = start + j
            p = lev + 1
            jj = j + g
            which = jj // per
            kk = (jj - which * per) * T
            from_left = edge_recv[k - 1, f, 0, which]
            from_right = edge_recv[k - 1, f, 1, which]
            lg = lev + (L - M) * g
            sx = 0.5 * cx_ref[lg]
            sy = 0.5 * cy_ref[lg]
            cen = ext[src][f, p, r0:r1, :]
            base = (
                (1.0 - 4.0 * NU_H - 2.0 * NU_V) * cen
                + NU_V * (ext[src][f, p + 1, r0:r1, :] + ext[src][f, p - 1, r0:r1, :])
                + (NU_H - sx) * ext[src][f, p, r0 + 1 : r1 + 1, :]
                + (NU_H + sx) * ext[src][f, p, r0 - 1 : r1 - 1, :]
            )
            res = []
            for t in range(t0, t1):
                q = 8 * (t - t0)
                v = cen[q : q + 8, :]
                kt = kk + t
                prev = jnp.where(lane == 0, pltpu.roll(from_left, lax.rem(C - kt, C), 1), pltpu.roll(v, 1, 1))
                nxt = jnp.where(
                    lane == C - 1, pltpu.roll(from_right, lax.rem(2 * C - 2 - kt, C), 1), pltpu.roll(v, C - 1, 1)
                )
                res.append(base[q : q + 8, :] + (NU_H - sy) * nxt + (NU_H + sy) * prev)
            new = jnp.concatenate(res, axis=0)
            if last:
                outs[f][j] = new
            else:
                ext[dst][f, p, RLO : RLO + RE, :] = new
            return new

        count = LE - k
        if last:
            @pl.loop(0, count, unroll=UNROLL)
            def _(j):
                values(j)
            return None
        run_levels(k, f, count, values)
        return send_edges(k, f)

    for c in halos:
        c.wait()
    flight = [first(0), first(1)]
    sent = []

    def advance(ks):
        for k in ks:
            for f in range(2):
                for c in flight[f]:
                    c.wait()
                flight[f] = sweep(k, f)

    advance((1, 2))

    c_heat.wait()
    hi, lo = split_bf16(jnp.concatenate([heat[h, hb] for h in range(2) for hb in range(B // 128)], axis=1))
    spread = jnp.dot(jnp.concatenate([hi, lo], axis=0), qt[...], preferred_element_type=F32)
    spread = spread[:L] + spread[L:]
    LT = L // 8
    ehi = zero
    elo = zero
    for i in range(RI):
        ui = spread[:, i * C : (i + 1) * C]
        ucols[i] = ui
        for t in range(LT):
            k = i * LT + t
            turned = pltpu.roll(ui[8 * t : 8 * t + 8, :], (k + 1) % C, 1)
            ehi = jnp.where(lane == k, turned, ehi)
            elo = jnp.where(lane == (k + 1) % C, turned, elo)
    hedge_send[0] = ehi
    hedge_send[1] = elo
    c_he = [
        remote(hedge_send.at[0], hedge_recv.at[0], misc_send_sem.at[2], misc_recv_sem.at[2], (g, x, yn)),
        remote(hedge_send.at[1], hedge_recv.at[1], misc_send_sem.at[3], misc_recv_sem.at[3], (g, x, yp)),
    ]
    advance((3,))
    for c in c_he:
        c.wait()
    from_left = hedge_recv[0]
    from_right = hedge_recv[1]
    even = lane % 2 == 0
    for i in range(RI):
        for t in range(LT):
            k = i * LT + t
            v = ucols[i, 8 * t : 8 * t + 8, :]
            prev = jnp.where(lane == 0, pltpu.roll(from_left, (C - k) % C, 1), pltpu.roll(v, 1, 1))
            nxt = jnp.where(lane == C - 1, pltpu.roll(from_right, (2 * C - 2 - k) % C, 1), pltpu.roll(v, C - 1, 1))
            w = 0.75 * v + 0.25 * jnp.where(even, prev, nxt)
            ucols[i, 8 * t : 8 * t + 8, :] = w
            if i == 0:
                rows_send[0, 8 * t : 8 * t + 8, :] = w
            if i == RI - 1:
                rows_send[1, 8 * t : 8 * t + 8, :] = w
    c_rows = [
        remote(rows_send.at[0], rows_recv.at[0], misc_send_sem.at[4], misc_recv_sem.at[4], (g, xp, y)),
        remote(rows_send.at[1], rows_recv.at[1], misc_send_sem.at[5], misc_recv_sem.at[5], (g, xn, y)),
    ]
    advance(range(4, SWEEPS + 1))
    for c in c_rows:
        c.wait()
    flat = t_out.reshape(L * R, C)
    for i in range(RI):
        v = ucols[i]
        above = rows_recv[1] if i == 0 else ucols[i - 1]
        below = rows_recv[0] if i == RI - 1 else ucols[i + 1]
        flat[pl.ds(2 * i, L, stride=R), :] = flat[pl.ds(2 * i, L, stride=R), :] + HEATING_INTERVAL * (0.75 * v + 0.25 * above)
        flat[pl.ds(2 * i + 1, L, stride=R), :] = flat[pl.ds(2 * i + 1, L, stride=R), :] + HEATING_INTERVAL * (0.75 * v + 0.25 * below)


def hand_on(t_in, m_in, r_in, t_out, m_out, r_out):
    t_out[...] = t_in[...]
    m_out[...] = m_in[...]
    r_out[...] = r_in[...]


def wide_body(n_gx, n_gy, warm, humid, cx, cy, gas, drop, sw, lw, flags, slots):
    L, R, C = warm.shape
    S = slots.shape[0] * slots.shape[1]
    B = flags.shape[0]
    flags = flags.T
    G = gas.shape[0]
    LE = L + M
    T = (R + 2 * M) // 8
    NP = -(-LE // (C // T))
    vmem = pl.BlockSpec(memory_space=pltpu.VMEM)
    smem = pl.BlockSpec(memory_space=pltpu.SMEM)
    t, m, rates = pl.pallas_call(
        functools.partial(wide_kernel, n_gx, n_gy, L, R, C, S, B, G),
        out_shape=(
            jax.ShapeDtypeStruct((L, R, C), F32),
            jax.ShapeDtypeStruct((L, R, C), F32),
            jax.ShapeDtypeStruct((2 * L, B), F32),
        ),
        in_specs=[vmem, vmem, smem, smem] + [vmem] * 6,
        out_specs=(vmem, vmem, vmem),
        scratch_shapes=[
            pltpu.VMEM((2, LE + 2, R + 2 * M + 16, C), F32),
            pltpu.VMEM((2, LE + 2, R + 2 * M + 16, C), F32),
            pltpu.VMEM((SWEEPS, 2, 2, NP, 8, C), F32),
            pltpu.VMEM((SWEEPS, 2, 2, NP, 8, C), F32),
            pltpu.VMEM((S, (R // 2) * C), BF),
            pltpu.VMEM((2, 2 * L, B), F32),
            pltpu.VMEM((2, 2 * L, B), F32),
            pltpu.VMEM((4, G, 128), F32),
            pltpu.VMEM((B // 128, 2 * L, 128), F32),
            pltpu.VMEM((B // 128, 2 * L, 128), F32),
            pltpu.VMEM((B // 128, 2 * L, 128), F32),
            pltpu.VMEM((2, B // 128, L, 128), F32),
            pltpu.VMEM((2, B // 128, L, 128), F32),
            pltpu.VMEM((R // 2, L, C), F32),
            pltpu.VMEM((2, 8, C), F32),
            pltpu.VMEM((2, 8, C), F32),
            pltpu.VMEM((2, L, C), F32),
            pltpu.VMEM((2, L, C), F32),
            pltpu.SemaphoreType.DMA((10,)),
            pltpu.SemaphoreType.DMA((10,)),
            pltpu.SemaphoreType.DMA((SWEEPS, 2, 2)),
            pltpu.SemaphoreType.DMA((SWEEPS, 2, 2)),
            pltpu.SemaphoreType.DMA((6,)),
            pltpu.SemaphoreType.DMA((6,)),
        ],
        compiler_params=pltpu.CompilerParams(collective_id=0, has_side_effects=True),
    )(
        warm, humid, cx, cy, gas[None], drop[None], sw[None], lw[None], flags, slots,
    )
    t, m, rates = pl.pallas_call(
        hand_on,
        out_shape=tuple(jax.ShapeDtypeStruct(a.shape, F32) for a in (t, m, rates)),
        in_specs=[vmem] * 3,
        out_specs=(vmem,) * 3,
    )(t, m, rates)
    return t, m, rates.T


CHUNKS = ((0, 4), (4, 7), (7, 8))
PAD = 8


def pair_kernel(
    n_gx, L, R, C, S, B, G,
    warm_hbm, humid_hbm, cx_hbm, cy_hbm, gas_hbm, drop_hbm, sw_hbm, lw_hbm, flags_hbm, slot_hbm,
    res, heat_out, rates_out,
    fields, small, gpoint, flags_ref, slot_ref,
    loc, buf0, buf1, fin, got, warm, adv, lines, qt, packed, rad, coef, cloudy, absorber, theta, passed, rates, heat, ucols, ends_send, ends_recv, corner_send, corner_recv,
    in_sem, pair_sem, lev_sem, row_send_sem, row_recv_sem, corner_sem, misc_sem, gate,
):
    g = lax.axis_index("grp")
    x = lax.axis_index("gx")
    y = lax.axis_index("gy")
    og = 1 - g
    oy = 1 - y
    xn, xp = lax.rem(x + 1, n_gx), lax.rem(x + n_gx - 1, n_gx)
    LE = L + M
    RE = R + 2 * M
    RI = R // 2
    bufs = (buf0, buf1)

    sub = lax.broadcasted_iota(jnp.int32, (M, C), 0)
    barrier = pltpu.get_barrier_semaphore()
    partners = [(g, x, oy), (og, x, 0), (og, x, 1)]
    beside = [(g, xx, yy) for xx in (xn, xp) for yy in range(2)]
    partners += beside
    for dev in partners:
        pl.semaphore_signal(barrier, inc=1, device_id=dev, device_id_type=MESH)

    loads = []
    pairs = [(warm_hbm, fields.at[0]), (humid_hbm, fields.at[1]), (slot_hbm, slot_ref)]
    pairs += [(cx_hbm, small.at[0]), (cy_hbm, small.at[1])]
    pairs += [(r, gpoint.at[q]) for q, r in enumerate((gas_hbm, drop_hbm, sw_hbm, lw_hbm))]
    pairs += [(flags_hbm, flags_ref)]
    for n, (src, dst) in enumerate(pairs):
        c = pltpu.make_async_copy(src, dst, in_sem.at[n])
        c.start()
        loads.append(c)

    def remote(src, dst, ss, rs, dev):
        c = pltpu.make_async_remote_copy(
            src_ref=src, dst_ref=dst, send_sem=ss, recv_sem=rs, device_id=dev, device_id_type=MESH
        )
        c.start()
        return c

    def matching(ref, sem):
        return pltpu.make_async_remote_copy(
            src_ref=ref, dst_ref=ref, send_sem=sem, recv_sem=sem, device_id=(g, x, oy), device_id_type=MESH
        )

    def arrived(ref, sem):
        matching(ref, sem).wait_recv()

    def left(ref, sem):
        matching(ref, sem).wait_send()

    edge = jnp.zeros((RE, 8, C), F32)
    for b in bufs:
        for h in range(2):
            b[h, :, 0:PAD, :] = edge
            b[h, :, PAD + LE : PAD + LE + 8, :] = edge

    for n in range(2):
        loads[n].wait()
    for f in range(2):
        flat = fields.at[f].reshape(L * R, C)
        for r in range(R):
            loc[f, r] = flat[pl.ds(r, L, stride=R), :]

    own_dst = pl.multiple_of(PAD + M * g, 8)
    lev_src = pl.multiple_of((L - M) * og, 8)
    lev_own = pl.multiple_of(PAD + M * g + (L - M) * og, 8)
    lev_dst = pl.multiple_of(PAD + L * g, 8)
    lev_in = pl.multiple_of(PAD + L * og, 8)

    def send_levels(r0, r1):
        for f in range(2):
            remote(
                loc.at[f, r0:r1, pl.ds(lev_src, M), :], buf0.at[y, M + r0 : M + r1, pl.ds(lev_dst, M), :],
                lev_sem.at[0], lev_sem.at[1], (og, x, f),
            )

    def greet():
        pl.semaphore_wait(barrier, 7)
        for dev in beside:
            pl.semaphore_signal(gate, inc=1, device_id=dev, device_id_type=MESH)
        for c, (d1, d0) in enumerate(CHUNKS):
            for side, xx in ((0, xn), (1, xp)):
                s0 = R - d0 if side == 0 else d1
                t0 = M - d0 if side == 0 else M + R + d1
                for f in range(2):
                    remote(
                        loc.at[f, s0 : s0 + d0 - d1], buf0.at[y, t0 : t0 + d0 - d1, pl.ds(own_dst, L), :],
                        row_send_sem.at[0], row_recv_sem.at[side, c], (g, xx, f),
                    )
        remote(
            loc.at[oy], buf0.at[y, M : M + R, pl.ds(own_dst, L), :], pair_sem.at[0], pair_sem.at[1], (g, x, oy)
        )

    def gather():
        loads[2].wait()
        half = slot_ref.shape[1]
        slots = slot_ref[...]
        rep = (
            lax.broadcasted_iota(jnp.int32, (half, C), 1) // 2
            == lax.broadcasted_iota(jnp.int32, (half, C), 0)
        ).astype(F32).astype(BF)
        s_hi = (slots // 16).astype(F32).astype(BF)
        s_lo = (slots % 16).astype(F32).astype(BF)
        slot_rep = (
            16.0 * jnp.dot(s_hi, rep, preferred_element_type=F32)
            + jnp.dot(s_lo, rep, preferred_element_type=F32)
        ).astype(jnp.int32)
        s_iota = lax.broadcasted_iota(jnp.int32, (S, C), 0)
        for i in range(RI):
            qt[:, i * C : (i + 1) * C] = jnp.where(s_iota == slot_rep[i : i + 1, :], 1.0, 0.0).astype(BF)
        parts = []
        for i in range(RI):
            col = [loc[f, 2 * i] + loc[f, 2 * i + 1] for f in range(2)]
            hi, lo = split_bf16(0.25 * jnp.concatenate(col, axis=0))
            parts.append(jnp.concatenate([hi, lo], axis=0))
        lhs = jnp.concatenate(parts, axis=1)
        both = lax.dot_general(
            lhs, qt[...], (((1,), (1,)), ((), ())), preferred_element_type=F32
        )
        both = both[: 2 * L] + both[2 * L :]
        for h in range(2):
            packed[h] = both[:, h * B : (h + 1) * B]

    early = jnp.where(x == 0, 1, 1 - g)

    @pl.loop(0, 2)
    def _(turn):
        pl.when(turn == 1 - early)(gather)
        pl.when(turn == early)(greet)

    c_packed = remote(packed.at[og], rad.at[g], misc_sem.at[0], misc_sem.at[1], (og, x, y))
    send_levels(0, R)
    def send_corners():
        for f in range(2):
            for side in range(2):
                for j in range(M // 2):
                    d = j + 1
                    near, far = (R - d, R - M + d) if side == 0 else (d - 1, M - d - 1)
                    a = loc[f, near, pl.ds(lev_src, M), :]
                    b = loc[f, far, pl.ds(lev_src, M), :]
                    above = jnp.where(sub >= d, a, pltpu.roll(b, d, 0))
                    below = jnp.where(sub < M - d, a, pltpu.roll(b, M - d, 0))
                    corner_send[f, side, j] = jnp.where(g == 0, above, below)
        pl.semaphore_wait(gate, 4)
        for f in range(2):
            for side, xx in ((0, xn), (1, xp)):
                remote(
                    corner_send.at[f, side], corner_recv.at[y, side],
                    corner_sem.at[0], corner_sem.at[1], (og, xx, f),
                )

    def rows_arrived(side, c):
        d1, d0 = CHUNKS[c]
        arrived(buf0.at[:, 0 : d0 - d1, pl.ds(own_dst, L), :], row_recv_sem.at[side, c])

    def corners_arrived():
        arrived(corner_recv, corner_sem.at[1])
        for h in range(2):
            for side in range(2):
                for j in range(M // 2):
                    d = j + 1
                    near, far = (M - d, d) if side == 0 else (M + R + d - 1, R + 2 * M - d - 1)
                    v = corner_recv[h, side, j]
                    buf0[h, near, pl.ds(lev_in, M), :] = v
                    if near != far:
                        back = jnp.where(g == 1, pltpu.roll(v, M - d, 0), pltpu.roll(v, d, 0))
                        buf0[h, far, pl.ds(lev_in, M), :] = back

    rad[g] = packed[g]
    buf0[y, M : M + R, pl.ds(own_dst, L), :] = loc[y]

    for n in range(3, len(loads)):
        loads[n].wait()
    for q in range(2):
        lines[q] = jnp.broadcast_to(small[q], (C, 2 * L)).T
    for q in range(2):
        part = 0.5 * lines[q, pl.ds(pl.multiple_of((L - M) * g, 8), LE), :]
        adv[2 * q] = NU_H - part
        adv[2 * q + 1] = NU_H + part
    log2e = 1.0 / math.log(2.0)
    for q, scale in enumerate((-log2e, -log2e, 1.0, 1.0)):
        coef[q] = jnp.broadcast_to(gpoint[q] * scale, (128, G)).T
    for hb in range(B // 128):
        cloudy[hb] = flags_ref[:, hb * 128 : (hb + 1) * 128].astype(F32)

    GB = G // 8
    HB = B // 128
    norm = 4.0 / G
    c_heat = pltpu.make_async_remote_copy(
        src_ref=rates.at[og], dst_ref=heat.at[g], send_sem=misc_sem.at[2], recv_sem=misc_sem.at[3],
        device_id=(og, x, y), device_id_type=MESH,
    )
    pl.when(g == 1)(send_corners)
    for o in range(2):
        @pl.when(og == o)
        def _():
            c_packed.wait()

        mo = rad[o, L : 2 * L, :]
        soft = jnp.maximum(mo, 0.0) + jnp.log1p(jnp.exp(-jnp.abs(mo)))
        for hb in range(HB):
            absorber[hb, o * L : (o + 1) * L, :] = soft[:, hb * 128 : (hb + 1) * 128]
            theta[hb, o * L : (o + 1) * L, :] = rad[o, 0:L, hb * 128 : (hb + 1) * 128]
        for hb in range(HB):
            def level(l, flux, o=o, hb=hb):
                lg = l + o * L
                a = jnp.broadcast_to(absorber[hb, pl.ds(lg, 1), :], (8, 128))
                c = jnp.broadcast_to(cloudy[hb, pl.ds(lg, 1), :], (8, 128))
                th = 1.0 + 0.1 * theta[hb, pl.ds(lg, 1), :]
                sw = lw = None
                new = []
                for q in range(GB):
                    rows = slice(8 * q, 8 * q + 8)
                    d = 1.0 - jnp.exp2(a * coef[0, rows, :] + c * coef[1, rows, :])
                    s = flux[q] * d
                    w = coef[3, rows, :] * d
                    sw = s if sw is None else sw + s
                    lw = w if lw is None else lw + w
                    new.append(flux[q] - s)
                total = jnp.sum(sw - lw * th, axis=0, keepdims=True) * norm
                rates[o, hb, pl.ds(l, 1), :] = total
                return tuple(new)

            start = coef.at[2] if o == 0 else passed.at[hb]
            flux = tuple(start[8 * q : 8 * q + 8, :] for q in range(GB))
            flux = lax.fori_loop(0, L, level, flux, unroll=2)
            if o == 0:
                for q in range(GB):
                    passed[hb, 8 * q : 8 * q + 8, :] = flux[q]
            rates_out[o * L : (o + 1) * L, hb * 128 : (hb + 1) * 128] = rates[o, hb]

        @pl.when(og == o)
        def _():
            c_heat.start()
        if o == 0:
            pl.when(g == 0)(send_corners)
    heat[g] = rates[g]

    def stencil(k, i0, n):
        src, dst = bufs[(k - 1) % 2], bufs[k % 2]
        lane = lax.broadcasted_iota(jnp.int32, (n * LE, C), 1)
        span = [src[h, pl.ds(i0 - 1, n + 2), PAD : PAD + LE, :] for h in range(2)]
        mid = [v[1 : n + 1].reshape(n * LE, C) for v in span]
        right = [pltpu.roll(v, 1, 1) for v in mid]
        left = [pltpu.roll(v, C - 1, 1) for v in mid]
        for h in range(2):
            prev = jnp.where(lane == 0, right[1 - h], right[h]).reshape(n, LE, C)
            nxt = jnp.where(lane == C - 1, left[1 - h], left[h]).reshape(n, LE, C)
            up = src[h, pl.ds(i0, n), PAD - 1 : PAD + LE - 1, :]
            down = src[h, pl.ds(i0, n), PAD + 1 : PAD + LE + 1, :]
            new = (
                (1.0 - 4.0 * NU_H - 2.0 * NU_V) * span[h][1 : n + 1]
                + NU_V * (up + down)
                + adv[0][None] * span[h][2 : n + 2]
                + adv[1][None] * span[h][0:n]
                + adv[2][None] * nxt
                + adv[3][None] * prev
            )
            if k == SWEEPS:
                fin[h, pl.ds(i0 - M, n)] = new
            else:
                dst[h, pl.ds(i0, n), PAD : PAD + LE, :] = new

    mine = pl.multiple_of(M * g, 8)

    def widen(*parts, last=3):
        for k in range(1, SWEEPS + 1):
            for side, d1, d0 in parts:
                for e in range(d0, d1, -2):
                    n = min(2, e - d1)
                    stencil(k, M + k - e if side == 0 else M + R - k + e - n, n)
        for side, d1, d0 in parts:
            n = d0 - d1
            r = SWEEPS - d0 if side == 0 else R - SWEEPS + d1
            remote(
                fin.at[oy, r : r + n, pl.ds(mine, L), :], got.at[r : r + n],
                pair_sem.at[2], pair_sem.at[last], (g, x, oy),
            )

    arrived(buf0.at[oy, M : M + R, pl.ds(own_dst, L), :], pair_sem.at[1])
    arrived(buf0.at[:, M : M + R, pl.ds(lev_in, M), :], lev_sem.at[1])
    for k in range(1, SWEEPS):
        i0, i1 = M + k, M + R - k
        while i0 < i1:
            n = min(2, i1 - i0)
            stencil(k, i0, n)
            i0 += n

    LH = L // 2
    lane = lax.broadcasted_iota(jnp.int32, (LH, C), 1)
    even = lane % 2 == 0

    c_heat.wait()
    hi, lo = split_bf16(jnp.concatenate([heat[h, hb] for h in range(2) for hb in range(B // 128)], axis=1))
    spread = jnp.dot(jnp.concatenate([hi, lo], axis=0), qt[...], preferred_element_type=F32)
    spread = spread[:L] + spread[L:]
    for i in range(RI):
        ucols[y, 1 + i] = spread[:, i * C : (i + 1) * C]
    for e, i in ((1, 0), (0, RI - 1)):
        v = spread[:, i * C : (i + 1) * C]
        ends_send[e] = jnp.where(even, v[:LH], v[LH:])
    for e, xx in ((1, xp), (0, xn)):
        for yy in range(2):
            remote(ends_send.at[e], ends_recv.at[y, e], misc_sem.at[4], misc_sem.at[5], (g, xx, yy))
    remote(
        ucols.at[y, 1 : RI + 1], ucols.at[y, 1 : RI + 1], misc_sem.at[6], misc_sem.at[7], (g, x, oy)
    )
    corners_arrived()

    def heat_rows():
        left(ucols.at[y, 1 : RI + 1], misc_sem.at[6])
        arrived(ucols.at[oy, 1 : RI + 1], misc_sem.at[7])
        arrived(ends_recv, misc_sem.at[5])
        for h in range(2):
            for e, i in ((0, 0), (1, RI + 1)):
                v = ends_recv[h, e]
                ucols[h, i, 0:LH] = jnp.where(even, v, pltpu.roll(v, 1, 1))
                ucols[h, i, LH:L] = jnp.where(even, pltpu.roll(v, C - 1, 1), v)
        lane = lax.broadcasted_iota(jnp.int32, (L, C), 1)
        cols = []
        for i in range(RI + 2):
            v, o = ucols[y, i], ucols[oy, i]
            prev = jnp.where(lane == 0, pltpu.roll(o, 1, 1), pltpu.roll(v, 1, 1))
            nxt = jnp.where(lane == C - 1, pltpu.roll(o, C - 1, 1), pltpu.roll(v, C - 1, 1))
            cols.append(HEATING_INTERVAL * (0.75 * v + 0.25 * jnp.where(lane % 2 == 0, prev, nxt)))
        for i in range(RI):
            warm[2 * i] = 0.75 * cols[i + 1] + 0.25 * cols[i]
            warm[2 * i + 1] = 0.75 * cols[i + 1] + 0.25 * cols[i + 2]

    def rows_in(first):
        second = 1 - first
        rows_arrived(first, 0)
        widen((first, 0, 4))
        rows_arrived(first, 1)
        rows_arrived(first, 2)
        rows_arrived(second, 0)
        widen((first, 4, 8), (second, 0, 4))
        rows_arrived(second, 1)
        widen((second,) + CHUNKS[1], last=4)
        heat_rows()
        rows_arrived(second, 2)
        widen((second,) + CHUNKS[2], last=4)

    for first in range(2):
        pl.when(lax.rem(x, 2) == first)(functools.partial(rows_in, first))
    flat = res.reshape(2 * L * R, C)
    heat_flat = heat_out.reshape(L * R, C)
    for r in range(R):
        flat[pl.ds(y * (L * R) + r, L, stride=R), :] = fin[y, r, pl.ds(mine, L), :]
        heat_flat[pl.ds(r, L, stride=R), :] = warm[r]
    late = M - CHUNKS[0][1]
    arrived(got.at[0 : R - late], pair_sem.at[3])

    def take(side, near, far):
        for e in range(near + 1, far + 1):
            r = M - e if side == 0 else R - M + e - 1
            flat[pl.ds(oy * (L * R) + r, L, stride=R), :] = got[r]

    def take_early(first):
        take(first, 0, M)
        take(1 - first, 0, M - late)

    def take_late(first):
        take(1 - first, M - late, M)

    for first in range(2):
        pl.when(lax.rem(x, 2) == first)(functools.partial(take_early, first))
    left(buf0.at[:, 0 : 2 * M, 0:L, :], row_send_sem.at[0])
    left(corner_send, corner_sem.at[0])
    left(buf0.at[:, 0:R, 0:M, :], lev_sem.at[0])
    left(loc.at[oy], pair_sem.at[0])
    left(ends_recv, misc_sem.at[4])
    arrived(got.at[0:late], pair_sem.at[4])
    for first in range(2):
        pl.when(lax.rem(x, 2) == first)(functools.partial(take_late, first))
    left(got, pair_sem.at[2])


def settle(res, heat, r_in, t_out, m_out, r_out, t_ref, sem):
    copies = [
        pltpu.make_async_copy(res.at[1], m_out, sem.at[0]),
        pltpu.make_async_copy(r_in, r_out, sem.at[1]),
        pltpu.make_async_copy(t_ref, t_out, sem.at[2]),
    ]
    copies[0].start()
    copies[1].start()
    t_ref[...] = res[0] + heat[...]
    copies[2].start()
    for c in copies:
        c.wait()


def pair_body(n_gx, n_gy, warm, humid, cx, cy, gas, drop, sw, lw, flags, slots):
    L, R, C = warm.shape
    S = slots.shape[0] * slots.shape[1]
    B = flags.shape[0]
    flags = flags.T
    G = gas.shape[0]
    LE = L + M
    LP = PAD + LE + 8
    RE = R + 2 * M
    vmem = pl.BlockSpec(memory_space=pltpu.VMEM)
    hbm = pl.BlockSpec(memory_space=pltpu.HBM)
    res, heat, rates = pl.pallas_call(
        functools.partial(pair_kernel, n_gx, L, R, C, S, B, G),
        out_shape=(
            jax.ShapeDtypeStruct((2, L, R, C), F32),
            jax.ShapeDtypeStruct((L, R, C), F32),
            jax.ShapeDtypeStruct((2 * L, B), F32),
        ),
        in_specs=[hbm] * 10,
        out_specs=(vmem, vmem, vmem),
        scratch_shapes=[
            pltpu.VMEM((2, L, R, C), F32),
            pltpu.VMEM((2, 1, 2 * L), F32),
            pltpu.VMEM((4, 1, G), F32),
            pltpu.VMEM((2 * L, B), jnp.int32),
            pltpu.VMEM(slots.shape, jnp.int32),
            pltpu.VMEM((2, R, L, C), F32),
            pltpu.VMEM((2, RE, LP, C), F32),
            pltpu.VMEM((2, RE, LP, C), F32),
            pltpu.VMEM((2, R, LE, C), F32),
            pltpu.VMEM((R, L, C), F32),
            pltpu.VMEM((R, L, C), F32),
            pltpu.VMEM((4, LE, C), F32),
            pltpu.VMEM((2, 2 * L, C), F32),
            pltpu.VMEM((S, (R // 2) * C), BF),
            pltpu.VMEM((2, 2 * L, B), F32),
            pltpu.VMEM((2, 2 * L, B), F32),
            pltpu.VMEM((4, G, 128), F32),
            pltpu.VMEM((B // 128, 2 * L, 128), F32),
            pltpu.VMEM((B // 128, 2 * L, 128), F32),
            pltpu.VMEM((B // 128, 2 * L, 128), F32),
            pltpu.VMEM((B // 128, G, 128), F32),
            pltpu.VMEM((2, B // 128, L, 128), F32),
            pltpu.VMEM((2, B // 128, L, 128), F32),
            pltpu.VMEM((2, R // 2 + 2, L, C), F32),
            pltpu.VMEM((2, L // 2, C), F32),
            pltpu.VMEM((2, 2, L // 2, C), F32),
            pltpu.VMEM((2, 2, M // 2, M, C), F32),
            pltpu.VMEM((2, 2, M // 2, M, C), F32),
            pltpu.SemaphoreType.DMA((10,)),
            pltpu.SemaphoreType.DMA((5,)),
            pltpu.SemaphoreType.DMA((2,)),
            pltpu.SemaphoreType.DMA((1,)),
            pltpu.SemaphoreType.DMA((2, len(CHUNKS))),
            pltpu.SemaphoreType.DMA((2,)),
            pltpu.SemaphoreType.DMA((8,)),
            pltpu.SemaphoreType.REGULAR,
        ],
        compiler_params=pltpu.CompilerParams(
            collective_id=0, has_side_effects=True, vmem_limit_bytes=32 * 1024 * 1024
        ),
    )(*(
        pltpu.with_memory_space_constraint(a, pltpu.HBM)
        for a in (warm, humid, cx[None], cy[None], gas[None], drop[None], sw[None], lw[None], flags, slots)
    ))
    t, m, rates = pl.pallas_call(
        settle,
        out_shape=(
            jax.ShapeDtypeStruct((L, R, C), F32),
            jax.ShapeDtypeStruct((L, R, C), F32),
            jax.ShapeDtypeStruct((2 * L, B), F32),
        ),
        in_specs=[vmem] * 3,
        out_specs=(hbm,) * 3,
        scratch_shapes=[
            pltpu.VMEM((L, R, C), F32),
            pltpu.SemaphoreType.DMA((3,)),
        ],
        compiler_params=pltpu.CompilerParams(vmem_limit_bytes=8 * 1024 * 1024),
    )(res, heat, rates)
    return t, m, rates.T


def solution(mesh):
    assert mesh.shape["grp"] == 2
    in_specs = (
        P("grp", "gx", "gy"), P("grp", "gx", "gy"), P(), P(), P(), P(), P(), P(),
        P(("grp", "gx", "gy"), None), P("gx", "gy"),
    )
    out_specs = (P("grp", "gx", "gy"), P("grp", "gx", "gy"), P(("grp", "gx", "gy"), None))
    paired = mesh.shape["gy"] == 2 and mesh.shape["gx"] > 2
    return jax.shard_map(
        functools.partial(pair_body if paired else wide_body, mesh.shape["gx"], mesh.shape["gy"]),
        mesh=mesh, in_specs=in_specs, out_specs=out_specs, check_vma=False,
    )
```

```python
import functools
import math

import jax
import jax.numpy as jnp
from jax import lax
from jax.experimental import pallas as pl
from jax.experimental.pallas import tpu as pltpu
from jax.sharding import PartitionSpec as P

SWEEPS = 8
NU_H = 0.15
NU_V = 0.15
HEATING_INTERVAL = 0.5
UNROLL = 8
M = 8
MESH = pl.DeviceIdType.MESH
BF = jnp.bfloat16
F32 = jnp.float32


def split_bf16(x):
    hi = x.astype(BF)
    lo = (x - hi.astype(F32)).astype(BF)
    return hi, lo


def wide_kernel(
    n_gx, n_gy, L, R, C, S, B, G,
    warm_in, humid_in, cx_ref, cy_ref, gas_ref, drop_ref, sw_ref, lw_ref, flags_ref, slot_ref,
    t_out, m_out, rates_out,
    ext0, ext1, edge_send, edge_recv, qt, packed, rad, coef, cloudy, absorber, theta, rates, heat, ucols,
    hedge_send, hedge_recv, rows_send, rows_recv,
    halo_send_sem, halo_recv_sem, edge_send_sem, edge_recv_sem, misc_send_sem, misc_recv_sem,
):
    g = lax.axis_index("grp")
    x = lax.axis_index("gx")
    y = lax.axis_index("gy")
    og = 1 - g
    xn, xp = lax.rem(x + 1, n_gx), lax.rem(x + n_gx - 1, n_gx)
    yn, yp = lax.rem(y + 1, n_gy), lax.rem(y + n_gy - 1, n_gy)
    fields = (warm_in, humid_in)
    ext = (ext0, ext1)
    outs = (t_out, m_out)
    LE = L + M
    T = (R + 2 * M) // 8
    per = C // T
    NP = -(-LE // per)
    RI = R // 2
    RLO = 8
    ROWN = RLO + M
    RE = R + 2 * M

    barrier = pltpu.get_barrier_semaphore()
    for dev in ((g, xn, y), (g, xp, y), (og, x, y), (og, xn, y), (og, xp, y), (g, x, yn), (g, x, yp)):
        pl.semaphore_signal(barrier, inc=1, device_id=dev, device_id_type=MESH)
    pl.semaphore_wait(barrier, 7)

    def remote(src, dst, ss, rs, dev):
        c = pltpu.make_async_remote_copy(
            src_ref=src, dst_ref=dst, send_sem=ss, recv_sem=rs, device_id=dev, device_id_type=MESH
        )
        c.start()
        return c

    half = slot_ref.shape[1]
    slots = slot_ref[...]
    rep = (
        lax.broadcasted_iota(jnp.int32, (half, C), 1) // 2
        == lax.broadcasted_iota(jnp.int32, (half, C), 0)
    ).astype(F32).astype(BF)
    s_hi = (slots // 16).astype(F32).astype(BF)
    s_lo = (slots % 16).astype(F32).astype(BF)
    slot_rep = (
        16.0 * jnp.dot(s_hi, rep, preferred_element_type=F32)
        + jnp.dot(s_lo, rep, preferred_element_type=F32)
    ).astype(jnp.int32)
    s_iota = lax.broadcasted_iota(jnp.int32, (S, C), 0)
    for i in range(RI):
        qt[:, i * C : (i + 1) * C] = jnp.where(s_iota == slot_rep[i : i + 1, :], 1.0, 0.0).astype(BF)
    parts = []
    for i in range(RI):
        col = []
        for f in range(2):
            flat = fields[f].reshape(L * R, C)
            col.append(
                flat[pl.ds(2 * i, L, stride=R), :] + flat[pl.ds(2 * i + 1, L, stride=R), :]
            )
        hi, lo = split_bf16(0.25 * jnp.concatenate(col, axis=0))
        parts.append(jnp.concatenate([hi, lo], axis=0))
    lhs = jnp.concatenate(parts, axis=1)
    both = lax.dot_general(
        lhs, qt[...], (((1,), (1,)), ((), ())), preferred_element_type=F32
    )
    both = both[: 2 * L] + both[2 * L :]
    for h in range(2):
        packed[h] = both[:, h * B : (h + 1) * B]
    c_packed = remote(packed.at[og], rad.at[g], misc_send_sem.at[0], misc_recv_sem.at[0], (og, x, y))

    lev_src = (L - M) * og
    lev_dst = 1 + L * g
    own_dst = 1 + M * g
    halos = []
    n = 0
    for f in range(2):
        for levs, dlevs, count, gg in ((0, own_dst, L, g), (lev_src, lev_dst, M, og)):
            for r0, d0, xx in ((R - M, RLO, xn), (0, ROWN + R, xp)):
                halos.append(remote(
                    fields[f].at[pl.ds(levs, count), r0 : r0 + M, :],
                    ext0.at[f, pl.ds(dlevs, count), d0 : d0 + M, :],
                    halo_send_sem.at[n], halo_recv_sem.at[n], (gg, xx, y),
                ))
                n += 1
        halos.append(remote(
            fields[f].at[pl.ds(lev_src, M)],
            ext0.at[f, pl.ds(lev_dst, M), ROWN : ROWN + R, :],
            halo_send_sem.at[n], halo_recv_sem.at[n], (og, x, y),
        ))
        n += 1
    rad[g] = packed[g]
    for f in range(2):
        ext0[f, pl.ds(own_dst, L), ROWN : ROWN + R, :] = fields[f][...]
        for b in range(2):
            for p in (0, LE + 1):
                ext[b][f, p] = jnp.zeros((RE + 16, C), F32)

    log2e = 1.0 / math.log(2.0)
    for q, (ref, scale) in enumerate(((gas_ref, -log2e), (drop_ref, -log2e), (sw_ref, 1.0), (lw_ref, 1.0))):
        coef[q] = jnp.broadcast_to(ref[...] * scale, (128, G)).T
    for hb in range(B // 128):
        cloudy[hb] = flags_ref[:, hb * 128 : (hb + 1) * 128].astype(F32)

    c_packed.wait()
    for o in range(2):
        mo = rad[o, L : 2 * L, :]
        soft = jnp.maximum(mo, 0.0) + jnp.log1p(jnp.exp(-jnp.abs(mo)))
        for hb in range(B // 128):
            absorber[hb, o * L : (o + 1) * L, :] = soft[:, hb * 128 : (hb + 1) * 128]
            theta[hb, o * L : (o + 1) * L, :] = rad[o, 0:L, hb * 128 : (hb + 1) * 128]

    GB = G // 8
    norm = 4.0 / G
    for hb in range(B // 128):
        for o in range(2):
            def level(l, flux, o=o, hb=hb):
                lg = l + o * L
                a = jnp.broadcast_to(absorber[hb, pl.ds(lg, 1), :], (8, 128))
                c = jnp.broadcast_to(cloudy[hb, pl.ds(lg, 1), :], (8, 128))
                th = 1.0 + 0.1 * theta[hb, pl.ds(lg, 1), :]
                sw = lw = None
                new = []
                for q in range(GB):
                    rows = slice(8 * q, 8 * q + 8)
                    d = 1.0 - jnp.exp2(a * coef[0, rows, :] + c * coef[1, rows, :])
                    s = flux[q] * d
                    w = coef[3, rows, :] * d
                    sw = s if sw is None else sw + s
                    lw = w if lw is None else lw + w
                    new.append(flux[q] - s)
                total = jnp.sum(sw - lw * th, axis=0, keepdims=True) * norm
                rates[o, hb, pl.ds(l, 1), :] = total
                return tuple(new)

            if o == 0:
                flux = tuple(coef[2, 8 * q : 8 * q + 8, :] for q in range(GB))
            flux = lax.fori_loop(0, L, level, flux, unroll=2)
    c_heat = remote(rates.at[og], heat.at[g], misc_send_sem.at[1], misc_recv_sem.at[1], (og, x, y))
    heat[g] = rates[g]
    for o in range(2):
        for hb in range(B // 128):
            rates_out[o * L : (o + 1) * L, hb * 128 : (hb + 1) * 128] = rates[o, hb]

    lane = lax.broadcasted_iota(jnp.int32, (8, C), 1)

    def pack(vals, j, accs):
        right, left = accs
        for t in range(T):
            k = j * T + t
            turned = pltpu.roll(vals[8 * t : 8 * t + 8, :], lax.rem(k + 1, C), 1)
            right = jnp.where(lane == k, turned, right)
            left = jnp.where(lane == lax.rem(k + 1, C), turned, left)
        return right, left

    def send_edges(k, f):
        return (
            remote(edge_send.at[k, f, 0], edge_recv.at[k, f, 0],
                   edge_send_sem.at[k, f, 0], edge_recv_sem.at[k, f, 0], (g, x, yn)),
            remote(edge_send.at[k, f, 1], edge_recv.at[k, f, 1],
                   edge_send_sem.at[k, f, 1], edge_recv_sem.at[k, f, 1], (g, x, yp)),
        )

    zero = jnp.zeros((8, C), F32)

    def run_levels(k, f, count, values):
        for p in range(NP):
            lo, hi = p * per, min(count, (p + 1) * per)
            if lo >= hi:
                edge_send[k, f, 0, p] = zero
                edge_send[k, f, 1, p] = zero
                continue
            right, left = lax.fori_loop(
                lo, hi, lambda j, accs, lo=lo: pack(values(j), j - lo, accs), (zero, zero),
                unroll=min(UNROLL, hi - lo),
            )
            edge_send[k, f, 0, p] = right
            edge_send[k, f, 1, p] = left

    def first(f):
        run_levels(0, f, LE, lambda j: ext0[f, j + 1, RLO : RLO + RE, :])
        return send_edges(0, f)

    def sweep(k, f):
        src, dst = (k - 1) % 2, k % 2
        start = g * k
        last = k == SWEEPS
        t0, t1 = (M // 8, M // 8 + R // 8) if last else (0, T)
        r0, r1 = RLO + 8 * t0, RLO + 8 * t1

        def values(j):
            lev = start + j
            p = lev + 1
            jj = j + g
            which = jj // per
            kk = (jj - which * per) * T
            from_left = edge_recv[k - 1, f, 0, which]
            from_right = edge_recv[k - 1, f, 1, which]
            lg = lev + (L - M) * g
            sx = 0.5 * cx_ref[lg]
            sy = 0.5 * cy_ref[lg]
            cen = ext[src][f, p, r0:r1, :]
            base = (
                (1.0 - 4.0 * NU_H - 2.0 * NU_V) * cen
                + NU_V * (ext[src][f, p + 1, r0:r1, :] + ext[src][f, p - 1, r0:r1, :])
                + (NU_H - sx) * ext[src][f, p, r0 + 1 : r1 + 1, :]
                + (NU_H + sx) * ext[src][f, p, r0 - 1 : r1 - 1, :]
            )
            res = []
            for t in range(t0, t1):
                q = 8 * (t - t0)
                v = cen[q : q + 8, :]
                kt = kk + t
                prev = jnp.where(lane == 0, pltpu.roll(from_left, lax.rem(C - kt, C), 1), pltpu.roll(v, 1, 1))
                nxt = jnp.where(
                    lane == C - 1, pltpu.roll(from_right, lax.rem(2 * C - 2 - kt, C), 1), pltpu.roll(v, C - 1, 1)
                )
                res.append(base[q : q + 8, :] + (NU_H - sy) * nxt + (NU_H + sy) * prev)
            new = jnp.concatenate(res, axis=0)
            if last:
                outs[f][j] = new
            else:
                ext[dst][f, p, RLO : RLO + RE, :] = new
            return new

        count = LE - k
        if last:
            @pl.loop(0, count, unroll=UNROLL)
            def _(j):
                values(j)
            return None
        run_levels(k, f, count, values)
        return send_edges(k, f)

    for c in halos:
        c.wait()
    flight = [first(0), first(1)]
    sent = []

    def advance(ks):
        for k in ks:
            for f in range(2):
                for c in flight[f]:
                    c.wait()
                flight[f] = sweep(k, f)

    advance((1, 2))

    c_heat.wait()
    hi, lo = split_bf16(jnp.concatenate([heat[h, hb] for h in range(2) for hb in range(B // 128)], axis=1))
    spread = jnp.dot(jnp.concatenate([hi, lo], axis=0), qt[...], preferred_element_type=F32)
    spread = spread[:L] + spread[L:]
    LT = L // 8
    ehi = zero
    elo = zero
    for i in range(RI):
        ui = spread[:, i * C : (i + 1) * C]
        ucols[i] = ui
        for t in range(LT):
            k = i * LT + t
            turned = pltpu.roll(ui[8 * t : 8 * t + 8, :], (k + 1) % C, 1)
            ehi = jnp.where(lane == k, turned, ehi)
            elo = jnp.where(lane == (k + 1) % C, turned, elo)
    hedge_send[0] = ehi
    hedge_send[1] = elo
    c_he = [
        remote(hedge_send.at[0], hedge_recv.at[0], misc_send_sem.at[2], misc_recv_sem.at[2], (g, x, yn)),
        remote(hedge_send.at[1], hedge_recv.at[1], misc_send_sem.at[3], misc_recv_sem.at[3], (g, x, yp)),
    ]
    advance((3,))
    for c in c_he:
        c.wait()
    from_left = hedge_recv[0]
    from_right = hedge_recv[1]
    even = lane % 2 == 0
    for i in range(RI):
        for t in range(LT):
            k = i * LT + t
            v = ucols[i, 8 * t : 8 * t + 8, :]
            prev = jnp.where(lane == 0, pltpu.roll(from_left, (C - k) % C, 1), pltpu.roll(v, 1, 1))
            nxt = jnp.where(lane == C - 1, pltpu.roll(from_right, (2 * C - 2 - k) % C, 1), pltpu.roll(v, C - 1, 1))
            w = 0.75 * v + 0.25 * jnp.where(even, prev, nxt)
            ucols[i, 8 * t : 8 * t + 8, :] = w
            if i == 0:
                rows_send[0, 8 * t : 8 * t + 8, :] = w
            if i == RI - 1:
                rows_send[1, 8 * t : 8 * t + 8, :] = w
    c_rows = [
        remote(rows_send.at[0], rows_recv.at[0], misc_send_sem.at[4], misc_recv_sem.at[4], (g, xp, y)),
        remote(rows_send.at[1], rows_recv.at[1], misc_send_sem.at[5], misc_recv_sem.at[5], (g, xn, y)),
    ]
    advance(range(4, SWEEPS + 1))
    for c in c_rows:
        c.wait()
    flat = t_out.reshape(L * R, C)
    for i in range(RI):
        v = ucols[i]
        above = rows_recv[1] if i == 0 else ucols[i - 1]
        below = rows_recv[0] if i == RI - 1 else ucols[i + 1]
        flat[pl.ds(2 * i, L, stride=R), :] = flat[pl.ds(2 * i, L, stride=R), :] + HEATING_INTERVAL * (0.75 * v + 0.25 * above)
        flat[pl.ds(2 * i + 1, L, stride=R), :] = flat[pl.ds(2 * i + 1, L, stride=R), :] + HEATING_INTERVAL * (0.75 * v + 0.25 * below)


def hand_on(t_in, m_in, r_in, t_out, m_out, r_out):
    t_out[...] = t_in[...]
    m_out[...] = m_in[...]
    r_out[...] = r_in[...]


def wide_body(n_gx, n_gy, warm, humid, cx, cy, gas, drop, sw, lw, flags, slots):
    L, R, C = warm.shape
    S = slots.shape[0] * slots.shape[1]
    B = flags.shape[0]
    flags = flags.T
    G = gas.shape[0]
    LE = L + M
    T = (R + 2 * M) // 8
    NP = -(-LE // (C // T))
    vmem = pl.BlockSpec(memory_space=pltpu.VMEM)
    smem = pl.BlockSpec(memory_space=pltpu.SMEM)
    t, m, rates = pl.pallas_call(
        functools.partial(wide_kernel, n_gx, n_gy, L, R, C, S, B, G),
        out_shape=(
            jax.ShapeDtypeStruct((L, R, C), F32),
            jax.ShapeDtypeStruct((L, R, C), F32),
            jax.ShapeDtypeStruct((2 * L, B), F32),
        ),
        in_specs=[vmem, vmem, smem, smem] + [vmem] * 6,
        out_specs=(vmem, vmem, vmem),
        scratch_shapes=[
            pltpu.VMEM((2, LE + 2, R + 2 * M + 16, C), F32),
            pltpu.VMEM((2, LE + 2, R + 2 * M + 16, C), F32),
            pltpu.VMEM((SWEEPS, 2, 2, NP, 8, C), F32),
            pltpu.VMEM((SWEEPS, 2, 2, NP, 8, C), F32),
            pltpu.VMEM((S, (R // 2) * C), BF),
            pltpu.VMEM((2, 2 * L, B), F32),
            pltpu.VMEM((2, 2 * L, B), F32),
            pltpu.VMEM((4, G, 128), F32),
            pltpu.VMEM((B // 128, 2 * L, 128), F32),
            pltpu.VMEM((B // 128, 2 * L, 128), F32),
            pltpu.VMEM((B // 128, 2 * L, 128), F32),
            pltpu.VMEM((2, B // 128, L, 128), F32),
            pltpu.VMEM((2, B // 128, L, 128), F32),
            pltpu.VMEM((R // 2, L, C), F32),
            pltpu.VMEM((2, 8, C), F32),
            pltpu.VMEM((2, 8, C), F32),
            pltpu.VMEM((2, L, C), F32),
            pltpu.VMEM((2, L, C), F32),
            pltpu.SemaphoreType.DMA((10,)),
            pltpu.SemaphoreType.DMA((10,)),
            pltpu.SemaphoreType.DMA((SWEEPS, 2, 2)),
            pltpu.SemaphoreType.DMA((SWEEPS, 2, 2)),
            pltpu.SemaphoreType.DMA((6,)),
            pltpu.SemaphoreType.DMA((6,)),
        ],
        compiler_params=pltpu.CompilerParams(collective_id=0, has_side_effects=True),
    )(
        warm, humid, cx, cy, gas[None], drop[None], sw[None], lw[None], flags, slots,
    )
    t, m, rates = pl.pallas_call(
        hand_on,
        out_shape=tuple(jax.ShapeDtypeStruct(a.shape, F32) for a in (t, m, rates)),
        in_specs=[vmem] * 3,
        out_specs=(vmem,) * 3,
    )(t, m, rates)
    return t, m, rates.T


CHUNKS = ((0, 4), (4, 7), (7, 8))
PAD = 8


def pair_kernel(
    n_gx, L, R, C, S, B, G,
    warm_hbm, humid_hbm, cx_hbm, cy_hbm, gas_hbm, drop_hbm, sw_hbm, lw_hbm, flags_hbm, slot_hbm,
    res, heat_out, rates_out,
    fields, small, gpoint, flags_ref, slot_ref,
    loc, buf0, buf1, fin, got, adv, lines, qt, packed, rad, coef, cloudy, absorber, theta, passed, rates, heat, ucols, ends_send, ends_recv, corner_send, corner_recv,
    in_sem, pair_sem, lev_sem, row_send_sem, row_recv_sem, corner_sem, misc_sem, gate,
):
    g = lax.axis_index("grp")
    x = lax.axis_index("gx")
    y = lax.axis_index("gy")
    og = 1 - g
    oy = 1 - y
    xn, xp = lax.rem(x + 1, n_gx), lax.rem(x + n_gx - 1, n_gx)
    LE = L + M
    RE = R + 2 * M
    RI = R // 2
    bufs = (buf0, buf1)

    sub = lax.broadcasted_iota(jnp.int32, (M, C), 0)
    barrier = pltpu.get_barrier_semaphore()
    partners = [(g, x, oy), (og, x, 0), (og, x, 1)]
    beside = [(g, xx, yy) for xx in (xn, xp) for yy in range(2)]
    partners += beside
    for dev in partners:
        pl.semaphore_signal(barrier, inc=1, device_id=dev, device_id_type=MESH)

    tail = x == n_gx - 1

    @pl.when(x == 0)
    def _():
        for yy in range(2):
            pl.semaphore_signal(barrier, inc=1, device_id=(og, xp, yy), device_id_type=MESH)

    loads = []
    pairs = [(warm_hbm, fields.at[0]), (humid_hbm, fields.at[1]), (slot_hbm, slot_ref)]
    pairs += [(cx_hbm, small.at[0]), (cy_hbm, small.at[1])]
    pairs += [(r, gpoint.at[q]) for q, r in enumerate((gas_hbm, drop_hbm, sw_hbm, lw_hbm))]
    pairs += [(flags_hbm, flags_ref)]
    for n, (src, dst) in enumerate(pairs):
        c = pltpu.make_async_copy(src, dst, in_sem.at[n])
        c.start()
        loads.append(c)

    def remote(src, dst, ss, rs, dev):
        c = pltpu.make_async_remote_copy(
            src_ref=src, dst_ref=dst, send_sem=ss, recv_sem=rs, device_id=dev, device_id_type=MESH
        )
        c.start()
        return c

    def matching(ref, sem):
        return pltpu.make_async_remote_copy(
            src_ref=ref, dst_ref=ref, send_sem=sem, recv_sem=sem, device_id=(g, x, oy), device_id_type=MESH
        )

    def arrived(ref, sem):
        matching(ref, sem).wait_recv()

    def left(ref, sem):
        matching(ref, sem).wait_send()

    edge = jnp.zeros((RE, 8, C), F32)
    for b in bufs:
        for h in range(2):
            b[h, :, 0:PAD, :] = edge
            b[h, :, PAD + LE : PAD + LE + 8, :] = edge

    for n in range(2):
        loads[n].wait()
    for f in range(2):
        flat = fields.at[f].reshape(L * R, C)
        for r in range(R):
            loc[f, r] = flat[pl.ds(r, L, stride=R), :]

    own_dst = pl.multiple_of(PAD + M * g, 8)
    lev_src = pl.multiple_of((L - M) * og, 8)
    lev_own = pl.multiple_of(PAD + M * g + (L - M) * og, 8)
    lev_dst = pl.multiple_of(PAD + L * g, 8)
    lev_in = pl.multiple_of(PAD + L * og, 8)

    def send_levels(r0, r1):
        for f in range(2):
            remote(
                loc.at[f, r0:r1, pl.ds(lev_src, M), :], buf0.at[y, M + r0 : M + r1, pl.ds(lev_dst, M), :],
                lev_sem.at[0], lev_sem.at[1], (og, x, f),
            )

    def greet():
        pl.semaphore_wait(barrier, jnp.where(tail, 9, 7))

        def pass_on(xx):
            for yy in range(2):
                pl.semaphore_signal(gate, inc=1, device_id=(g, xx, yy), device_id_type=MESH)

        pass_on(xn)
        pl.when(x > 0)(functools.partial(pass_on, xp))

        for c, (d1, d0) in enumerate(CHUNKS):
            for side, xx in ((0, xn), (1, xp)):
                s0 = R - d0 if side == 0 else d1
                t0 = M - d0 if side == 0 else M + R + d1
                for f in range(2):
                    remote(
                        loc.at[f, s0 : s0 + d0 - d1], buf0.at[y, t0 : t0 + d0 - d1, pl.ds(own_dst, L), :],
                        row_send_sem.at[0], row_recv_sem.at[side, c], (g, xx, f),
                    )
        remote(
            loc.at[oy], buf0.at[y, M : M + R, pl.ds(own_dst, L), :], pair_sem.at[0], pair_sem.at[1], (g, x, oy)
        )

    def gather():
        loads[2].wait()
        half = slot_ref.shape[1]
        slots = slot_ref[...]
        rep = (
            lax.broadcasted_iota(jnp.int32, (half, C), 1) // 2
            == lax.broadcasted_iota(jnp.int32, (half, C), 0)
        ).astype(F32).astype(BF)
        s_hi = (slots // 16).astype(F32).astype(BF)
        s_lo = (slots % 16).astype(F32).astype(BF)
        slot_rep = (
            16.0 * jnp.dot(s_hi, rep, preferred_element_type=F32)
            + jnp.dot(s_lo, rep, preferred_element_type=F32)
        ).astype(jnp.int32)
        s_iota = lax.broadcasted_iota(jnp.int32, (S, C), 0)
        for i in range(RI):
            qt[:, i * C : (i + 1) * C] = jnp.where(s_iota == slot_rep[i : i + 1, :], 1.0, 0.0).astype(BF)
        parts = []
        for i in range(RI):
            col = [loc[f, 2 * i] + loc[f, 2 * i + 1] for f in range(2)]
            hi, lo = split_bf16(0.25 * jnp.concatenate(col, axis=0))
            parts.append(jnp.concatenate([hi, lo], axis=0))
        lhs = jnp.concatenate(parts, axis=1)
        both = lax.dot_general(
            lhs, qt[...], (((1,), (1,)), ((), ())), preferred_element_type=F32
        )
        both = both[: 2 * L] + both[2 * L :]
        for h in range(2):
            packed[h] = both[:, h * B : (h + 1) * B]
        for n in range(3, len(loads)):
            loads[n].wait()
        for q in range(2):
            lines[q] = jnp.broadcast_to(small[q], (C, 2 * L)).T
        for q in range(2):
            part = 0.5 * lines[q, pl.ds(pl.multiple_of((L - M) * g, 8), LE), :]
            adv[2 * q] = NU_H - part
            adv[2 * q + 1] = NU_H + part
        log2e = 1.0 / math.log(2.0)
        for q, scale in enumerate((-log2e, -log2e, 1.0, 1.0)):
            coef[q] = jnp.broadcast_to(gpoint[q] * scale, (128, G)).T
        for hb in range(B // 128):
            cloudy[hb] = flags_ref[:, hb * 128 : (hb + 1) * 128].astype(F32)

    early = jnp.where(x == 0, 1, 0)

    @pl.loop(0, 2)
    def _(turn):
        pl.when(turn == 1 - early)(gather)
        pl.when(turn == early)(greet)

    c_packed = remote(packed.at[og], rad.at[g], misc_sem.at[0], misc_sem.at[1], (og, x, y))
    for f in range(2):
        for side in range(2):
            for j in range(M // 2):
                d = j + 1
                near, far = (R - d, R - M + d) if side == 0 else (d - 1, M - d - 1)
                a = loc[f, near, pl.ds(lev_src, M), :]
                b = loc[f, far, pl.ds(lev_src, M), :]
                above = jnp.where(sub >= d, a, pltpu.roll(b, d, 0))
                below = jnp.where(sub < M - d, a, pltpu.roll(b, M - d, 0))
                corner_send[f, side, j] = jnp.where(g == 0, above, below)

    def corners_to(side, xx):
        for f in range(2):
            remote(
                corner_send.at[f, side], corner_recv.at[y, side],
                corner_sem.at[0], corner_sem.at[1], (og, xx, f),
            )

    def send_corners():
        pl.semaphore_wait(gate, jnp.where(tail, 2, 4))
        pl.when(x < n_gx - 1)(functools.partial(corners_to, 0, xn))
        corners_to(1, xp)

    pl.when(tail)(functools.partial(corners_to, 0, xn))
    send_levels(0, R)

    def rows_arrived(side, c):
        d1, d0 = CHUNKS[c]
        arrived(buf0.at[:, 0 : d0 - d1, pl.ds(own_dst, L), :], row_recv_sem.at[side, c])

    def corners_arrived():
        arrived(corner_recv, corner_sem.at[1])
        for h in range(2):
            for side in range(2):
                for j in range(M // 2):
                    d = j + 1
                    near, far = (M - d, d) if side == 0 else (M + R + d - 1, R + 2 * M - d - 1)
                    v = corner_recv[h, side, j]
                    buf0[h, near, pl.ds(lev_in, M), :] = v
                    if near != far:
                        back = jnp.where(g == 1, pltpu.roll(v, M - d, 0), pltpu.roll(v, d, 0))
                        buf0[h, far, pl.ds(lev_in, M), :] = back

    rad[g] = packed[g]
    buf0[y, M : M + R, pl.ds(own_dst, L), :] = loc[y]

    GB = G // 8
    HB = B // 128
    norm = 4.0 / G
    c_heat = pltpu.make_async_remote_copy(
        src_ref=rates.at[og], dst_ref=heat.at[g], send_sem=misc_sem.at[2], recv_sem=misc_sem.at[3],
        device_id=(og, x, y), device_id_type=MESH,
    )
    pl.when(g == 1)(send_corners)
    for o in range(2):
        @pl.when(og == o)
        def _():
            c_packed.wait()

        mo = rad[o, L : 2 * L, :]
        soft = jnp.maximum(mo, 0.0) + jnp.log1p(jnp.exp(-jnp.abs(mo)))
        for hb in range(HB):
            absorber[hb, o * L : (o + 1) * L, :] = soft[:, hb * 128 : (hb + 1) * 128]
            theta[hb, o * L : (o + 1) * L, :] = rad[o, 0:L, hb * 128 : (hb + 1) * 128]
        for hb in range(HB):
            def level(l, flux, o=o, hb=hb):
                lg = l + o * L
                a = jnp.broadcast_to(absorber[hb, pl.ds(lg, 1), :], (8, 128))
                c = jnp.broadcast_to(cloudy[hb, pl.ds(lg, 1), :], (8, 128))
                th = 1.0 + 0.1 * theta[hb, pl.ds(lg, 1), :]
                sw = lw = None
                new = []
                for q in range(GB):
                    rows = slice(8 * q, 8 * q + 8)
                    d = 1.0 - jnp.exp2(a * coef[0, rows, :] + c * coef[1, rows, :])
                    s = flux[q] * d
                    w = coef[3, rows, :] * d
                    sw = s if sw is None else sw + s
                    lw = w if lw is None else lw + w
                    new.append(flux[q] - s)
                total = jnp.sum(sw - lw * th, axis=0, keepdims=True) * norm
                rates[o, hb, pl.ds(l, 1), :] = total
                return tuple(new)

            start = coef.at[2] if o == 0 else passed.at[hb]
            flux = tuple(start[8 * q : 8 * q + 8, :] for q in range(GB))
            flux = lax.fori_loop(0, L, level, flux, unroll=2)
            if o == 0:
                for q in range(GB):
                    passed[hb, 8 * q : 8 * q + 8, :] = flux[q]
            rates_out[o * L : (o + 1) * L, hb * 128 : (hb + 1) * 128] = rates[o, hb]

        @pl.when(og == o)
        def _():
            c_heat.start()
        if o == 0:
            pl.when(g == 0)(send_corners)
    heat[g] = rates[g]

    def stencil(k, i0, n):
        src, dst = bufs[(k - 1) % 2], bufs[k % 2]
        lane = lax.broadcasted_iota(jnp.int32, (n * LE, C), 1)
        span = [src[h, pl.ds(i0 - 1, n + 2), PAD : PAD + LE, :] for h in range(2)]
        mid = [v[1 : n + 1].reshape(n * LE, C) for v in span]
        right = [pltpu.roll(v, 1, 1) for v in mid]
        left = [pltpu.roll(v, C - 1, 1) for v in mid]
        for h in range(2):
            prev = jnp.where(lane == 0, right[1 - h], right[h]).reshape(n, LE, C)
            nxt = jnp.where(lane == C - 1, left[1 - h], left[h]).reshape(n, LE, C)
            up = src[h, pl.ds(i0, n), PAD - 1 : PAD + LE - 1, :]
            down = src[h, pl.ds(i0, n), PAD + 1 : PAD + LE + 1, :]
            new = (
                (1.0 - 4.0 * NU_H - 2.0 * NU_V) * span[h][1 : n + 1]
                + NU_V * (up + down)
                + adv[0][None] * span[h][2 : n + 2]
                + adv[1][None] * span[h][0:n]
                + adv[2][None] * nxt
                + adv[3][None] * prev
            )
            if k == SWEEPS:
                fin[h, pl.ds(i0 - M, n)] = new
            else:
                dst[h, pl.ds(i0, n), PAD : PAD + LE, :] = new

    mine = pl.multiple_of(M * g, 8)

    def widen(*parts, last=3):
        for d in range(max(d0 - d1 for _, d1, d0 in parts)):
            for k in range(1, SWEEPS + 1):
                for side, d1, d0 in parts:
                    e = d1 + d + 1
                    if e <= d0:
                        stencil(k, M + k - e if side == 0 else M + R - 1 - k + e, 1)
        for side, d1, d0 in parts:
            n = d0 - d1
            r = SWEEPS - d0 if side == 0 else R - SWEEPS + d1
            remote(
                fin.at[oy, r : r + n, pl.ds(mine, L), :], got.at[r : r + n],
                pair_sem.at[2], pair_sem.at[last], (g, x, oy),
            )

    arrived(buf0.at[oy, M : M + R, pl.ds(own_dst, L), :], pair_sem.at[1])
    arrived(buf0.at[:, M : M + R, pl.ds(lev_in, M), :], lev_sem.at[1])
    for k in range(1, SWEEPS):
        i0, i1 = M + k, M + R - k
        while i0 < i1:
            n = min(2, i1 - i0)
            stencil(k, i0, n)
            i0 += n

    LH = L // 2
    lane = lax.broadcasted_iota(jnp.int32, (LH, C), 1)
    even = lane % 2 == 0

    c_heat.wait()
    hi, lo = split_bf16(jnp.concatenate([heat[h, hb] for h in range(2) for hb in range(B // 128)], axis=1))
    spread = jnp.dot(jnp.concatenate([hi, lo], axis=0), qt[...], preferred_element_type=F32)
    spread = spread[:L] + spread[L:]
    for i in range(RI):
        ucols[y, 1 + i] = spread[:, i * C : (i + 1) * C]
    for e, i in ((1, 0), (0, RI - 1)):
        v = spread[:, i * C : (i + 1) * C]
        ends_send[e] = jnp.where(even, v[:LH], v[LH:])
    for e, xx in ((1, xp), (0, xn)):
        for yy in range(2):
            remote(ends_send.at[e], ends_recv.at[y, e], misc_sem.at[4], misc_sem.at[5], (g, xx, yy))
    remote(
        ucols.at[y, 1 : RI + 1], ucols.at[y, 1 : RI + 1], misc_sem.at[6], misc_sem.at[7], (g, x, oy)
    )
    corners_arrived()

    heat_flat = heat_out.reshape(L * R, C)

    def heat_rows():
        left(ucols.at[y, 1 : RI + 1], misc_sem.at[6])
        arrived(ucols.at[oy, 1 : RI + 1], misc_sem.at[7])
        arrived(ends_recv, misc_sem.at[5])
        for h in range(2):
            for e, i in ((0, 0), (1, RI + 1)):
                v = ends_recv[h, e]
                ucols[h, i, 0:LH] = jnp.where(even, v, pltpu.roll(v, 1, 1))
                ucols[h, i, LH:L] = jnp.where(even, pltpu.roll(v, C - 1, 1), v)
        lane = lax.broadcasted_iota(jnp.int32, (L, C), 1)
        cols = []
        for i in range(RI + 2):
            v, o = ucols[y, i], ucols[oy, i]
            prev = jnp.where(lane == 0, pltpu.roll(o, 1, 1), pltpu.roll(v, 1, 1))
            nxt = jnp.where(lane == C - 1, pltpu.roll(o, C - 1, 1), pltpu.roll(v, C - 1, 1))
            cols.append(HEATING_INTERVAL * (0.75 * v + 0.25 * jnp.where(lane % 2 == 0, prev, nxt)))
        for i in range(RI):
            heat_flat[pl.ds(2 * i, L, stride=R), :] = 0.75 * cols[i + 1] + 0.25 * cols[i]
            heat_flat[pl.ds(2 * i + 1, L, stride=R), :] = 0.75 * cols[i + 1] + 0.25 * cols[i + 2]

    def rows_in(first):
        second = 1 - first
        rows_arrived(first, 0)
        widen((first, 0, 4))
        rows_arrived(first, 1)
        rows_arrived(first, 2)
        rows_arrived(second, 0)
        widen((first, 4, 8), (second, 0, 4))
        rows_arrived(second, 1)
        widen((second,) + CHUNKS[1], last=4)
        rows_arrived(second, 2)
        widen((second,) + CHUNKS[2], last=4)

    for first in range(2):
        pl.when(lax.rem(x, 2) == first)(functools.partial(rows_in, first))
    flat = res.reshape(2 * L * R, C)
    for r in range(R):
        flat[pl.ds(y * (L * R) + r, L, stride=R), :] = fin[y, r, pl.ds(mine, L), :]
    late = M - CHUNKS[0][1]
    arrived(got.at[0 : R - late], pair_sem.at[3])

    def take(side, near, far):
        for e in range(near + 1, far + 1):
            r = M - e if side == 0 else R - M + e - 1
            flat[pl.ds(oy * (L * R) + r, L, stride=R), :] = got[r]

    def take_early(first):
        take(first, 0, M)
        take(1 - first, 0, M - late)

    def take_late(first):
        take(1 - first, M - late, M)

    for first in range(2):
        pl.when(lax.rem(x, 2) == first)(functools.partial(take_early, first))
    heat_rows()
    left(buf0.at[:, 0 : 2 * M, 0:L, :], row_send_sem.at[0])
    left(corner_send, corner_sem.at[0])
    left(buf0.at[:, 0:R, 0:M, :], lev_sem.at[0])
    left(loc.at[oy], pair_sem.at[0])
    left(ends_recv, misc_sem.at[4])
    arrived(got.at[0:late], pair_sem.at[4])
    for first in range(2):
        pl.when(lax.rem(x, 2) == first)(functools.partial(take_late, first))
    left(got, pair_sem.at[2])


def settle(res, heat, r_in, t_out, m_out, r_out, t_ref, sem):
    copies = [
        pltpu.make_async_copy(res.at[1], m_out, sem.at[0]),
        pltpu.make_async_copy(r_in, r_out, sem.at[1]),
        pltpu.make_async_copy(t_ref, t_out, sem.at[2]),
    ]
    copies[0].start()
    copies[1].start()
    t_ref[...] = res[0] + heat[...]
    copies[2].start()
    for c in copies:
        c.wait()


def pair_body(n_gx, n_gy, warm, humid, cx, cy, gas, drop, sw, lw, flags, slots):
    L, R, C = warm.shape
    S = slots.shape[0] * slots.shape[1]
    B = flags.shape[0]
    flags = flags.T
    G = gas.shape[0]
    LE = L + M
    LP = PAD + LE + 8
    RE = R + 2 * M
    vmem = pl.BlockSpec(memory_space=pltpu.VMEM)
    hbm = pl.BlockSpec(memory_space=pltpu.HBM)
    res, heat, rates = pl.pallas_call(
        functools.partial(pair_kernel, n_gx, L, R, C, S, B, G),
        out_shape=(
            jax.ShapeDtypeStruct((2, L, R, C), F32),
            jax.ShapeDtypeStruct((L, R, C), F32),
            jax.ShapeDtypeStruct((2 * L, B), F32),
        ),
        in_specs=[hbm] * 10,
        out_specs=(vmem, vmem, vmem),
        scratch_shapes=[
            pltpu.VMEM((2, L, R, C), F32),
            pltpu.VMEM((2, 1, 2 * L), F32),
            pltpu.VMEM((4, 1, G), F32),
            pltpu.VMEM((2 * L, B), jnp.int32),
            pltpu.VMEM(slots.shape, jnp.int32),
            pltpu.VMEM((2, R, L, C), F32),
            pltpu.VMEM((2, RE, LP, C), F32),
            pltpu.VMEM((2, RE, LP, C), F32),
            pltpu.VMEM((2, R, LE, C), F32),
            pltpu.VMEM((R, L, C), F32),
            pltpu.VMEM((4, LE, C), F32),
            pltpu.VMEM((2, 2 * L, C), F32),
            pltpu.VMEM((S, (R // 2) * C), BF),
            pltpu.VMEM((2, 2 * L, B), F32),
            pltpu.VMEM((2, 2 * L, B), F32),
            pltpu.VMEM((4, G, 128), F32),
            pltpu.VMEM((B // 128, 2 * L, 128), F32),
            pltpu.VMEM((B // 128, 2 * L, 128), F32),
            pltpu.VMEM((B // 128, 2 * L, 128), F32),
            pltpu.VMEM((B // 128, G, 128), F32),
            pltpu.VMEM((2, B // 128, L, 128), F32),
            pltpu.VMEM((2, B // 128, L, 128), F32),
            pltpu.VMEM((2, R // 2 + 2, L, C), F32),
            pltpu.VMEM((2, L // 2, C), F32),
            pltpu.VMEM((2, 2, L // 2, C), F32),
            pltpu.VMEM((2, 2, M // 2, M, C), F32),
            pltpu.VMEM((2, 2, M // 2, M, C), F32),
            pltpu.SemaphoreType.DMA((10,)),
            pltpu.SemaphoreType.DMA((5,)),
            pltpu.SemaphoreType.DMA((2,)),
            pltpu.SemaphoreType.DMA((1,)),
            pltpu.SemaphoreType.DMA((2, len(CHUNKS))),
            pltpu.SemaphoreType.DMA((2,)),
            pltpu.SemaphoreType.DMA((8,)),
            pltpu.SemaphoreType.REGULAR,
        ],
        compiler_params=pltpu.CompilerParams(
            collective_id=0, has_side_effects=True, vmem_limit_bytes=32 * 1024 * 1024
        ),
    )(*(
        pltpu.with_memory_space_constraint(a, pltpu.HBM)
        for a in (warm, humid, cx[None], cy[None], gas[None], drop[None], sw[None], lw[None], flags, slots)
    ))
    t, m, rates = pl.pallas_call(
        settle,
        out_shape=(
            jax.ShapeDtypeStruct((L, R, C), F32),
            jax.ShapeDtypeStruct((L, R, C), F32),
            jax.ShapeDtypeStruct((2 * L, B), F32),
        ),
        in_specs=[vmem] * 3,
        out_specs=(hbm,) * 3,
        scratch_shapes=[
            pltpu.VMEM((L, R, C), F32),
            pltpu.SemaphoreType.DMA((3,)),
        ],
        compiler_params=pltpu.CompilerParams(vmem_limit_bytes=8 * 1024 * 1024),
    )(res, heat, rates)
    return t, m, rates.T


def solution(mesh):
    assert mesh.shape["grp"] == 2
    in_specs = (
        P("grp", "gx", "gy"), P("grp", "gx", "gy"), P(), P(), P(), P(), P(), P(),
        P(("grp", "gx", "gy"), None), P("gx", "gy"),
    )
    out_specs = (P("grp", "gx", "gy"), P("grp", "gx", "gy"), P(("grp", "gx", "gy"), None))
    paired = mesh.shape["gy"] == 2 and mesh.shape["gx"] > 2
    return jax.shard_map(
        functools.partial(pair_body if paired else wide_body, mesh.shape["gx"], mesh.shape["gy"]),
        mesh=mesh, in_specs=in_specs, out_specs=out_specs, check_vma=False,
    )
```

```python
import functools
import math

import jax
import jax.numpy as jnp
from jax import lax
from jax.experimental import pallas as pl
from jax.experimental.pallas import tpu as pltpu
from jax.sharding import PartitionSpec as P

SWEEPS = 8
NU_H = 0.15
NU_V = 0.15
HEATING_INTERVAL = 0.5
UNROLL = 8
M = 8
MESH = pl.DeviceIdType.MESH
BF = jnp.bfloat16
F32 = jnp.float32


def split_bf16(x):
    hi = x.astype(BF)
    lo = (x - hi.astype(F32)).astype(BF)
    return hi, lo


def wide_kernel(
    n_gx, n_gy, L, R, C, S, B, G,
    warm_in, humid_in, cx_ref, cy_ref, gas_ref, drop_ref, sw_ref, lw_ref, flags_ref, slot_ref,
    t_out, m_out, rates_out,
    ext0, ext1, edge_send, edge_recv, qt, packed, rad, coef, cloudy, absorber, theta, rates, heat, ucols,
    hedge_send, hedge_recv, rows_send, rows_recv,
    halo_send_sem, halo_recv_sem, edge_send_sem, edge_recv_sem, misc_send_sem, misc_recv_sem,
):
    g = lax.axis_index("grp")
    x = lax.axis_index("gx")
    y = lax.axis_index("gy")
    og = 1 - g
    xn, xp = lax.rem(x + 1, n_gx), lax.rem(x + n_gx - 1, n_gx)
    yn, yp = lax.rem(y + 1, n_gy), lax.rem(y + n_gy - 1, n_gy)
    fields = (warm_in, humid_in)
    ext = (ext0, ext1)
    outs = (t_out, m_out)
    LE = L + M
    T = (R + 2 * M) // 8
    per = C // T
    NP = -(-LE // per)
    RI = R // 2
    RLO = 8
    ROWN = RLO + M
    RE = R + 2 * M

    barrier = pltpu.get_barrier_semaphore()
    for dev in ((g, xn, y), (g, xp, y), (og, x, y), (og, xn, y), (og, xp, y), (g, x, yn), (g, x, yp)):
        pl.semaphore_signal(barrier, inc=1, device_id=dev, device_id_type=MESH)
    pl.semaphore_wait(barrier, 7)

    def remote(src, dst, ss, rs, dev):
        c = pltpu.make_async_remote_copy(
            src_ref=src, dst_ref=dst, send_sem=ss, recv_sem=rs, device_id=dev, device_id_type=MESH
        )
        c.start()
        return c

    half = slot_ref.shape[1]
    slots = slot_ref[...]
    rep = (
        lax.broadcasted_iota(jnp.int32, (half, C), 1) // 2
        == lax.broadcasted_iota(jnp.int32, (half, C), 0)
    ).astype(F32).astype(BF)
    s_hi = (slots // 16).astype(F32).astype(BF)
    s_lo = (slots % 16).astype(F32).astype(BF)
    slot_rep = (
        16.0 * jnp.dot(s_hi, rep, preferred_element_type=F32)
        + jnp.dot(s_lo, rep, preferred_element_type=F32)
    ).astype(jnp.int32)
    s_iota = lax.broadcasted_iota(jnp.int32, (S, C), 0)
    for i in range(RI):
        qt[:, i * C : (i + 1) * C] = jnp.where(s_iota == slot_rep[i : i + 1, :], 1.0, 0.0).astype(BF)
    parts = []
    for i in range(RI):
        col = []
        for f in range(2):
            flat = fields[f].reshape(L * R, C)
            col.append(
                flat[pl.ds(2 * i, L, stride=R), :] + flat[pl.ds(2 * i + 1, L, stride=R), :]
            )
        hi, lo = split_bf16(0.25 * jnp.concatenate(col, axis=0))
        parts.append(jnp.concatenate([hi, lo], axis=0))
    lhs = jnp.concatenate(parts, axis=1)
    both = lax.dot_general(
        lhs, qt[...], (((1,), (1,)), ((), ())), preferred_element_type=F32
    )
    both = both[: 2 * L] + both[2 * L :]
    for h in range(2):
        packed[h] = both[:, h * B : (h + 1) * B]
    c_packed = remote(packed.at[og], rad.at[g], misc_send_sem.at[0], misc_recv_sem.at[0], (og, x, y))

    lev_src = (L - M) * og
    lev_dst = 1 + L * g
    own_dst = 1 + M * g
    halos = []
    n = 0
    for f in range(2):
        for levs, dlevs, count, gg in ((0, own_dst, L, g), (lev_src, lev_dst, M, og)):
            for r0, d0, xx in ((R - M, RLO, xn), (0, ROWN + R, xp)):
                halos.append(remote(
                    fields[f].at[pl.ds(levs, count), r0 : r0 + M, :],
                    ext0.at[f, pl.ds(dlevs, count), d0 : d0 + M, :],
                    halo_send_sem.at[n], halo_recv_sem.at[n], (gg, xx, y),
                ))
                n += 1
        halos.append(remote(
            fields[f].at[pl.ds(lev_src, M)],
            ext0.at[f, pl.ds(lev_dst, M), ROWN : ROWN + R, :],
            halo_send_sem.at[n], halo_recv_sem.at[n], (og, x, y),
        ))
        n += 1
    rad[g] = packed[g]
    for f in range(2):
        ext0[f, pl.ds(own_dst, L), ROWN : ROWN + R, :] = fields[f][...]
        for b in range(2):
            for p in (0, LE + 1):
                ext[b][f, p] = jnp.zeros((RE + 16, C), F32)

    log2e = 1.0 / math.log(2.0)
    for q, (ref, scale) in enumerate(((gas_ref, -log2e), (drop_ref, -log2e), (sw_ref, 1.0), (lw_ref, 1.0))):
        coef[q] = jnp.broadcast_to(ref[...] * scale, (128, G)).T
    for hb in range(B // 128):
        cloudy[hb] = flags_ref[:, hb * 128 : (hb + 1) * 128].astype(F32)

    c_packed.wait()
    for o in range(2):
        mo = rad[o, L : 2 * L, :]
        soft = jnp.maximum(mo, 0.0) + jnp.log1p(jnp.exp(-jnp.abs(mo)))
        for hb in range(B // 128):
            absorber[hb, o * L : (o + 1) * L, :] = soft[:, hb * 128 : (hb + 1) * 128]
            theta[hb, o * L : (o + 1) * L, :] = rad[o, 0:L, hb * 128 : (hb + 1) * 128]

    GB = G // 8
    norm = 4.0 / G
    for hb in range(B // 128):
        for o in range(2):
            def level(l, flux, o=o, hb=hb):
                lg = l + o * L
                a = jnp.broadcast_to(absorber[hb, pl.ds(lg, 1), :], (8, 128))
                c = jnp.broadcast_to(cloudy[hb, pl.ds(lg, 1), :], (8, 128))
                th = 1.0 + 0.1 * theta[hb, pl.ds(lg, 1), :]
                sw = lw = None
                new = []
                for q in range(GB):
                    rows = slice(8 * q, 8 * q + 8)
                    d = 1.0 - jnp.exp2(a * coef[0, rows, :] + c * coef[1, rows, :])
                    s = flux[q] * d
                    w = coef[3, rows, :] * d
                    sw = s if sw is None else sw + s
                    lw = w if lw is None else lw + w
                    new.append(flux[q] - s)
                total = jnp.sum(sw - lw * th, axis=0, keepdims=True) * norm
                rates[o, hb, pl.ds(l, 1), :] = total
                return tuple(new)

            if o == 0:
                flux = tuple(coef[2, 8 * q : 8 * q + 8, :] for q in range(GB))
            flux = lax.fori_loop(0, L, level, flux, unroll=2)
    c_heat = remote(rates.at[og], heat.at[g], misc_send_sem.at[1], misc_recv_sem.at[1], (og, x, y))
    heat[g] = rates[g]
    for o in range(2):
        for hb in range(B // 128):
            rates_out[o * L : (o + 1) * L, hb * 128 : (hb + 1) * 128] = rates[o, hb]

    lane = lax.broadcasted_iota(jnp.int32, (8, C), 1)

    def pack(vals, j, accs):
        right, left = accs
        for t in range(T):
            k = j * T + t
            turned = pltpu.roll(vals[8 * t : 8 * t + 8, :], lax.rem(k + 1, C), 1)
            right = jnp.where(lane == k, turned, right)
            left = jnp.where(lane == lax.rem(k + 1, C), turned, left)
        return right, left

    def send_edges(k, f):
        return (
            remote(edge_send.at[k, f, 0], edge_recv.at[k, f, 0],
                   edge_send_sem.at[k, f, 0], edge_recv_sem.at[k, f, 0], (g, x, yn)),
            remote(edge_send.at[k, f, 1], edge_recv.at[k, f, 1],
                   edge_send_sem.at[k, f, 1], edge_recv_sem.at[k, f, 1], (g, x, yp)),
        )

    zero = jnp.zeros((8, C), F32)

    def run_levels(k, f, count, values):
        for p in range(NP):
            lo, hi = p * per, min(count, (p + 1) * per)
            if lo >= hi:
                edge_send[k, f, 0, p] = zero
                edge_send[k, f, 1, p] = zero
                continue
            right, left = lax.fori_loop(
                lo, hi, lambda j, accs, lo=lo: pack(values(j), j - lo, accs), (zero, zero),
                unroll=min(UNROLL, hi - lo),
            )
            edge_send[k, f, 0, p] = right
            edge_send[k, f, 1, p] = left

    def first(f):
        run_levels(0, f, LE, lambda j: ext0[f, j + 1, RLO : RLO + RE, :])
        return send_edges(0, f)

    def sweep(k, f):
        src, dst = (k - 1) % 2, k % 2
        start = g * k
        last = k == SWEEPS
        t0, t1 = (M // 8, M // 8 + R // 8) if last else (0, T)
        r0, r1 = RLO + 8 * t0, RLO + 8 * t1

        def values(j):
            lev = start + j
            p = lev + 1
            jj = j + g
            which = jj // per
            kk = (jj - which * per) * T
            from_left = edge_recv[k - 1, f, 0, which]
            from_right = edge_recv[k - 1, f, 1, which]
            lg = lev + (L - M) * g
            sx = 0.5 * cx_ref[lg]
            sy = 0.5 * cy_ref[lg]
            cen = ext[src][f, p, r0:r1, :]
            base = (
                (1.0 - 4.0 * NU_H - 2.0 * NU_V) * cen
                + NU_V * (ext[src][f, p + 1, r0:r1, :] + ext[src][f, p - 1, r0:r1, :])
                + (NU_H - sx) * ext[src][f, p, r0 + 1 : r1 + 1, :]
                + (NU_H + sx) * ext[src][f, p, r0 - 1 : r1 - 1, :]
            )
            res = []
            for t in range(t0, t1):
                q = 8 * (t - t0)
                v = cen[q : q + 8, :]
                kt = kk + t
                prev = jnp.where(lane == 0, pltpu.roll(from_left, lax.rem(C - kt, C), 1), pltpu.roll(v, 1, 1))
                nxt = jnp.where(
                    lane == C - 1, pltpu.roll(from_right, lax.rem(2 * C - 2 - kt, C), 1), pltpu.roll(v, C - 1, 1)
                )
                res.append(base[q : q + 8, :] + (NU_H - sy) * nxt + (NU_H + sy) * prev)
            new = jnp.concatenate(res, axis=0)
            if last:
                outs[f][j] = new
            else:
                ext[dst][f, p, RLO : RLO + RE, :] = new
            return new

        count = LE - k
        if last:
            @pl.loop(0, count, unroll=UNROLL)
            def _(j):
                values(j)
            return None
        run_levels(k, f, count, values)
        return send_edges(k, f)

    for c in halos:
        c.wait()
    flight = [first(0), first(1)]
    sent = []

    def advance(ks):
        for k in ks:
            for f in range(2):
                for c in flight[f]:
                    c.wait()
                flight[f] = sweep(k, f)

    advance((1, 2))

    c_heat.wait()
    hi, lo = split_bf16(jnp.concatenate([heat[h, hb] for h in range(2) for hb in range(B // 128)], axis=1))
    spread = jnp.dot(jnp.concatenate([hi, lo], axis=0), qt[...], preferred_element_type=F32)
    spread = spread[:L] + spread[L:]
    LT = L // 8
    ehi = zero
    elo = zero
    for i in range(RI):
        ui = spread[:, i * C : (i + 1) * C]
        ucols[i] = ui
        for t in range(LT):
            k = i * LT + t
            turned = pltpu.roll(ui[8 * t : 8 * t + 8, :], (k + 1) % C, 1)
            ehi = jnp.where(lane == k, turned, ehi)
            elo = jnp.where(lane == (k + 1) % C, turned, elo)
    hedge_send[0] = ehi
    hedge_send[1] = elo
    c_he = [
        remote(hedge_send.at[0], hedge_recv.at[0], misc_send_sem.at[2], misc_recv_sem.at[2], (g, x, yn)),
        remote(hedge_send.at[1], hedge_recv.at[1], misc_send_sem.at[3], misc_recv_sem.at[3], (g, x, yp)),
    ]
    advance((3,))
    for c in c_he:
        c.wait()
    from_left = hedge_recv[0]
    from_right = hedge_recv[1]
    even = lane % 2 == 0
    for i in range(RI):
        for t in range(LT):
            k = i * LT + t
            v = ucols[i, 8 * t : 8 * t + 8, :]
            prev = jnp.where(lane == 0, pltpu.roll(from_left, (C - k) % C, 1), pltpu.roll(v, 1, 1))
            nxt = jnp.where(lane == C - 1, pltpu.roll(from_right, (2 * C - 2 - k) % C, 1), pltpu.roll(v, C - 1, 1))
            w = 0.75 * v + 0.25 * jnp.where(even, prev, nxt)
            ucols[i, 8 * t : 8 * t + 8, :] = w
            if i == 0:
                rows_send[0, 8 * t : 8 * t + 8, :] = w
            if i == RI - 1:
                rows_send[1, 8 * t : 8 * t + 8, :] = w
    c_rows = [
        remote(rows_send.at[0], rows_recv.at[0], misc_send_sem.at[4], misc_recv_sem.at[4], (g, xp, y)),
        remote(rows_send.at[1], rows_recv.at[1], misc_send_sem.at[5], misc_recv_sem.at[5], (g, xn, y)),
    ]
    advance(range(4, SWEEPS + 1))
    for c in c_rows:
        c.wait()
    flat = t_out.reshape(L * R, C)
    for i in range(RI):
        v = ucols[i]
        above = rows_recv[1] if i == 0 else ucols[i - 1]
        below = rows_recv[0] if i == RI - 1 else ucols[i + 1]
        flat[pl.ds(2 * i, L, stride=R), :] = flat[pl.ds(2 * i, L, stride=R), :] + HEATING_INTERVAL * (0.75 * v + 0.25 * above)
        flat[pl.ds(2 * i + 1, L, stride=R), :] = flat[pl.ds(2 * i + 1, L, stride=R), :] + HEATING_INTERVAL * (0.75 * v + 0.25 * below)


def hand_on(t_in, m_in, r_in, t_out, m_out, r_out):
    t_out[...] = t_in[...]
    m_out[...] = m_in[...]
    r_out[...] = r_in[...]


def wide_body(n_gx, n_gy, warm, humid, cx, cy, gas, drop, sw, lw, flags, slots):
    L, R, C = warm.shape
    S = slots.shape[0] * slots.shape[1]
    B = flags.shape[0]
    flags = flags.T
    G = gas.shape[0]
    LE = L + M
    T = (R + 2 * M) // 8
    NP = -(-LE // (C // T))
    vmem = pl.BlockSpec(memory_space=pltpu.VMEM)
    smem = pl.BlockSpec(memory_space=pltpu.SMEM)
    t, m, rates = pl.pallas_call(
        functools.partial(wide_kernel, n_gx, n_gy, L, R, C, S, B, G),
        out_shape=(
            jax.ShapeDtypeStruct((L, R, C), F32),
            jax.ShapeDtypeStruct((L, R, C), F32),
            jax.ShapeDtypeStruct((2 * L, B), F32),
        ),
        in_specs=[vmem, vmem, smem, smem] + [vmem] * 6,
        out_specs=(vmem, vmem, vmem),
        scratch_shapes=[
            pltpu.VMEM((2, LE + 2, R + 2 * M + 16, C), F32),
            pltpu.VMEM((2, LE + 2, R + 2 * M + 16, C), F32),
            pltpu.VMEM((SWEEPS, 2, 2, NP, 8, C), F32),
            pltpu.VMEM((SWEEPS, 2, 2, NP, 8, C), F32),
            pltpu.VMEM((S, (R // 2) * C), BF),
            pltpu.VMEM((2, 2 * L, B), F32),
            pltpu.VMEM((2, 2 * L, B), F32),
            pltpu.VMEM((4, G, 128), F32),
            pltpu.VMEM((B // 128, 2 * L, 128), F32),
            pltpu.VMEM((B // 128, 2 * L, 128), F32),
            pltpu.VMEM((B // 128, 2 * L, 128), F32),
            pltpu.VMEM((2, B // 128, L, 128), F32),
            pltpu.VMEM((2, B // 128, L, 128), F32),
            pltpu.VMEM((R // 2, L, C), F32),
            pltpu.VMEM((2, 8, C), F32),
            pltpu.VMEM((2, 8, C), F32),
            pltpu.VMEM((2, L, C), F32),
            pltpu.VMEM((2, L, C), F32),
            pltpu.SemaphoreType.DMA((10,)),
            pltpu.SemaphoreType.DMA((10,)),
            pltpu.SemaphoreType.DMA((SWEEPS, 2, 2)),
            pltpu.SemaphoreType.DMA((SWEEPS, 2, 2)),
            pltpu.SemaphoreType.DMA((6,)),
            pltpu.SemaphoreType.DMA((6,)),
        ],
        compiler_params=pltpu.CompilerParams(collective_id=0, has_side_effects=True),
    )(
        warm, humid, cx, cy, gas[None], drop[None], sw[None], lw[None], flags, slots,
    )
    t, m, rates = pl.pallas_call(
        hand_on,
        out_shape=tuple(jax.ShapeDtypeStruct(a.shape, F32) for a in (t, m, rates)),
        in_specs=[vmem] * 3,
        out_specs=(vmem,) * 3,
    )(t, m, rates)
    return t, m, rates.T


CHUNKS = ((0, 4), (4, 7), (7, 8))
PAD = 8


def pair_kernel(
    n_gx, L, R, C, S, B, G,
    warm_hbm, humid_hbm, cx_hbm, cy_hbm, gas_hbm, drop_hbm, sw_hbm, lw_hbm, flags_hbm, slot_hbm,
    res, heat_out, rates_out,
    fields, small, gpoint, flags_ref, slot_ref,
    loc, buf0, buf1, fin, got, adv, lines, qt, packed, rad, coef, cloudy, absorber, theta, passed, rates, heat, ucols, ends_send, ends_recv, corner_send, corner_recv,
    in_sem, pair_sem, lev_sem, row_send_sem, row_recv_sem, corner_sem, misc_sem, half_sem, gate,
):
    g = lax.axis_index("grp")
    x = lax.axis_index("gx")
    y = lax.axis_index("gy")
    og = 1 - g
    oy = 1 - y
    xn, xp = lax.rem(x + 1, n_gx), lax.rem(x + n_gx - 1, n_gx)
    LE = L + M
    RE = R + 2 * M
    RI = R // 2
    bufs = (buf0, buf1)

    sub = lax.broadcasted_iota(jnp.int32, (M, C), 0)
    barrier = pltpu.get_barrier_semaphore()
    partners = [(g, x, oy), (og, x, 0), (og, x, 1)]
    beside = [(g, xx, yy) for xx in (xn, xp) for yy in range(2)]
    partners += beside
    for dev in partners:
        pl.semaphore_signal(barrier, inc=1, device_id=dev, device_id_type=MESH)

    tail = x == n_gx - 1

    @pl.when(x == 0)
    def _():
        for yy in range(2):
            pl.semaphore_signal(barrier, inc=1, device_id=(og, xp, yy), device_id_type=MESH)

    loads = []
    pairs = [(warm_hbm, fields.at[0]), (humid_hbm, fields.at[1]), (slot_hbm, slot_ref)]
    pairs += [(cx_hbm, small.at[0]), (cy_hbm, small.at[1])]
    pairs += [(r, gpoint.at[q]) for q, r in enumerate((gas_hbm, drop_hbm, sw_hbm, lw_hbm))]
    pairs += [(flags_hbm, flags_ref)]
    for n, (src, dst) in enumerate(pairs):
        c = pltpu.make_async_copy(src, dst, in_sem.at[n])
        c.start()
        loads.append(c)

    def remote(src, dst, ss, rs, dev):
        c = pltpu.make_async_remote_copy(
            src_ref=src, dst_ref=dst, send_sem=ss, recv_sem=rs, device_id=dev, device_id_type=MESH
        )
        c.start()
        return c

    def matching(ref, sem):
        return pltpu.make_async_remote_copy(
            src_ref=ref, dst_ref=ref, send_sem=sem, recv_sem=sem, device_id=(g, x, oy), device_id_type=MESH
        )

    def arrived(ref, sem):
        matching(ref, sem).wait_recv()

    def left(ref, sem):
        matching(ref, sem).wait_send()

    edge = jnp.zeros((RE, 8, C), F32)
    for b in bufs:
        for h in range(2):
            b[h, :, 0:PAD, :] = edge
            b[h, :, PAD + LE : PAD + LE + 8, :] = edge

    for n in range(2):
        loads[n].wait()
    for f in range(2):
        flat = fields.at[f].reshape(L * R, C)
        for r in range(R):
            loc[f, r] = flat[pl.ds(r, L, stride=R), :]

    own_dst = pl.multiple_of(PAD + M * g, 8)
    lev_src = pl.multiple_of((L - M) * og, 8)
    lev_own = pl.multiple_of(PAD + M * g + (L - M) * og, 8)
    lev_dst = pl.multiple_of(PAD + L * g, 8)
    lev_in = pl.multiple_of(PAD + L * og, 8)

    def send_levels(r0, r1):
        for f in range(2):
            remote(
                loc.at[f, r0:r1, pl.ds(lev_src, M), :], buf0.at[y, M + r0 : M + r1, pl.ds(lev_dst, M), :],
                lev_sem.at[0], lev_sem.at[1], (og, x, f),
            )

    def greet():
        pl.semaphore_wait(barrier, jnp.where(tail, 9, 7))

        def pass_on(xx):
            for yy in range(2):
                pl.semaphore_signal(gate, inc=1, device_id=(g, xx, yy), device_id_type=MESH)

        pass_on(xn)
        pl.when(x > 0)(functools.partial(pass_on, xp))

        for c, (d1, d0) in enumerate(CHUNKS):
            for side, xx in ((0, xn), (1, xp)):
                s0 = R - d0 if side == 0 else d1
                t0 = M - d0 if side == 0 else M + R + d1
                for f in range(2):
                    remote(
                        loc.at[f, s0 : s0 + d0 - d1], buf0.at[y, t0 : t0 + d0 - d1, pl.ds(own_dst, L), :],
                        row_send_sem.at[0], row_recv_sem.at[side, c], (g, xx, f),
                    )
        remote(
            loc.at[oy], buf0.at[y, M : M + R, pl.ds(own_dst, L), :], pair_sem.at[0], pair_sem.at[1], (g, x, oy)
        )

    def gather():
        loads[2].wait()
        half = slot_ref.shape[1]
        slots = slot_ref[...]
        rep = (
            lax.broadcasted_iota(jnp.int32, (half, C), 1) // 2
            == lax.broadcasted_iota(jnp.int32, (half, C), 0)
        ).astype(F32).astype(BF)
        s_hi = (slots // 16).astype(F32).astype(BF)
        s_lo = (slots % 16).astype(F32).astype(BF)
        slot_rep = (
            16.0 * jnp.dot(s_hi, rep, preferred_element_type=F32)
            + jnp.dot(s_lo, rep, preferred_element_type=F32)
        ).astype(jnp.int32)
        s_iota = lax.broadcasted_iota(jnp.int32, (S, C), 0)
        for i in range(RI):
            qt[:, i * C : (i + 1) * C] = jnp.where(s_iota == slot_rep[i : i + 1, :], 1.0, 0.0).astype(BF)
        parts = []
        for i in range(RI):
            col = [loc[f, 2 * i] + loc[f, 2 * i + 1] for f in range(2)]
            hi, lo = split_bf16(0.25 * jnp.concatenate(col, axis=0))
            parts.append(jnp.concatenate([hi, lo], axis=0))
        lhs = jnp.concatenate(parts, axis=1)
        both = lax.dot_general(
            lhs, qt[...], (((1,), (1,)), ((), ())), preferred_element_type=F32
        )
        both = both[: 2 * L] + both[2 * L :]
        for h in range(2):
            packed[h] = both[:, h * B : (h + 1) * B]
        for n in range(3, len(loads)):
            loads[n].wait()
        for q in range(2):
            lines[q] = jnp.broadcast_to(small[q], (C, 2 * L)).T
        for q in range(2):
            part = 0.5 * lines[q, pl.ds(pl.multiple_of((L - M) * g, 8), LE), :]
            adv[2 * q] = NU_H - part
            adv[2 * q + 1] = NU_H + part
        log2e = 1.0 / math.log(2.0)
        for q, scale in enumerate((-log2e, -log2e, 1.0, 1.0)):
            coef[q] = jnp.broadcast_to(gpoint[q] * scale, (128, G)).T
        for hb in range(B // 128):
            cloudy[hb] = flags_ref[:, hb * 128 : (hb + 1) * 128].astype(F32)

    early = jnp.where(x == 0, 1, 0)

    @pl.loop(0, 2)
    def _(turn):
        pl.when(turn == 1 - early)(gather)
        pl.when(turn == early)(greet)

    c_packed = [
        remote(
            packed.at[og, :, hb * 128 : (hb + 1) * 128], rad.at[g, :, hb * 128 : (hb + 1) * 128],
            half_sem.at[0, hb], half_sem.at[1, hb], (og, x, y),
        )
        for hb in range(B // 128)
    ]
    for f in range(2):
        for side in range(2):
            for j in range(M // 2):
                d = j + 1
                near, far = (R - d, R - M + d) if side == 0 else (d - 1, M - d - 1)
                a = loc[f, near, pl.ds(lev_src, M), :]
                b = loc[f, far, pl.ds(lev_src, M), :]
                above = jnp.where(sub >= d, a, pltpu.roll(b, d, 0))
                below = jnp.where(sub < M - d, a, pltpu.roll(b, M - d, 0))
                corner_send[f, side, j] = jnp.where(g == 0, above, below)

    def corners_to(side, xx):
        for f in range(2):
            remote(
                corner_send.at[f, side], corner_recv.at[y, side],
                corner_sem.at[0], corner_sem.at[1], (og, xx, f),
            )

    def send_corners():
        pl.semaphore_wait(gate, jnp.where(tail, 2, 4))
        pl.when(x < n_gx - 1)(functools.partial(corners_to, 0, xn))
        corners_to(1, xp)

    pl.when(tail)(functools.partial(corners_to, 0, xn))
    send_levels(0, R)

    def rows_arrived(side, c):
        d1, d0 = CHUNKS[c]
        arrived(buf0.at[:, 0 : d0 - d1, pl.ds(own_dst, L), :], row_recv_sem.at[side, c])

    def corners_arrived():
        arrived(corner_recv, corner_sem.at[1])
        for h in range(2):
            for side in range(2):
                for j in range(M // 2):
                    d = j + 1
                    near, far = (M - d, d) if side == 0 else (M + R + d - 1, R + 2 * M - d - 1)
                    v = corner_recv[h, side, j]
                    buf0[h, near, pl.ds(lev_in, M), :] = v
                    if near != far:
                        back = jnp.where(g == 1, pltpu.roll(v, M - d, 0), pltpu.roll(v, d, 0))
                        buf0[h, far, pl.ds(lev_in, M), :] = back

    rad[g] = packed[g]
    buf0[y, M : M + R, pl.ds(own_dst, L), :] = loc[y]

    GB = G // 8
    HB = B // 128
    norm = 4.0 / G
    c_heat = pltpu.make_async_remote_copy(
        src_ref=rates.at[og], dst_ref=heat.at[g], send_sem=misc_sem.at[2], recv_sem=misc_sem.at[3],
        device_id=(og, x, y), device_id_type=MESH,
    )
    pl.when(g == 1)(send_corners)
    for o in range(2):
        for hb in range(HB):
            pl.when(og == o)(c_packed[hb].wait)
            cut = slice(hb * 128, (hb + 1) * 128)
            mo = rad[o, L : 2 * L, cut]
            soft = jnp.maximum(mo, 0.0) + jnp.log1p(jnp.exp(-jnp.abs(mo)))
            absorber[hb, o * L : (o + 1) * L, :] = soft
            theta[hb, o * L : (o + 1) * L, :] = rad[o, 0:L, cut]

            def level(l, flux, o=o, hb=hb):
                lg = l + o * L
                a = jnp.broadcast_to(absorber[hb, pl.ds(lg, 1), :], (8, 128))
                c = jnp.broadcast_to(cloudy[hb, pl.ds(lg, 1), :], (8, 128))
                th = 1.0 + 0.1 * theta[hb, pl.ds(lg, 1), :]
                sw = lw = None
                new = []
                for q in range(GB):
                    rows = slice(8 * q, 8 * q + 8)
                    d = 1.0 - jnp.exp2(a * coef[0, rows, :] + c * coef[1, rows, :])
                    s = flux[q] * d
                    w = coef[3, rows, :] * d
                    sw = s if sw is None else sw + s
                    lw = w if lw is None else lw + w
                    new.append(flux[q] - s)
                total = jnp.sum(sw - lw * th, axis=0, keepdims=True) * norm
                rates[o, hb, pl.ds(l, 1), :] = total
                return tuple(new)

            start = coef.at[2] if o == 0 else passed.at[hb]
            flux = tuple(start[8 * q : 8 * q + 8, :] for q in range(GB))
            flux = lax.fori_loop(0, L, level, flux, unroll=2)
            if o == 0:
                for q in range(GB):
                    passed[hb, 8 * q : 8 * q + 8, :] = flux[q]
            rates_out[o * L : (o + 1) * L, hb * 128 : (hb + 1) * 128] = rates[o, hb]

        @pl.when(og == o)
        def _():
            c_heat.start()
        if o == 0:
            pl.when(g == 0)(send_corners)
    heat[g] = rates[g]

    def stencil(k, i0, n):
        src, dst = bufs[(k - 1) % 2], bufs[k % 2]
        lane = lax.broadcasted_iota(jnp.int32, (n * LE, C), 1)
        span = [src[h, pl.ds(i0 - 1, n + 2), PAD : PAD + LE, :] for h in range(2)]
        mid = [v[1 : n + 1].reshape(n * LE, C) for v in span]
        right = [pltpu.roll(v, 1, 1) for v in mid]
        left = [pltpu.roll(v, C - 1, 1) for v in mid]
        for h in range(2):
            prev = jnp.where(lane == 0, right[1 - h], right[h]).reshape(n, LE, C)
            nxt = jnp.where(lane == C - 1, left[1 - h], left[h]).reshape(n, LE, C)
            up = src[h, pl.ds(i0, n), PAD - 1 : PAD + LE - 1, :]
            down = src[h, pl.ds(i0, n), PAD + 1 : PAD + LE + 1, :]
            new = (
                (1.0 - 4.0 * NU_H - 2.0 * NU_V) * span[h][1 : n + 1]
                + NU_V * (up + down)
                + adv[0][None] * span[h][2 : n + 2]
                + adv[1][None] * span[h][0:n]
                + adv[2][None] * nxt
                + adv[3][None] * prev
            )
            if k == SWEEPS:
                fin[h, pl.ds(i0 - M, n)] = new
            else:
                dst[h, pl.ds(i0, n), PAD : PAD + LE, :] = new

    mine = pl.multiple_of(M * g, 8)

    def widen(*parts, last=3):
        for d in range(max(d0 - d1 for _, d1, d0 in parts)):
            for k in range(1, SWEEPS + 1):
                for side, d1, d0 in parts:
                    e = d1 + d + 1
                    if e <= d0:
                        stencil(k, M + k - e if side == 0 else M + R - 1 - k + e, 1)
        for side, d1, d0 in parts:
            n = d0 - d1
            r = SWEEPS - d0 if side == 0 else R - SWEEPS + d1
            remote(
                fin.at[oy, r : r + n, pl.ds(mine, L), :], got.at[r : r + n],
                pair_sem.at[2], pair_sem.at[last], (g, x, oy),
            )

    arrived(buf0.at[oy, M : M + R, pl.ds(own_dst, L), :], pair_sem.at[1])
    arrived(buf0.at[:, M : M + R, pl.ds(lev_in, M), :], lev_sem.at[1])
    for k in range(1, SWEEPS):
        i0, i1 = M + k, M + R - k
        while i0 < i1:
            n = min(2, i1 - i0)
            stencil(k, i0, n)
            i0 += n

    LH = L // 2
    lane = lax.broadcasted_iota(jnp.int32, (LH, C), 1)
    even = lane % 2 == 0

    c_heat.wait()
    hi, lo = split_bf16(jnp.concatenate([heat[h, hb] for h in range(2) for hb in range(B // 128)], axis=1))
    spread = jnp.dot(jnp.concatenate([hi, lo], axis=0), qt[...], preferred_element_type=F32)
    spread = spread[:L] + spread[L:]
    for i in range(RI):
        ucols[y, 1 + i] = spread[:, i * C : (i + 1) * C]
    for e, i in ((1, 0), (0, RI - 1)):
        v = spread[:, i * C : (i + 1) * C]
        ends_send[e] = jnp.where(even, v[:LH], v[LH:])
    for e, xx in ((1, xp), (0, xn)):
        for yy in range(2):
            remote(ends_send.at[e], ends_recv.at[y, e], misc_sem.at[4], misc_sem.at[5], (g, xx, yy))
    remote(
        ucols.at[y, 1 : RI + 1], ucols.at[y, 1 : RI + 1], misc_sem.at[6], misc_sem.at[7], (g, x, oy)
    )
    corners_arrived()

    heat_flat = heat_out.reshape(L * R, C)

    def heat_rows():
        left(ucols.at[y, 1 : RI + 1], misc_sem.at[6])
        arrived(ucols.at[oy, 1 : RI + 1], misc_sem.at[7])
        arrived(ends_recv, misc_sem.at[5])
        for h in range(2):
            for e, i in ((0, 0), (1, RI + 1)):
                v = ends_recv[h, e]
                ucols[h, i, 0:LH] = jnp.where(even, v, pltpu.roll(v, 1, 1))
                ucols[h, i, LH:L] = jnp.where(even, pltpu.roll(v, C - 1, 1), v)
        lane = lax.broadcasted_iota(jnp.int32, (L, C), 1)
        cols = []
        for i in range(RI + 2):
            v, o = ucols[y, i], ucols[oy, i]
            prev = jnp.where(lane == 0, pltpu.roll(o, 1, 1), pltpu.roll(v, 1, 1))
            nxt = jnp.where(lane == C - 1, pltpu.roll(o, C - 1, 1), pltpu.roll(v, C - 1, 1))
            cols.append(HEATING_INTERVAL * (0.75 * v + 0.25 * jnp.where(lane % 2 == 0, prev, nxt)))
        for i in range(RI):
            heat_flat[pl.ds(2 * i, L, stride=R), :] = 0.75 * cols[i + 1] + 0.25 * cols[i]
            heat_flat[pl.ds(2 * i + 1, L, stride=R), :] = 0.75 * cols[i + 1] + 0.25 * cols[i + 2]

    def rows_in(first):
        second = 1 - first
        rows_arrived(first, 0)
        widen((first, 0, 4))
        rows_arrived(first, 1)
        rows_arrived(first, 2)
        rows_arrived(second, 0)
        widen((first, 4, 8), (second, 0, 4))
        rows_arrived(second, 1)
        widen((second,) + CHUNKS[1], last=4)
        rows_arrived(second, 2)
        widen((second,) + CHUNKS[2], last=4)

    for first in range(2):
        pl.when(lax.rem(x, 2) == first)(functools.partial(rows_in, first))
    flat = res.reshape(2 * L * R, C)
    for r in range(R):
        flat[pl.ds(y * (L * R) + r, L, stride=R), :] = fin[y, r, pl.ds(mine, L), :]
    late = M - CHUNKS[0][1]
    arrived(got.at[0 : R - late], pair_sem.at[3])

    def take(side, near, far):
        for e in range(near + 1, far + 1):
            r = M - e if side == 0 else R - M + e - 1
            flat[pl.ds(oy * (L * R) + r, L, stride=R), :] = got[r]

    def take_early(first):
        take(first, 0, M)
        take(1 - first, 0, M - late)

    def take_late(first):
        take(1 - first, M - late, M)

    for first in range(2):
        pl.when(lax.rem(x, 2) == first)(functools.partial(take_early, first))
    heat_rows()
    left(buf0.at[:, 0 : 2 * M, 0:L, :], row_send_sem.at[0])
    left(corner_send, corner_sem.at[0])
    left(buf0.at[:, 0:R, 0:M, :], lev_sem.at[0])
    left(loc.at[oy], pair_sem.at[0])
    left(ends_recv, misc_sem.at[4])
    arrived(got.at[0:late], pair_sem.at[4])
    for first in range(2):
        pl.when(lax.rem(x, 2) == first)(functools.partial(take_late, first))
    left(got, pair_sem.at[2])


def settle(res, heat, r_in, t_out, m_out, r_out, t_ref, sem):
    copies = [
        pltpu.make_async_copy(res.at[1], m_out, sem.at[0]),
        pltpu.make_async_copy(r_in, r_out, sem.at[1]),
        pltpu.make_async_copy(t_ref, t_out, sem.at[2]),
    ]
    copies[0].start()
    copies[1].start()
    t_ref[...] = res[0] + heat[...]
    copies[2].start()
    for c in copies:
        c.wait()


def pair_body(n_gx, n_gy, warm, humid, cx, cy, gas, drop, sw, lw, flags, slots):
    L, R, C = warm.shape
    S = slots.shape[0] * slots.shape[1]
    B = flags.shape[0]
    flags = flags.T
    G = gas.shape[0]
    LE = L + M
    LP = PAD + LE + 8
    RE = R + 2 * M
    vmem = pl.BlockSpec(memory_space=pltpu.VMEM)
    hbm = pl.BlockSpec(memory_space=pltpu.HBM)
    res, heat, rates = pl.pallas_call(
        functools.partial(pair_kernel, n_gx, L, R, C, S, B, G),
        out_shape=(
            jax.ShapeDtypeStruct((2, L, R, C), F32),
            jax.ShapeDtypeStruct((L, R, C), F32),
            jax.ShapeDtypeStruct((2 * L, B), F32),
        ),
        in_specs=[hbm] * 10,
        out_specs=(vmem, vmem, vmem),
        scratch_shapes=[
            pltpu.VMEM((2, L, R, C), F32),
            pltpu.VMEM((2, 1, 2 * L), F32),
            pltpu.VMEM((4, 1, G), F32),
            pltpu.VMEM((2 * L, B), jnp.int32),
            pltpu.VMEM(slots.shape, jnp.int32),
            pltpu.VMEM((2, R, L, C), F32),
            pltpu.VMEM((2, RE, LP, C), F32),
            pltpu.VMEM((2, RE, LP, C), F32),
            pltpu.VMEM((2, R, LE, C), F32),
            pltpu.VMEM((R, L, C), F32),
            pltpu.VMEM((4, LE, C), F32),
            pltpu.VMEM((2, 2 * L, C), F32),
            pltpu.VMEM((S, (R // 2) * C), BF),
            pltpu.VMEM((2, 2 * L, B), F32),
            pltpu.VMEM((2, 2 * L, B), F32),
            pltpu.VMEM((4, G, 128), F32),
            pltpu.VMEM((B // 128, 2 * L, 128), F32),
            pltpu.VMEM((B // 128, 2 * L, 128), F32),
            pltpu.VMEM((B // 128, 2 * L, 128), F32),
            pltpu.VMEM((B // 128, G, 128), F32),
            pltpu.VMEM((2, B // 128, L, 128), F32),
            pltpu.VMEM((2, B // 128, L, 128), F32),
            pltpu.VMEM((2, R // 2 + 2, L, C), F32),
            pltpu.VMEM((2, L // 2, C), F32),
            pltpu.VMEM((2, 2, L // 2, C), F32),
            pltpu.VMEM((2, 2, M // 2, M, C), F32),
            pltpu.VMEM((2, 2, M // 2, M, C), F32),
            pltpu.SemaphoreType.DMA((10,)),
            pltpu.SemaphoreType.DMA((5,)),
            pltpu.SemaphoreType.DMA((2,)),
            pltpu.SemaphoreType.DMA((1,)),
            pltpu.SemaphoreType.DMA((2, len(CHUNKS))),
            pltpu.SemaphoreType.DMA((2,)),
            pltpu.SemaphoreType.DMA((8,)),
            pltpu.SemaphoreType.DMA((2, B // 128)),
            pltpu.SemaphoreType.REGULAR,
        ],
        compiler_params=pltpu.CompilerParams(
            collective_id=0, has_side_effects=True, vmem_limit_bytes=32 * 1024 * 1024
        ),
    )(*(
        pltpu.with_memory_space_constraint(a, pltpu.HBM)
        for a in (warm, humid, cx[None], cy[None], gas[None], drop[None], sw[None], lw[None], flags, slots)
    ))
    t, m, rates = pl.pallas_call(
        settle,
        out_shape=(
            jax.ShapeDtypeStruct((L, R, C), F32),
            jax.ShapeDtypeStruct((L, R, C), F32),
            jax.ShapeDtypeStruct((2 * L, B), F32),
        ),
        in_specs=[vmem] * 3,
        out_specs=(hbm,) * 3,
        scratch_shapes=[
            pltpu.VMEM((L, R, C), F32),
            pltpu.SemaphoreType.DMA((3,)),
        ],
        compiler_params=pltpu.CompilerParams(vmem_limit_bytes=8 * 1024 * 1024),
    )(res, heat, rates)
    return t, m, rates.T


def solution(mesh):
    assert mesh.shape["grp"] == 2
    in_specs = (
        P("grp", "gx", "gy"), P("grp", "gx", "gy"), P(), P(), P(), P(), P(), P(),
        P(("grp", "gx", "gy"), None), P("gx", "gy"),
    )
    out_specs = (P("grp", "gx", "gy"), P("grp", "gx", "gy"), P(("grp", "gx", "gy"), None))
    paired = mesh.shape["gy"] == 2 and mesh.shape["gx"] > 2
    return jax.shard_map(
        functools.partial(pair_body if paired else wide_body, mesh.shape["gx"], mesh.shape["gy"]),
        mesh=mesh, in_specs=in_specs, out_specs=out_specs, check_vma=False,
    )
```
